64 devices in a mesh: dp: 4 (over x, y), sp: 16 (over z, core).
Axes of the slice: x: 2, y: 2, z: 8, core: 2. Of those that a mesh axis runs over, the one named last changes fastest.
The devices are a block of a 4x4x8 slice.
Arguments:
- x_in: bfloat16 [4, 4096, 2048], P('dp', 'sp'), parts along dimension 0
- grad_y: bfloat16 [4, 4096, 2048], P('dp', 'sp'), parts along dimension 0
- positions: int32 [4, 4096], P('dp', 'sp'), parts along dimension 0
- g_norm: bfloat16 [2048], replicated
- w_query: bfloat16 [2048, 2048], replicated
- w_key: bfloat16 [2048, 2048], replicated
- w_value: bfloat16 [2048, 2048], replicated
- w_out: bfloat16 [2048, 2048], replicated
- g_query: bfloat16 [2048], replicated
- g_key: bfloat16 [2048], replicated
Outputs:
- output 1: bfloat16 [4, 4096, 2048], P('dp', 'sp'), parts along dimension 0
- output 2: bfloat16 [4, 4096, 2048], P('dp', 'sp'), parts along dimension 0
- output 3: float32 [8192], P(('dp', 'sp')), parts along dimension 0
- output 4: float32 [8192, 2048], P(('dp', 'sp')), parts along dimension 0
- output 5: float32 [8192, 2048], P(('dp', 'sp')), parts along dimension 0
- output 6: float32 [8192, 2048], P(('dp', 'sp')), parts along dimension 0
- output 7: float32 [8192, 2048], P(('dp', 'sp')), parts along dimension 0
- output 8: float32 [8192], P(('dp', 'sp')), parts along dimension 0
- output 9: float32 [8192], P(('dp', 'sp')), parts along dimension 0
There are 4 independent parts. The reference program is written for one: setup_inputs(seed, part) draws one part's arguments, and reference() takes and returns one part's arrays. A program takes and returns all parts, laid end to end along the dimension named above; an argument that names none is the same for every part.
All inputs are finite; a program needn't handle non-finite values.
Results may differ from the reference program's by a relative error of at most 0.0111848.
Values are sent between devices in bfloat16 or wider.
A program may use at most 768 MiB of HBM per device.

```python
import jax
import jax.numpy as jnp
from jax import lax

N_BATCH = 1
SEQ_LEN = 4096
D_MODEL = 2048
N_HEADS = 16
HEAD_DIM = 128
QUERY_BLOCK = min(128, SEQ_LEN)
NORM_EPS = 1e-5
ROPE_BASE = 10000.0
NEG_BIG = -1e30


def setup_inputs(seed: int = 0, part: int = 0) -> dict:
    part_key = jax.random.fold_in(jax.random.key(seed), part)
    key_x, key_dy, key_pos = jax.random.split(part_key, 3)
    weight_keys = jax.random.split(jax.random.key(seed + 1), 9)
    act_shape = (N_BATCH, SEQ_LEN, D_MODEL)
    x_in = jax.random.normal(key_x, act_shape, jnp.float32).astype(jnp.bfloat16)
    grad_y = jax.random.normal(key_dy, act_shape, jnp.float32).astype(jnp.bfloat16)
    tok_idx = jnp.arange(SEQ_LEN, dtype=jnp.int32)
    restart = jax.random.randint(key_pos, (N_BATCH, SEQ_LEN), 0, 256) == 0
    doc_start = lax.cummax(jnp.where(restart, tok_idx[None, :], 0), axis=1)
    positions = (tok_idx[None, :] - doc_start).astype(jnp.int32)
    fan_scale = D_MODEL ** -0.5
    head_q = jnp.repeat(jax.random.uniform(weight_keys[0], (N_HEADS,), jnp.float32, 0.5, 1.5), HEAD_DIM)
    head_k = jnp.repeat(jax.random.uniform(weight_keys[1], (N_HEADS,), jnp.float32, 0.5, 1.5), HEAD_DIM)
    w_shape = (D_MODEL, D_MODEL)
    w_query = (jax.random.normal(weight_keys[2], w_shape, jnp.float32) * fan_scale * head_q[None, :]).astype(jnp.bfloat16)
    w_key = (jax.random.normal(weight_keys[3], w_shape, jnp.float32) * fan_scale * head_k[None, :]).astype(jnp.bfloat16)
    w_value = (jax.random.normal(weight_keys[4], w_shape, jnp.float32) * fan_scale).astype(jnp.bfloat16)
    w_out = (jax.random.normal(weight_keys[5], w_shape, jnp.float32) * fan_scale).astype(jnp.bfloat16)
    g_norm = (1.0 + 0.3 * jax.random.normal(weight_keys[6], (D_MODEL,), jnp.float32)).astype(jnp.bfloat16)
    g_query = (1.7 + 0.4 * jax.random.normal(weight_keys[7], (D_MODEL,), jnp.float32)).astype(jnp.bfloat16)
    g_key = (1.7 + 0.4 * jax.random.normal(weight_keys[8], (D_MODEL,), jnp.float32)).astype(jnp.bfloat16)
    return {'x_in': x_in, 'grad_y': grad_y, 'positions': positions, 'g_norm': g_norm, 'w_query': w_query, 'w_key': w_key, 'w_value': w_value, 'w_out': w_out, 'g_query': g_query, 'g_key': g_key}


def rms_scale(values, gain_vec):
    inv_rms = lax.rsqrt(jnp.mean(values * values, axis=-1, keepdims=True) + NORM_EPS)
    return values * inv_rms * gain_vec


def rope_tables(positions):
    half_dim = HEAD_DIM // 2
    inv_freq = ROPE_BASE ** (-jnp.arange(half_dim, dtype=jnp.float32) * (2.0 / HEAD_DIM))
    angles = positions.astype(jnp.float32)[..., None] * inv_freq
    return jnp.cos(angles)[:, :, None, :], jnp.sin(angles)[:, :, None, :]


def rope_apply(values, cos_t, sin_t):
    half_dim = values.shape[-1] // 2
    first_half = values[..., :half_dim]
    second_half = values[..., half_dim:]
    return jnp.concatenate([first_half * cos_t - second_half * sin_t, second_half * cos_t + first_half * sin_t], axis=-1)


def mat_f32(left_op, right_op):
    return jnp.dot(left_op, right_op, precision=lax.Precision.HIGHEST)


def causal_attention(q_bf, k_bf, v_bf):
    q_f = q_bf.astype(jnp.float32)
    k_f = k_bf.astype(jnp.float32)
    v_f = v_bf.astype(jnp.float32)
    key_pos = jnp.arange(SEQ_LEN)
    qk_scale = HEAD_DIM ** -0.5

    def one_block(q_start):
        q_blk = lax.dynamic_slice_in_dim(q_f, q_start, QUERY_BLOCK, axis=1)
        scores = jnp.einsum('bqhd,bkhd->bhqk', q_blk, k_f, precision=lax.Precision.HIGHEST) * qk_scale
        q_pos = q_start + jnp.arange(QUERY_BLOCK)
        scores = jnp.where(q_pos[:, None] >= key_pos[None, :], scores, NEG_BIG)
        prob_f = jax.nn.softmax(scores, axis=-1)
        return jnp.einsum('bhqk,bkhd->bqhd', prob_f, v_f, precision=lax.Precision.HIGHEST)

    starts = jnp.arange(SEQ_LEN // QUERY_BLOCK) * QUERY_BLOCK
    blocks = lax.map(jax.checkpoint(one_block), starts)
    merged = jnp.moveaxis(blocks, 0, 1).reshape(q_bf.shape)
    return merged.astype(jnp.bfloat16)


def reference(x_in, grad_y, positions, g_norm, w_query, w_key, w_value, w_out, g_query, g_key):
    cos_t, sin_t = rope_tables(positions)
    head_shape = (N_BATCH, SEQ_LEN, N_HEADS, HEAD_DIM)
    flat_shape = (N_BATCH, SEQ_LEN, D_MODEL)

    def forward(x_f, gain_n, wq_f, wk_f, wv_f, wo_f, gain_q, gain_k):
        hidden = rms_scale(x_f, gain_n).astype(jnp.bfloat16).astype(jnp.float32)
        q_raw = mat_f32(hidden, wq_f)
        k_raw = mat_f32(hidden, wk_f)
        v_val = mat_f32(hidden, wv_f).astype(jnp.bfloat16)
        q_rot = rope_apply(rms_scale(q_raw, gain_q).reshape(head_shape), cos_t, sin_t).astype(jnp.bfloat16)
        k_rot = rope_apply(rms_scale(k_raw, gain_k).reshape(head_shape), cos_t, sin_t).astype(jnp.bfloat16)
        attended = causal_attention(q_rot, k_rot, v_val.reshape(head_shape))
        o_proj = mat_f32(attended.reshape(flat_shape).astype(jnp.float32), wo_f)
        return (x_f + o_proj).astype(jnp.bfloat16)

    y_out, pullback = jax.vjp(forward, x_in.astype(jnp.float32), g_norm.astype(jnp.float32), w_query.astype(jnp.float32), w_key.astype(jnp.float32), w_value.astype(jnp.float32), w_out.astype(jnp.float32), g_query.astype(jnp.float32), g_key.astype(jnp.float32))
    cotangents = pullback(grad_y)
    return (y_out, cotangents[0].astype(jnp.bfloat16), cotangents[1], cotangents[2], cotangents[3], cotangents[4], cotangents[5], cotangents[6], cotangents[7])
```

```python
import functools
import jax
import jax.numpy as jnp
from jax import lax
from jax.experimental import pallas as pl
from jax.experimental.pallas import tpu as pltpu
from jax.sharding import PartitionSpec as P

HEAD=128
NT=(((1,),(1,)),((),()))
TN=(((0,),(0,)),((),()))
LOG2E=1.4426950408889634

def dotf(a,b,dims):
    return lax.dot_general(a,b,dims,preferred_element_type=jnp.float32)

def fwd_kernel(bq,bk,q_ref,k_ref,v_ref,o_ref,of_ref,lse_ref):
    j=pl.program_id(0)
    c=HEAD**-0.5*LOG2E
    q=q_ref[...]
    def step(kb,carry,masked):
        m,l,acc=carry
        ks=pl.multiple_of(kb*bk,bk)
        s=dotf(q,k_ref[pl.ds(ks,bk),:],NT)
        if masked:
            r=lax.broadcasted_iota(jnp.int32,(bq,bk),0)+j*bq
            cc=lax.broadcasted_iota(jnp.int32,(bq,bk),1)+ks
            s=jnp.where(r>=cc,s,-1e30)
        mn=jnp.maximum(m,jnp.max(s,axis=1,keepdims=True))
        al=jnp.exp2((m-mn)*c)
        p=jnp.exp2((s-mn)*c)
        l=l*al+jnp.sum(p,axis=1,keepdims=True)
        acc=acc*al+dotf(p.astype(jnp.bfloat16),v_ref[pl.ds(ks,bk),:],(((1,),(0,)),((),())))
        return mn,l,acc
    init=(jnp.full((bq,1),-1e30,jnp.float32),jnp.zeros((bq,1),jnp.float32),jnp.zeros((bq,HEAD),jnp.float32))
    nfull=j*(bq//bk)
    carry=lax.fori_loop(0,nfull,functools.partial(step,masked=False),init)
    for t in range(bq//bk):
        carry=step(nfull+t,carry,True)
    m,l,acc=carry
    o=acc/l
    of_ref[...]=o
    o_ref[...]=o.astype(jnp.bfloat16)
    lse=m*c+jnp.log2(l)
    lse_ref[...]=jnp.broadcast_to(jnp.broadcast_to(lse,(bq,HEAD)).T[0:1,:],(8,bq))

def attn_fwd(q,k,v,bq=512,bk=512):
    n=q.shape[0]
    full=pl.BlockSpec((n,HEAD),lambda j:(0,0))
    return pl.pallas_call(functools.partial(fwd_kernel,bq,bk),grid=(n//bq,),
      in_specs=[pl.BlockSpec((bq,HEAD),lambda j:(j,0)),full,full],
      out_specs=[pl.BlockSpec((bq,HEAD),lambda j:(j,0)),pl.BlockSpec((bq,HEAD),lambda j:(j,0)),pl.BlockSpec((8,bq),lambda j:(0,j))],
      out_shape=[jax.ShapeDtypeStruct((n,HEAD),jnp.bfloat16),jax.ShapeDtypeStruct((n,HEAD),jnp.float32),jax.ShapeDtypeStruct((8,n),jnp.float32)],
      name="attn_fwd")(q,k,v)

def bwd_kernel(bq,bk,q_ref,k_ref,v_ref,do_ref,lse_ref,dl_ref,dq_ref,dk_ref,dv_ref,dqa):
    j=pl.program_id(0)
    n=q_ref.shape[0]
    c=HEAD**-0.5*LOG2E
    scale=HEAD**-0.5
    @pl.when(j==0)
    def _(): dqa[...]=jnp.zeros_like(dqa)
    k=k_ref[...]; v=v_ref[...]
    def step(qb,carry,masked):
        dk,dv=carry
        qs=pl.multiple_of(qb*bq,bq)
        q=q_ref[pl.ds(qs,bq),:]; do=do_ref[pl.ds(qs,bq),:]
        st=dotf(k,q,NT)
        p=jnp.exp2(st*c-lse_ref[0:1,pl.ds(qs,bq)])
        if masked:
            r=lax.broadcasted_iota(jnp.int32,(bk,bq),0)+j*bk
            cc=lax.broadcasted_iota(jnp.int32,(bk,bq),1)+qs
            p=jnp.where(cc>=r,p,0.0)
        dp=dotf(v,do,NT)
        ds=(p*(dp-dl_ref[0:1,pl.ds(qs,bq)])).astype(jnp.bfloat16)
        dv=dv+dotf(p.astype(jnp.bfloat16),do,(((1,),(0,)),((),())))
        dk=dk+dotf(ds,q,(((1,),(0,)),((),())))
        dqa[pl.ds(qs,bq),:]+=dotf(ds,k,TN)
        return dk,dv
    z=jnp.zeros((bk,HEAD),jnp.float32)
    carry=(z,z)
    for t in range(bk//bq):
        carry=step(j*(bk//bq)+t,carry,True)
    dk,dv=lax.fori_loop((j+1)*(bk//bq),n//bq,functools.partial(step,masked=False),carry)
    dk_ref[...]=(dk*scale).astype(jnp.bfloat16); dv_ref[...]=dv.astype(jnp.bfloat16)
    @pl.when(j==pl.num_programs(0)-1)
    def _(): dq_ref[...]=(dqa[...]*scale).astype(jnp.bfloat16)

def attn_bwd(q,k,v,do,lse,dl,bq=512,bk=512):
    n=q.shape[0]
    full=pl.BlockSpec((n,HEAD),lambda j:(0,0))
    row=pl.BlockSpec((8,n),lambda j:(0,0))
    blk=pl.BlockSpec((bk,HEAD),lambda j:(j,0))
    o=jax.ShapeDtypeStruct((n,HEAD),jnp.bfloat16)
    return pl.pallas_call(functools.partial(bwd_kernel,bq,bk),grid=(n//bk,),
      in_specs=[full,blk,blk,full,row,row],out_specs=[full,blk,blk],out_shape=[o,o,o],
      scratch_shapes=[pltpu.VMEM((n,HEAD),jnp.float32)],name="attn_bwd")(q,k,v,do,lse,dl)

NORM_EPS = 1e-5
ROPE_BASE = 10000.0
MESH = pl.DeviceIdType.MESH
f32 = jnp.float32
bf16 = jnp.bfloat16


def spread_kernel(n, gather, x_ref, o_ref, send_sem, recv_sem):
    me = lax.axis_index('sp')
    barrier = pltpu.get_barrier_semaphore()
    for d in range(1, n):
        pl.semaphore_signal(barrier, inc=1, device_id={'sp': lax.rem(me + d, n)}, device_id_type=MESH)
    pl.semaphore_wait(barrier, n - 1)
    copies = []
    for d in range(1, n):
        to = lax.rem(me + d, n)
        src = x_ref if gather else x_ref.at[to]
        cp = pltpu.make_async_remote_copy(src_ref=src, dst_ref=o_ref.at[me], send_sem=send_sem.at[d], recv_sem=recv_sem.at[d], device_id={'sp': to}, device_id_type=MESH)
        cp.start()
        copies.append(cp)
    o_ref[me] = x_ref[...] if gather else x_ref[me]
    for cp in copies:
        cp.wait()


def spread(x, n, gather, cid):
    shape = (n,) + x.shape if gather else x.shape
    return pl.pallas_call(functools.partial(spread_kernel, n, gather), out_shape=jax.ShapeDtypeStruct(shape, x.dtype),
        in_specs=[pl.BlockSpec(memory_space=pltpu.VMEM)], out_specs=pl.BlockSpec(memory_space=pltpu.VMEM),
        scratch_shapes=[pltpu.SemaphoreType.DMA((n,)), pltpu.SemaphoreType.DMA((n,))],
        compiler_params=pltpu.CompilerParams(collective_id=cid, has_side_effects=True), name='spread%d' % cid)(x)


def rope_tables(positions):
    half = HEAD // 2
    inv_freq = ROPE_BASE ** (-jnp.arange(half, dtype=f32) * (2.0 / HEAD))
    ang = positions.astype(f32)[:, None] * inv_freq
    return jnp.cos(ang), jnp.sin(ang)


def rope(x, cos, sin):
    a, b = x[..., :HEAD // 2], x[..., HEAD // 2:]
    return jnp.concatenate([a * cos - b * sin, b * cos + a * sin], -1)


def unrope(x, cos, sin):
    a, b = x[..., :HEAD // 2], x[..., HEAD // 2:]
    return jnp.concatenate([a * cos + b * sin, b * cos - a * sin], -1)


def mm(a, b, dims=(((1,), (0,)), ((), ()))):
    return lax.dot_general(a, b, dims, preferred_element_type=f32)


def solution(mesh):
    n = mesh.shape['sp']

    def device_step(x_in, grad_y, positions, g_norm, wq, wk, wv, wo, gq, gk):
        me = lax.axis_index('sp')
        x = x_in[0].astype(f32)
        gy = grad_y[0]
        t_loc, d = x.shape
        t_all = t_loc * n
        hd = d // n
        nh = n
        gn_f, gq_f, gk_f = g_norm.astype(f32), gq.astype(f32), gk.astype(f32)
        x_inv = lax.rsqrt(jnp.mean(x * x, -1, keepdims=True) + NORM_EPS)
        x_hat = x * x_inv
        hid = (x_hat * gn_f).astype(bf16)
        h_all = lax.all_gather(hid, 'sp', axis=0, tiled=True)
        gy_all = lax.all_gather(gy, 'sp', axis=0, tiled=True)
        q1l = mm(hid, wq)
        k1l = mm(hid, wk)
        q_inv = lax.rsqrt(jnp.mean(q1l * q1l, -1) + NORM_EPS)
        k_inv = lax.rsqrt(jnp.mean(k1l * k1l, -1) + NORM_EPS)
        pos = positions[0]
        st = spread(jnp.stack([q_inv, k_inv, pos.astype(f32), q_inv, q_inv, q_inv, q_inv, q_inv]), n, True, 1)
        st = jnp.swapaxes(st, 0, 1).reshape(8, t_all)
        qi, ki = st[0][:, None], st[1][:, None]
        cos, sin = rope_tables(st[2])
        sl = lambda w: lax.dynamic_slice_in_dim(w, me * hd, hd, w.ndim - 1)
        gq_h, gk_h = sl(gq_f), sl(gk_f)
        qkv = mm(h_all, jnp.concatenate([sl(wq), sl(wk), sl(wv)], 1))
        q_hat, k_hat = qkv[:, :hd] * qi, qkv[:, hd:2 * hd] * ki
        q = rope(q_hat * gq_h, cos, sin).astype(bf16)
        k = rope(k_hat * gk_h, cos, sin).astype(bf16)
        v = qkv[:, 2 * hd:].astype(bf16)
        o, o_f, lse = attn_fwd(q, k, v)
        att = lax.all_to_all(o, 'sp', split_axis=0, concat_axis=1, tiled=True)
        wo_h = lax.dynamic_slice_in_dim(wo, me * hd, hd, 0)
        do = mm(gy_all, wo_h, (((1,), (1,)), ((), ()))).astype(bf16)
        delta = jnp.broadcast_to(jnp.sum(o_f * do.astype(f32), -1)[None], (8, t_all))
        dwo = mm(o, gy_all, (((0,), (0,)), ((), ())))
        y = (x + mm(att, wo)).astype(bf16)
        dq, dk, dv = attn_bwd(q, k, v, do, lse, delta)
        to_tok = lambda z: lax.all_to_all(z, 'sp', split_axis=0, concat_axis=1, tiled=True)
        dqt, dkt, dvt = to_tok(dq), to_tok(dk), to_tok(dv)
        cl, sn = rope_tables(pos)
        cl, sn = cl[:, None], sn[:, None]
        revert = lambda z: unrope(z.astype(f32).reshape(t_loc, nh, HEAD), cl, sn).reshape(t_loc, d)
        qh_l, kh_l = q1l * q_inv[:, None], k1l * k_inv[:, None]
        dqn, dkn = revert(dqt) * gq_f, revert(dkt) * gk_f
        mq, mk = jnp.mean(dqn * qh_l, -1), jnp.mean(dkn * kh_l, -1)
        ms = spread(jnp.stack([mq, mk, mq, mq, mq, mq, mq, mq]), n, True, 2)
        ms = jnp.swapaxes(ms, 0, 1).reshape(8, t_all)
        dq_rot, dk_rot = unrope(dq.astype(f32), cos, sin), unrope(dk.astype(f32), cos, sin)
        ggq, ggk = jnp.sum(dq_rot * q_hat, 0), jnp.sum(dk_rot * k_hat, 0)
        dq_raw = (qi * (dq_rot * gq_h - q_hat * ms[0][:, None])).astype(bf16)
        dk_raw = (ki * (dk_rot * gk_h - k_hat * ms[1][:, None])).astype(bf16)
        dw = mm(h_all, jnp.concatenate([dq_raw, dk_raw, dv], 1), (((0,), (0,)), ((), ())))
        dw = lax.all_to_all(dw.reshape(n, d // n, 3 * hd), 'sp', split_axis=0, concat_axis=0, tiled=True)
        dw = jnp.transpose(dw.reshape(n, d // n, 3, hd), (2, 1, 0, 3)).reshape(3, d // n, d)
        dq_l = (q_inv[:, None] * (dqn - qh_l * mq[:, None])).astype(bf16)
        dk_l = (k_inv[:, None] * (dkn - kh_l * mk[:, None])).astype(bf16)
        nt = (((1,), (1,)), ((), ()))
        d_hid = mm(dq_l, wq, nt) + mm(dk_l, wk, nt) + mm(dvt, wv, nt)
        d_hid = d_hid.astype(bf16).astype(f32)
        dxn = d_hid * gn_f
        gx = (gy.astype(f32) + x_inv * (dxn - x_hat * jnp.mean(dxn * x_hat, -1, keepdims=True))).astype(bf16)
        gn_part = jnp.sum(d_hid * x_hat, 0).reshape(n, 1, d // n)
        gn = jnp.sum(spread(jnp.broadcast_to(gn_part, (n, 8, d // n)), n, False, 3)[:, 0], 0)
        return (y[None], gx[None], gn, dw[0], dw[1], dw[2], dwo, ggq, ggk)

    seq_spec = P('dp', 'sp', None)
    rep2, rep1 = P(None, None), P(None)
    row_spec, vec_spec = P(('dp', 'sp'), None), P(('dp', 'sp'))
    return jax.shard_map(device_step, mesh=mesh, in_specs=(seq_spec, seq_spec, P('dp', 'sp'), rep1, rep2, rep2, rep2, rep2, rep1, rep1), out_specs=(seq_spec, seq_spec, vec_spec, row_spec, row_spec, row_spec, row_spec, vec_spec, vec_spec), check_vma=False)
```

```python
import contextlib
import functools
import jax
import jax.numpy as jnp
from jax import lax
from jax.experimental import pallas as pl
from jax.experimental.pallas import tpu as pltpu
from jax.sharding import PartitionSpec as P

HEAD=128
NORM_EPS = 1e-5
ROPE_BASE = 10000.0

NT=(((1,),(1,)),((),()))
TN=(((0,),(0,)),((),()))
LOG2E=1.4426950408889634

def dotf(a,b,dims):
    return lax.dot_general(a,b,dims,preferred_element_type=jnp.float32)

def fwd_kernel(bq,bk,q_ref,k_ref,v_ref,o_ref,of_ref,lse_ref):
    j=pl.program_id(0)
    c=HEAD**-0.5*LOG2E
    q=q_ref[...]
    def step(kb,carry,masked):
        m,l,acc=carry
        ks=pl.multiple_of(kb*bk,bk)
        s=dotf(q,k_ref[pl.ds(ks,bk),:],NT)
        if masked:
            r=lax.broadcasted_iota(jnp.int32,(bq,bk),0)+j*bq
            cc=lax.broadcasted_iota(jnp.int32,(bq,bk),1)+ks
            s=jnp.where(r>=cc,s,-1e30)
        mn=jnp.maximum(m,jnp.max(s,axis=1,keepdims=True))
        al=jnp.exp2((m-mn)*c)
        p=jnp.exp2((s-mn)*c)
        l=l*al+jnp.sum(p,axis=1,keepdims=True)
        acc=acc*al+dotf(p.astype(jnp.bfloat16),v_ref[pl.ds(ks,bk),:],(((1,),(0,)),((),())))
        return mn,l,acc
    init=(jnp.full((bq,1),-1e30,jnp.float32),jnp.zeros((bq,1),jnp.float32),jnp.zeros((bq,HEAD),jnp.float32))
    nfull=j*(bq//bk)
    carry=lax.fori_loop(0,nfull,functools.partial(step,masked=False),init)
    for t in range(bq//bk):
        carry=step(nfull+t,carry,True)
    m,l,acc=carry
    o=acc/l
    of_ref[...]=o
    o_ref[...]=o.astype(jnp.bfloat16)
    lse=m*c+jnp.log2(l)
    lse_ref[...]=jnp.broadcast_to(jnp.broadcast_to(lse,(bq,HEAD)).T[0:1,:],(8,bq))

def attn_fwd(q,k,v,bq=512,bk=512):
    n=q.shape[0]
    full=pl.BlockSpec((n,HEAD),lambda j:(0,0))
    return pl.pallas_call(functools.partial(fwd_kernel,bq,bk),grid=(n//bq,),
      in_specs=[pl.BlockSpec((bq,HEAD),lambda j:(j,0)),full,full],
      out_specs=[pl.BlockSpec((bq,HEAD),lambda j:(j,0)),pl.BlockSpec((bq,HEAD),lambda j:(j,0)),pl.BlockSpec((8,bq),lambda j:(0,j))],
      out_shape=[jax.ShapeDtypeStruct((n,HEAD),jnp.bfloat16),jax.ShapeDtypeStruct((n,HEAD),jnp.float32),jax.ShapeDtypeStruct((8,n),jnp.float32)],
      name="attn_fwd")(q,k,v)

f32 = jnp.float32
bf16 = jnp.bfloat16
MESH = pl.DeviceIdType.MESH
PROF = 0
scope = jax.named_scope if PROF else (lambda name: contextlib.nullcontext())
NN = (((1,), (0,)), ((), ()))


def greet(n, me):
    barrier = pltpu.get_barrier_semaphore()
    for d in range(1, n):
        pl.semaphore_signal(barrier, inc=1, device_id={'sp': lax.rem(me + d, n)}, device_id_type=MESH)
    pl.semaphore_wait(barrier, n - 1)


def remote(src, dst, ss, rs, to):
    return pltpu.make_async_remote_copy(src_ref=src, dst_ref=dst, send_sem=ss, recv_sem=rs, device_id={'sp': to}, device_id_type=MESH)


def back_kernel(n, q_ref, k_ref, v_ref, do_ref, o_ref, lse_ref, dl_ref, x_ref, wo_ref, gy_ref, h_ref,
                dq_ref, dkv_ref, tq_ref, tkv_ref, y_ref, dwo_ref, dwv_ref,
                dqa, att, dt, tile, wtile, s_o, r_o, s_kv, r_kv, s_q, r_q, s_t, s_w):
    me = lax.axis_index('sp')
    t_all = q_ref.shape[0]
    t_loc = t_all // n
    d = x_ref.shape[1]
    blk = 2 * t_loc
    nb = t_all // blk
    z = me // 2
    c = HEAD ** -0.5 * LOG2E
    scale = HEAD ** -0.5
    cw = tile.shape[2]
    nt = d // cw
    cols = pl.ds(pl.multiple_of(me * HEAD, HEAD), HEAD)

    def tile_copy(t):
        cs = pl.ds(pl.multiple_of(lax.rem(t, nt) * cw, cw), cw)
        return cs

    def gy_copy(t):
        return pltpu.make_async_copy(gy_ref.at[:, tile_copy(t)], tile.at[lax.rem(t, 2)], s_t.at[lax.rem(t, 2)])

    def h_copy(t):
        return pltpu.make_async_copy(h_ref.at[:, tile_copy(t)], tile.at[lax.rem(t, 2)], s_t.at[lax.rem(t, 2)])

    def w_copy(t):
        return pltpu.make_async_copy(wo_ref.at[:, tile_copy(t)], wtile.at[lax.rem(t, 2)], s_w.at[lax.rem(t, 2)])

    gy_copy(0).start()
    w_copy(0).start()
    with scope('greet'):
        greet(n, me)

    def rows(i):
        return pl.ds(pl.multiple_of(i * t_loc, t_loc), t_loc)

    def o_send(e):
        to = lax.rem(me + e, n)
        return remote(o_ref.at[rows(to), :], att.at[:, cols], s_o.at[e], r_o.at[e], to)

    def q_send(e):
        to = lax.rem(me + e, n)
        return remote(dq_ref.at[rows(to), :], tq_ref.at[:, cols], s_q.at[e], r_q.at[e], to)

    def kv_send(to):
        e = lax.rem(to + n - me, n)
        return remote(dkv_ref.at[to], tkv_ref.at[:, :, cols], s_kv.at[e], r_kv.at[e], to)

    for e in range(1, n):
        o_send(e).start()
    att[:, cols] = o_ref[rows(me), :]
    dqa[...] = jnp.zeros_like(dqa)

    def step(s, _):
        kb = lax.rem(z + 1 + s, nb)
        ks = pl.ds(pl.multiple_of(kb * blk, blk), blk)
        k = k_ref[ks, :]
        v = v_ref[ks, :]

        def unit(qb, carry, masked):
            dk, dv = carry
            qs = pl.ds(pl.multiple_of(qb * blk, blk), blk)
            q = q_ref[qs, :]
            do = do_ref[qs, :]
            st = dotf(k, q, NT)
            p = jnp.exp2(st * c - lse_ref[0:1, qs])
            if masked:
                r = lax.broadcasted_iota(jnp.int32, (blk, blk), 0)
                cc = lax.broadcasted_iota(jnp.int32, (blk, blk), 1)
                p = jnp.where(cc >= r, p, 0.0)
            dp = dotf(v, do, NT)
            ds = (p * (dp - dl_ref[0:1, qs])).astype(bf16)
            dv = dv + dotf(p.astype(bf16), do, NN)
            dk = dk + dotf(ds, q, NN)
            dqa[qs, :] += dotf(ds, k, TN)
            return dk, dv

        zero = jnp.zeros((blk, HEAD), f32)
        carry = unit(kb, (zero, zero), True)
        dk, dv = lax.fori_loop(kb + 1, nb, functools.partial(unit, masked=False), carry)
        dk = (dk * scale).astype(bf16)
        dv = dv.astype(bf16)
        for u in range(2):
            to = 2 * kb + u
            dkv_ref[to, 0] = dk[u * t_loc:(u + 1) * t_loc]
            dkv_ref[to, 1] = dv[u * t_loc:(u + 1) * t_loc]

        @pl.when(kb != z)
        def _():
            for u in range(2):
                kv_send(2 * kb + u).start()

        @pl.when(kb == z)
        def _():
            kv_send(me + 1 - 2 * lax.rem(me, 2)).start()
        return 0

    with scope('bwd'):
        lax.fori_loop(0, nb, step, 0)
    with scope('dqsend'):
        dq_ref[...] = (dqa[...] * scale).astype(bf16)
        for e in range(1, n):
            q_send(e).start()
        tq_ref[:, cols] = dq_ref[rows(me), :]
        tkv_ref[:, :, cols] = dkv_ref[me]

    def flip(i, _):
        dt[:, rows(i)] = o_ref[rows(i), :].T
        return 0

    with scope('flip'):
        lax.fori_loop(0, n, flip, 0)

    def dwo_step(t, _):
        gy_copy(t).wait()

        @pl.when(t + 1 < nt)
        def _():
            gy_copy(t + 1).start()

        @pl.when(t + 1 == nt)
        def _():
            h_copy(t + 1).start()
        dwo_ref[:, tile_copy(t)] = dotf(dt[...], tile[lax.rem(t, 2)], NN)
        return 0

    with scope('dwo'):
        lax.fori_loop(0, nt, dwo_step, 0)

    def flip2(i, _):
        dt[:, rows(i)] = dkv_ref[i, 1].T
        return 0

    with scope('flip2'):
        lax.fori_loop(0, n, flip2, 0)

    def dwv_step(t, _):
        h_copy(t).wait()

        @pl.when(t + 1 < 2 * nt)
        def _():
            h_copy(t + 1).start()
        r = dotf(dt[...], tile[lax.rem(t, 2)], NN)
        for u in range(2):
            dwv_ref[2 * (t - nt) + u] = r[:, u * HEAD:(u + 1) * HEAD].T
        return 0

    with scope('dwv'):
        lax.fori_loop(nt, 2 * nt, dwv_step, 0)
    with scope('waito'):
        for e in range(1, n):
            o_send(e).wait()

    def y_step(t, _):
        w_copy(t).wait()

        @pl.when(t + 1 < nt)
        def _():
            w_copy(t + 1).start()
        y_ref[:, tile_copy(t)] = (x_ref[:, tile_copy(t)].astype(f32) + dotf(att[...], wtile[lax.rem(t, 2)], NN)).astype(bf16)
        return 0

    with scope('y'):
        lax.fori_loop(0, nt, y_step, 0)
    for e in range(1, n):
        kv_send(lax.rem(me + e, n)).wait()
        q_send(e).wait()


def back(n, q, k, v, do, o, lse, dl, x, wo, gy, h, cid):
    t_all, d = h.shape
    t_loc = t_all // n
    vm = pl.BlockSpec(memory_space=pltpu.VMEM)
    hb = pl.BlockSpec(memory_space=pl.ANY)
    S = jax.ShapeDtypeStruct
    sem = pltpu.SemaphoreType.DMA
    return pl.pallas_call(functools.partial(back_kernel, n),
        in_specs=[vm] * 8 + [hb] * 3, out_specs=[vm] * 7,
        out_shape=[S((t_all, HEAD), bf16), S((n, 2, t_loc, HEAD), bf16), S((t_loc, d), bf16), S((2, t_loc, d), bf16), S((t_loc, d), bf16), S((HEAD, d), f32), S((n, d // n, HEAD), f32)],
        scratch_shapes=[pltpu.VMEM((t_all, HEAD), f32), pltpu.VMEM((t_loc, d), bf16), pltpu.VMEM((HEAD, t_all), bf16), pltpu.VMEM((2, t_all, 2 * HEAD), bf16), pltpu.VMEM((2, d, 2 * HEAD), bf16)]
        + [sem((n,))] * 6 + [sem((2,))] * 2,
        compiler_params=pltpu.CompilerParams(collective_id=cid, has_side_effects=True, vmem_limit_bytes=60 * 1024 * 1024), name='back')(q, k, v, do, o, lse, dl, x, wo, gy, h)


def last_kernel(n, dq_ref, dkv_ref, tq_ref, tkv_ref, bv_ref, qt_ref, kt_ref, iv_ref, cs_ref, gc_ref,
                ql_ref, kl_ref, il_ref, cl_ref, sl_ref, g_ref, x_ref, gy_ref, h_ref, wq_ref, wk_ref, wv_ref,
                gx_ref, dwq_ref, dwk_ref, dwv_ref, gg_ref, gn_ref,
                raw, stage, dloc, dh, mine, mall, gpart, gall, tile, wtile,
                s_v, r_v, s_a, r_a, s_b, r_b, s_m, r_m, s_g, r_g, s_t, s_w):
    me = lax.axis_index('sp')
    t_all = h_ref.shape[0]
    t_loc, d = x_ref.shape
    z = me // 2
    cw = tile.shape[2]
    nt = d // cw
    wr = wtile.shape[2]
    nw = d // wr
    half = HEAD // 2
    cols = pl.ds(pl.multiple_of(me * HEAD, HEAD), HEAD)

    def h_copy(t):
        cs = pl.ds(pl.multiple_of(lax.rem(z + 1 + t, nt) * cw, cw), cw)
        return pltpu.make_async_copy(h_ref.at[:, cs], tile.at[lax.rem(t, 2)], s_t.at[lax.rem(t, 2)])

    def w_copies(t):
        rs = pl.ds(pl.multiple_of(t * wr, wr), wr)
        sl = lax.rem(t, 2)
        return [pltpu.make_async_copy(w.at[rs, :], wtile.at[sl, i], s_w.at[sl, i]) for i, w in enumerate((wq_ref, wk_ref, wv_ref))]

    h_copy(0).start()
    for cp in w_copies(0):
        cp.start()
    with scope('greet'):
        greet(n, me)

    def v_send(e):
        to = lax.rem(me + e, n)
        return remote(bv_ref.at[to], dwv_ref.at[:, cols], s_v.at[e], r_v.at[e], to)

    def a_send(to):
        e = lax.rem(to + n - me, n)
        return remote(stage.at[0, to], dwq_ref.at[:, cols], s_a.at[e], r_a.at[e], to)

    def b_send(to):
        e = lax.rem(to + n - me, n)
        return remote(stage.at[1, to], dwk_ref.at[:, cols], s_b.at[e], r_b.at[e], to)

    def m_send(e):
        to = lax.rem(me + e, n)
        return remote(mine, mall.at[me], s_m.at[e], r_m.at[e], to)

    def g_send(e):
        to = lax.rem(me + e, n)
        return remote(gpart.at[to], gall.at[me], s_g.at[e], r_g.at[e], to)

    cl = cl_ref[...]
    sl = sl_ref[...]

    def back_rope(a):
        a = a.astype(f32)
        return a * cl + pltpu.roll(a, half, 1) * sl

    def hs(i):
        return pl.ds(pl.multiple_of(i * HEAD, HEAD), HEAD)

    def mean_step(i, carry):
        a, b = carry
        a = a + back_rope(tq_ref[:, hs(i)]) * g_ref[0:1, hs(i)] * ql_ref[:, hs(i)]
        b = b + back_rope(tkv_ref[0, :, hs(i)]) * g_ref[1:2, hs(i)] * kl_ref[:, hs(i)]
        return a, b

    zero = jnp.zeros((t_loc, HEAD), f32)
    with scope('mean'):
        a, b = lax.fori_loop(0, d // HEAD, mean_step, (zero, zero))
        mq = jnp.sum(a, axis=1, keepdims=True) * (1.0 / d)
        mk = jnp.sum(b, axis=1, keepdims=True) * (1.0 / d)
    with scope('msend'):
        mine[...] = jnp.zeros_like(mine)
        mine[0:1, :] = jnp.broadcast_to(mq, (t_loc, HEAD)).T[0:1, :]
        mine[1:2, :] = jnp.broadcast_to(mk, (t_loc, HEAD)).T[0:1, :]
        for e in range(1, n):
            m_send(e).start()
        for e in range(1, n):
            v_send(e).start()
        dwv_ref[:, cols] = bv_ref[me]
        mall[me] = mine[...]

    qi = il_ref[:, 0:1]
    ki = il_ref[:, 1:2]

    def loc_step(i, _):
        dloc[0, :, hs(i)] = (qi * (back_rope(tq_ref[:, hs(i)]) * g_ref[0:1, hs(i)] - ql_ref[:, hs(i)] * mq)).astype(bf16)
        dloc[1, :, hs(i)] = (ki * (back_rope(tkv_ref[0, :, hs(i)]) * g_ref[1:2, hs(i)] - kl_ref[:, hs(i)] * mk)).astype(bf16)
        return 0

    with scope('loc'):
        lax.fori_loop(0, d // HEAD, loc_step, 0)
    with scope('mwait'):
        for e in range(1, n):
            m_send(e).wait()

    def head_step(j, carry):
        js = pl.ds(pl.multiple_of(j * t_loc, t_loc), t_loc)
        rs = js
        ct = cs_ref[0, :, js]
        sn = cs_ref[1, :, js]
        out = []
        for u, (src, hat) in enumerate(((dq_ref[rs, :], qt_ref), (dkv_ref[j, 0], kt_ref))):
            w = src.astype(f32).T
            p, r = w[:half], w[half:]
            w = jnp.concatenate([p * ct + r * sn, r * ct - p * sn], axis=0)
            hat = hat[:, js]
            out.append(carry[u] + w * hat)
            raw[u * HEAD:(u + 1) * HEAD, js] = (iv_ref[u:u + 1, js] * (w * gc_ref[:, u:u + 1] - hat * mall[j, u:u + 1, :])).astype(bf16)
        return tuple(out)

    zt = jnp.zeros((HEAD, t_loc), f32)
    with scope('head'):
        aq, ak = lax.fori_loop(0, n, head_step, (zt, zt))
        for u, a in enumerate((aq, ak)):
            col = jnp.sum(a, axis=1, keepdims=True)
            gg_ref[u] = jnp.broadcast_to(col, (HEAD, HEAD)).T[0:8, :]

    def dw_step(t, _):
        h_copy(t).wait()

        @pl.when(t + 1 < nt)
        def _():
            h_copy(t + 1).start()
        nn = lax.rem(z + 1 + t, nt)
        r = dotf(raw[...], tile[lax.rem(t, 2)], NN)
        for u in range(2):
            to = 2 * nn + u
            for w in range(2):
                stage[w, to] = r[w * HEAD:(w + 1) * HEAD, u * HEAD:(u + 1) * HEAD].T

            @pl.when(to != me)
            def _():
                a_send(to).start()
                b_send(to).start()
        return 0

    with scope('dw'):
        lax.fori_loop(0, nt, dw_step, 0)
        dwq_ref[:, cols] = stage[0, me]
        dwk_ref[:, cols] = stage[1, me]

    def dh_step(t, _):
        for cp in w_copies(t):
            cp.wait()

        @pl.when(t + 1 < nw)
        def _():
            for cp in w_copies(t + 1):
                cp.start()
        sl = lax.rem(t, 2)
        r = dotf(dloc[0], wtile[sl, 0], NT) + dotf(dloc[1], wtile[sl, 1], NT) + dotf(tkv_ref[1], wtile[sl, 2], NT)
        dh[:, pl.ds(pl.multiple_of(t * wr, wr), wr)] = r.astype(bf16).astype(f32)
        return 0

    with scope('dh'):
        lax.fori_loop(0, nw, dh_step, 0)

    def ms_step(i, carry):
        sx, sg = carry
        xf = x_ref[:, hs(i)].astype(f32)
        return sx + xf * xf, sg + dh[:, hs(i)] * g_ref[2:3, hs(i)] * xf

    with scope('ms'):
        sx, sg = lax.fori_loop(0, d // HEAD, ms_step, (zero, zero))
        xi = lax.rsqrt(jnp.sum(sx, axis=1, keepdims=True) * (1.0 / d) + NORM_EPS)
        mx = jnp.sum(sg, axis=1, keepdims=True) * xi * (1.0 / d)

    def gx_step(i, _):
        xh = x_ref[:, hs(i)].astype(f32) * xi
        dhh = dh[:, hs(i)]
        gpart[i] = jnp.broadcast_to(jnp.sum(dhh * xh, axis=0, keepdims=True), (8, HEAD))
        gx_ref[:, hs(i)] = (gy_ref[:, hs(i)].astype(f32) + xi * (dhh * g_ref[2:3, hs(i)] - xh * mx)).astype(bf16)
        return 0

    with scope('gx'):
        lax.fori_loop(0, d // HEAD, gx_step, 0)
    with scope('gsend'):
        for e in range(1, n):
            g_send(e).start()
        gall[me] = gpart[me]
        for e in range(1, n):
            g_send(e).wait()
        gn_ref[...] = jnp.sum(gall[...], axis=0)
    for e in range(1, n):
        v_send(e).wait()
        a_send(lax.rem(me + e, n)).wait()
        b_send(lax.rem(me + e, n)).wait()


def last(n, vmem_args, hbm_args, cid):
    t_all, d = hbm_args[0].shape
    t_loc = t_all // n
    vm = pl.BlockSpec(memory_space=pltpu.VMEM)
    hb = pl.BlockSpec(memory_space=pl.ANY)
    S = jax.ShapeDtypeStruct
    V = pltpu.VMEM
    sem = pltpu.SemaphoreType.DMA
    return pl.pallas_call(functools.partial(last_kernel, n),
        in_specs=[vm] * len(vmem_args) + [hb] * 4, out_specs=[vm] * 6,
        out_shape=[S((t_loc, d), bf16)] + [S((d // n, d), f32)] * 3 + [S((2, 8, HEAD), f32), S((8, d // n), f32)],
        scratch_shapes=[V((2 * HEAD, t_all), bf16), V((2, n, d // n, HEAD), f32), V((2, t_loc, d), bf16), V((t_loc, d), f32), V((8, t_loc), f32), V((n, 8, t_loc), f32), V((n, 8, d // n), f32), V((n, 8, d // n), f32), V((2, t_all, 2 * HEAD), bf16), V((2, 3, 256, d), bf16)]
        + [sem((n,))] * 10 + [sem((2,)), sem((2, 3))],
        compiler_params=pltpu.CompilerParams(collective_id=cid, has_side_effects=True, vmem_limit_bytes=63 * 1024 * 1024), name='last')(*vmem_args, *hbm_args)


def spread_kernel(n, gather, x_ref, o_ref, send_sem, recv_sem):
    me = lax.axis_index('sp')
    barrier = pltpu.get_barrier_semaphore()
    for d in range(1, n):
        pl.semaphore_signal(barrier, inc=1, device_id={'sp': lax.rem(me + d, n)}, device_id_type=MESH)
    pl.semaphore_wait(barrier, n - 1)
    copies = []
    for d in range(1, n):
        to = lax.rem(me + d, n)
        src = x_ref if gather else x_ref.at[to]
        cp = pltpu.make_async_remote_copy(src_ref=src, dst_ref=o_ref.at[me], send_sem=send_sem.at[d], recv_sem=recv_sem.at[d], device_id={'sp': to}, device_id_type=MESH)
        cp.start()
        copies.append(cp)
    o_ref[me] = x_ref[...] if gather else x_ref[me]
    for cp in copies:
        cp.wait()


def spread(x, n, gather, cid):
    shape = (n,) + x.shape if gather else x.shape
    return pl.pallas_call(functools.partial(spread_kernel, n, gather), out_shape=jax.ShapeDtypeStruct(shape, x.dtype),
        in_specs=[pl.BlockSpec(memory_space=pltpu.VMEM)], out_specs=pl.BlockSpec(memory_space=pltpu.VMEM),
        scratch_shapes=[pltpu.SemaphoreType.DMA((n,)), pltpu.SemaphoreType.DMA((n,))],
        compiler_params=pltpu.CompilerParams(collective_id=cid, has_side_effects=True), name='spread%d' % cid)(x)


def rope_tables(positions):
    half = HEAD // 2
    inv_freq = ROPE_BASE ** (-jnp.arange(half, dtype=f32) * (2.0 / HEAD))
    ang = positions.astype(f32)[:, None] * inv_freq
    return jnp.cos(ang), jnp.sin(ang)


def rope(x, cos, sin):
    a, b = x[..., :HEAD // 2], x[..., HEAD // 2:]
    return jnp.concatenate([a * cos - b * sin, b * cos + a * sin], -1)


def mm(a, b, dims=(((1,), (0,)), ((), ()))):
    return lax.dot_general(a, b, dims, preferred_element_type=f32)


def solution(mesh):
    n = mesh.shape['sp']

    def device_step(x_in, grad_y, positions, g_norm, wq, wk, wv, wo, gq, gk):
        me = lax.axis_index('sp')
        xb = x_in[0]
        x = xb.astype(f32)
        gy = grad_y[0]
        t_loc, d = x.shape
        t_all = t_loc * n
        hd = d // n
        gn_f, gq_f, gk_f = g_norm.astype(f32), gq.astype(f32), gk.astype(f32)
        x_inv = lax.rsqrt(jnp.mean(x * x, -1, keepdims=True) + NORM_EPS)
        hid = (x * x_inv * gn_f).astype(bf16)
        h_all = lax.all_gather(hid, 'sp', axis=0, tiled=True)
        gy_all = lax.all_gather(gy, 'sp', axis=0, tiled=True)
        q1l = mm(hid, wq)
        k1l = mm(hid, wk)
        q_inv = lax.rsqrt(jnp.mean(q1l * q1l, -1) + NORM_EPS)
        k_inv = lax.rsqrt(jnp.mean(k1l * k1l, -1) + NORM_EPS)
        pos = positions[0]
        st = spread(jnp.stack([q_inv, k_inv, pos.astype(f32), q_inv, q_inv, q_inv, q_inv, q_inv]), n, True, 1)
        st = jnp.swapaxes(st, 0, 1).reshape(8, t_all)
        qi, ki = st[0][:, None], st[1][:, None]
        cos, sin = rope_tables(st[2])
        cs_t = jnp.stack([cos.T, sin.T])
        sl = lambda w: lax.dynamic_slice_in_dim(w, me * hd, hd, w.ndim - 1)
        gq_h, gk_h = sl(gq_f), sl(gk_f)
        qkv = mm(h_all, jnp.concatenate([sl(wq), sl(wk), sl(wv)], 1))
        q_hat, k_hat = qkv[:, :hd] * qi, qkv[:, hd:2 * hd] * ki
        q = rope(q_hat * gq_h, cos, sin).astype(bf16)
        k = rope(k_hat * gk_h, cos, sin).astype(bf16)
        v = qkv[:, 2 * hd:].astype(bf16)
        o, o_f, lse = attn_fwd(q, k, v)
        wo_h = lax.dynamic_slice_in_dim(wo, me * hd, hd, 0)
        do = mm(gy_all, wo_h, (((1,), (1,)), ((), ()))).astype(bf16)
        delta = jnp.broadcast_to(jnp.sum(o_f * do.astype(f32), -1)[None], (8, t_all))
        dq, dkv, tq, tkv, y, dwo, bv = back(n, q, k, v, do, o, lse, delta, xb, wo, gy_all, h_all, 4)
        cl, sn = rope_tables(pos)
        cl, sn = jnp.concatenate([cl, cl], 1), jnp.concatenate([sn, -sn], 1)
        qh_l, kh_l = q1l * q_inv[:, None], k1l * k_inv[:, None]
        gains = jnp.stack([gq_f, gk_f, gn_f] + [gn_f] * 5)
        gx, dwq, dwk, dwv, gg, gn = last(n, [dq, dkv, tq, tkv, bv, q_hat.T, k_hat.T, st, cs_t, jnp.stack([gq_h, gk_h], 1), qh_l, kh_l, jnp.stack([q_inv, k_inv], 1), cl, sn, gains, xb, gy], [h_all, wq, wk, wv], 5)
        return (y[None], gx[None], gn[0], dwq, dwk, dwv, dwo, gg[0, 0], gg[1, 0])

    seq_spec = P('dp', 'sp', None)
    rep2, rep1 = P(None, None), P(None)
    row_spec, vec_spec = P(('dp', 'sp'), None), P(('dp', 'sp'))
    return jax.shard_map(device_step, mesh=mesh, in_specs=(seq_spec, seq_spec, P('dp', 'sp'), rep1, rep2, rep2, rep2, rep2, rep1, rep1), out_specs=(seq_spec, seq_spec, vec_spec, row_spec, row_spec, row_spec, row_spec, vec_spec, vec_spec), check_vma=False)
```

```python
import contextlib
import functools
import jax
import jax.numpy as jnp
import numpy as np
from jax import lax
from jax.experimental import pallas as pl
from jax.experimental.pallas import tpu as pltpu
from jax.sharding import PartitionSpec as P

HEAD = 128
NORM_EPS = 1e-5
ROPE_BASE = 10000.0
LOG2E = 1.4426950408889634
f32 = jnp.float32
bf16 = jnp.bfloat16
MESH = pl.DeviceIdType.MESH
NN = (((1,), (0,)), ((), ()))
NT = (((1,), (1,)), ((), ()))
TN = (((0,), (0,)), ((), ()))
PROF = 0
scope = jax.named_scope if PROF else (lambda name: contextlib.nullcontext())


def dotf(a, b, dims):
    return lax.dot_general(a, b, dims, preferred_element_type=f32)


def remote(src, dst, ss, rs, to):
    return pltpu.make_async_remote_copy(src_ref=src, dst_ref=dst, send_sem=ss, recv_sem=rs, device_id={'sp': to}, device_id_type=MESH)


def ds(i, size):
    return pl.ds(pl.multiple_of(i * size, size), size)


def as_row(col):
    return jnp.broadcast_to(col, (col.shape[0], HEAD)).T[0:1, :]


def loop(lo, hi, body):
    def step(i, carry):
        body(i)
        return carry
    lax.fori_loop(lo, hi, step, 0)


def block_kernel(n, x_hbm, gy_hbm, pos_ref, g_ref, fr_ref, wq_ref, wk_ref, wv_ref, wo_ref,
                 y_out, gx_out, gn_ref, dwq_out, dwk_out, dwv_out, dwo_out, gg_ref, h_all, gy_all,
                 x_ref, gy_ref, hid, wh, woh, raw, xbuf, wtile, tile, wrow, qkl, hatT, csT, q_s, k_s, v_s, do_s, o_s, lse, dl,
                 dq_s, dkv, tq, tkv, att, dt, bv, rawT, y_s, dwo_s, gx_s, dh, ssq, cl_s, sl_s, inv, mine, sall, mine2, mall, gpart, gall,
                 s_ring, r_ring, s_par, r_par, s_own, r_own, s_st, r_st, s_o, r_o, s_kv, r_kv, s_q, r_q, s_v, r_v, s_a, r_a, s_b, r_b, s_m, r_m, s_g, r_g,
                 s_ld, s_t, s_w, s_x, s_loc, s_out):
    me = lax.axis_index('sp')
    t_loc, d = x_hbm.shape
    t_all = t_loc * n
    z = me // 2
    c = lax.rem(me, 2)
    nz = n // 2
    mate = me + 1 - 2 * c
    up = lax.rem(z + 1, nz) * 2 + c
    down = lax.rem(z + nz - 1, nz) * 2 + c
    nd = d // HEAD
    half = HEAD // 2
    sub = t_loc // 4
    last = nz - 2
    ticks = 2 * (nz - 1)
    blk = 2 * t_loc
    nb = t_all // blk
    cexp = HEAD ** -0.5 * LOG2E
    scale = HEAD ** -0.5
    cw = tile.shape[2]
    nt = d // cw
    wr = wrow.shape[2]
    nw = d // wr
    cols = ds(me, HEAD)
    far = sorted(range(1, n), key=lambda e: -min(e, n - e))
    early = far[:2]
    alls = (h_all, gy_all)
    own_src = (hid, gy_ref)

    def peer(e):
        return lax.rem(me + e, n)

    def rows(i):
        return ds(i, t_loc)

    def hs(i):
        return ds(i, HEAD)

    def chip(s):
        k = nz // 2 - (s + 1) // 2
        return lax.rem(z + nz + jnp.where(lax.rem(s, 2) == 0, -k, k), nz)

    def piece(core, direction, s, u):
        bz = lax.rem(z + nz - 1 - s, nz) if direction == 0 else lax.rem(z + 1 + s, nz)
        return ds((bz * 2 + core) * 4 + 2 * direction + u, sub)

    def ring(a, direction, s, u):
        ref = alls[a]
        bz = lax.rem(z + nz - s, nz) if direction == 0 else lax.rem(z + s, nz)
        rs = ds((bz * 2 + c) * 4 + 2 * direction + u, sub)
        return remote(ref.at[rs, :], ref.at[rs, :], s_ring.at[a, direction, s, u], r_ring.at[a, direction, s, u], up if direction == 0 else down)

    def ring0(a, direction, u):
        rs = ds(me * 4 + 2 * direction + u, sub)
        return remote(own_src[a].at[pl.ds((2 * direction + u) * sub, sub), :], alls[a].at[rs, :], s_ring.at[a, direction, 0, u], r_ring.at[a, direction, 0, u], up if direction == 0 else down)

    def par(a, direction, s, u):
        rs = piece(c, direction, s, u)
        return remote(alls[a].at[rs, :], alls[a].at[rs, :], s_par.at[a, direction, s, u], r_par.at[a, direction, s, u], mate)

    def own_par(a):
        return remote(own_src[a], alls[a].at[rows(me), :], s_own.at[a], r_own.at[a], mate)

    def own_loc(a):
        return pltpu.make_async_copy(own_src[a], alls[a].at[rows(me), :], s_loc.at[a])

    def comm(a, t):
        s = t // 2
        u = lax.rem(t, 2)
        for direction in range(2):
            ring(a, direction, s, u).wait_recv()

            @pl.when(s < last)
            def _():
                ring(a, direction, s + 1, u).start()
            par(a, direction, s, u).start()

    def loads(a, t):
        s = t // 2
        u = lax.rem(t, 2)
        slot = lax.rem(t, 2)
        out = []
        for i, (core, direction) in enumerate(((c, 0), (c, 1), (1 - c, 0), (1 - c, 1))):
            out.append(pltpu.make_async_copy(alls[a].at[piece(core, direction, s, u), :], xbuf.at[slot, pl.ds(i * sub, sub), :], s_ld.at[slot, i]))
        return out

    def mate_load(a):
        return pltpu.make_async_copy(alls[a].at[rows(mate), :], xbuf.at[1], s_ld.at[1, 0])

    def spots(t):
        s = t // 2
        u = lax.rem(t, 2)
        return [piece(c, 0, s, u), piece(c, 1, s, u), piece(1 - c, 0, s, u), piece(1 - c, 1, s, u)]

    def gather(a, t, work, put):
        @pl.when(t < ticks)
        def _():
            with scope('comm'):
                comm(a, t)

        @pl.when(t == 0)
        def _():
            own_par(a).wait_recv()
            mate_load(a).start()
            put(work(own_src[a][...]), [rows(me)])

        @pl.when(t == 1)
        def _():
            mate_load(a).wait()
            put(work(xbuf[1]), [rows(mate)])

        @pl.when(t >= 2)
        def _():
            for cp in loads(a, t - 2):
                cp.wait()
            put(work(xbuf[lax.rem(t, 2)]), spots(t - 2))

        @pl.when((t >= 1) & (t < ticks + 1))
        def _():
            for direction in range(2):
                par(a, direction, (t - 1) // 2, lax.rem(t - 1, 2)).wait_recv()
            for cp in loads(a, t - 1):
                cp.start()

    def stat_tile(i, act):
        slot = lax.rem(i, 2)
        cs = ds(lax.rem(i, nt), cw)

        @pl.when(i < nt)
        def _():
            act(pltpu.make_async_copy(wq_ref.at[:, cs], wtile.at[slot], s_w.at[slot]))

        @pl.when(i >= nt)
        def _():
            act(pltpu.make_async_copy(wk_ref.at[:, cs], wtile.at[slot], s_w.at[slot]))

    def start(cp):
        cp.start()

    def wait(cp):
        cp.wait()

    def stat_step(i):
        stat_tile(i, wait)

        @pl.when(i + 1 < 2 * nt)
        def _():
            stat_tile(i + 1, start)
        r = dotf(hid[...], wtile[lax.rem(i, 2)], NN)
        w = i // nt
        qkl[w, :, ds(lax.rem(i, nt), cw)] = r
        acc = r[:, :HEAD] * r[:, :HEAD]
        for j in range(1, cw // HEAD):
            acc = acc + r[:, j * HEAD:(j + 1) * HEAD] * r[:, j * HEAD:(j + 1) * HEAD]
        ssq[w] = ssq[w] + acc

    def st_send(e):
        return remote(mine, sall.at[me], s_st.at[e], r_st.at[e], peer(e))

    sgn = jnp.where(lax.broadcasted_iota(jnp.int32, (1, HEAD), 1) < half, -1.0, 1.0).astype(f32)

    def stat_done():
        for w in range(2):
            iv = lax.rsqrt(jnp.sum(ssq[w], axis=1, keepdims=True) * (1.0 / d) + NORM_EPS)
            inv[w] = jnp.broadcast_to(iv, (t_loc, HEAD))
            mine[w:w + 1, :] = as_row(iv)
        mine[2:3, :] = pos_ref[...].astype(f32)
        for e in range(1, n):
            st_send(e).start()
        sall[me] = mine[...]
        ang = spread_col(pos_ref[...].astype(f32)) * fr_ref[0:1, :]
        cl_s[...] = jnp.cos(ang)
        sl_s[...] = jnp.sin(ang) * (-sgn)

    def spread_col(row):
        return jnp.broadcast_to(row, (HEAD, row.shape[1])).T

    def head_w(i):
        w = (wq_ref, wk_ref, wv_ref)[i]
        return pltpu.make_async_copy(w.at[:, cols], wh.at[:, pl.ds(i * HEAD, HEAD)], s_x.at[i])

    def wo_load():
        return pltpu.make_async_copy(wo_ref.at[cols, :], woh, s_x.at[3])

    with scope('begin'):
        barrier = pltpu.get_barrier_semaphore()
        for e in range(1, n):
            pl.semaphore_signal(barrier, inc=1, device_id={'sp': peer(e)}, device_id_type=MESH)
        first = [pltpu.make_async_copy(x_hbm, x_ref, s_x.at[4]), pltpu.make_async_copy(gy_hbm, gy_ref, s_x.at[5])]
        for cp in first:
            cp.start()
        for i in range(3):
            head_w(i).start()
        wo_load().start()
        stat_tile(0, start)
        first[0].wait()
        zero = jnp.zeros((t_loc, HEAD), f32)

        def sq_step(i, acc):
            xf = x_ref[:, hs(i)].astype(f32)
            return acc + xf * xf

        x_inv = lax.rsqrt(jnp.sum(lax.fori_loop(0, nd, sq_step, zero), axis=1, keepdims=True) * (1.0 / d) + NORM_EPS)

        def hid_step(i):
            hid[:, hs(i)] = (x_ref[:, hs(i)].astype(f32) * x_inv * g_ref[2:3, hs(i)]).astype(bf16)

        loop(0, nd, hid_step)
        mine[...] = jnp.zeros_like(mine)
        mine2[...] = jnp.zeros_like(mine2)
        ssq[...] = jnp.zeros_like(ssq)
        first[1].wait()
        own_loc(1).start()
        pl.semaphore_wait(barrier, n - 1)
    for u in range(2):
        for direction in range(2):
            ring0(0, direction, u).start()
    own_par(0).start()
    own_par(1).start()
    own_loc(0).start()
    for i in range(3):
        head_w(i).wait()
    wo_load().wait()

    def qkv_work(xv):
        return dotf(xv, wh[...], NN)

    def qkv_put(r, where):
        step = r.shape[0] // len(where)
        for i, rs in enumerate(where):
            for w in range(3):
                raw[w, rs, :] = r[i * step:(i + 1) * step, w * HEAD:(w + 1) * HEAD]

    spt = 2 * nt // 4

    def x_tick(t):
        gather(0, t, qkv_work, qkv_put)

        @pl.when(t == 2 * last - 1)
        def _():
            for u in range(2):
                for direction in range(2):
                    ring0(1, direction, u).start()

        @pl.when(t < 4)
        def _():
            with scope('stat'):
                loop(t * spt, (t + 1) * spt, stat_step)

        @pl.when(t == 4)
        def _():
            with scope('statdone'):
                stat_done()

    with scope('gather_x'):
        loop(0, ticks + 2, x_tick)
        for e in range(1, n):
            st_send(e).wait()

    def finish(j):
        rs = rows(j)
        st = sall[j]
        ang = spread_col(st[2:3, :]) * fr_ref[0:1, :]
        co = jnp.cos(ang)
        si = jnp.sin(ang)
        csT[0, :, rs] = co.T[:half, :]
        csT[1, :, rs] = si.T[:half, :]
        si = si * sgn
        for w, dst in enumerate((q_s, k_s)):
            hat = raw[w, rs, :] * spread_col(st[w:w + 1, :])
            hatT[w, :, rs] = hat.T
            hat = hat * g_ref[w:w + 1, cols]
            dst[rs, :] = (hat * co + pltpu.roll(hat, half, 1) * si).astype(bf16)
        v_s[rs, :] = raw[2, rs, :].astype(bf16)

    def attend(j):
        qs = ds(j, blk)
        q = q_s[qs, :]

        def unit(kb, carry, masked):
            m, l, acc = carry
            ks = ds(kb, blk)
            s = dotf(q, k_s[ks, :], NT)
            if masked:
                r = lax.broadcasted_iota(jnp.int32, (blk, blk), 0)
                cc = lax.broadcasted_iota(jnp.int32, (blk, blk), 1)
                s = jnp.where(r >= cc, s, -1e30)
            mn = jnp.maximum(m, jnp.max(s, axis=1, keepdims=True))
            al = jnp.exp2((m - mn) * cexp)
            p = jnp.exp2((s - mn) * cexp)
            l = l * al + jnp.sum(p, axis=1, keepdims=True)
            acc = acc * al + dotf(p.astype(bf16), v_s[ks, :], NN)
            return mn, l, acc

        init = (jnp.full((blk, 1), -1e30, f32), jnp.zeros((blk, 1), f32), jnp.zeros((blk, HEAD), f32))
        carry = lax.fori_loop(0, j, functools.partial(unit, masked=False), init)
        m, l, acc = unit(j, carry, True)
        o = acc / l
        raw[2, qs, :] = o
        o_s[qs, :] = o.astype(bf16)
        lse[0:1, qs] = as_row(m * cexp + jnp.log2(l))

    def o_send(e):
        to = peer(e)
        return remote(o_s.at[rows(to), :], att.at[:, cols], s_o.at[e], r_o.at[e], to)

    def do_work(xv):
        return dotf(xv, woh[...], NT).astype(bf16)

    def do_put(r, where):
        step = r.shape[0] // len(where)
        for i, rs in enumerate(where):
            do_s[rs, :] = r[i * step:(i + 1) * step]

    fpt = n // 4

    def y_tick(t):
        gather(1, t, do_work, do_put)

        @pl.when(t < 4)
        def _():
            with scope('finish'):
                loop(t * fpt, (t + 1) * fpt, finish)

        @pl.when((t >= 4) & (t < 4 + nb))
        def _():
            with scope('attend'):
                attend(t - 4)

        @pl.when(t == 4 + nb)
        def _():
            for e in far:
                o_send(e).start()

    with scope('gather_y'):
        loop(0, ticks + 2, y_tick)

    def gy_copy(t):
        return pltpu.make_async_copy(gy_all.at[:, ds(t, cw)], tile.at[lax.rem(t, 2)], s_t.at[lax.rem(t, 2)])

    def h_copy(t):
        return pltpu.make_async_copy(h_all.at[:, ds(lax.rem(t, nt), cw)], tile.at[lax.rem(t, 2)], s_t.at[lax.rem(t, 2)])

    def h2_copy(t):
        return pltpu.make_async_copy(h_all.at[:, ds(chip(t), cw)], tile.at[lax.rem(t, 2)], s_t.at[lax.rem(t, 2)])

    def wo_copy(t):
        return pltpu.make_async_copy(wo_ref.at[:, ds(t, cw)], wtile.at[lax.rem(t, 2)], s_w.at[lax.rem(t, 2)])

    def q_send(e):
        to = peer(e)
        return remote(dq_s.at[rows(to), :], tq.at[:, cols], s_q.at[e], r_q.at[e], to)

    def kv_send(to):
        e = lax.rem(to + n - me, n)
        return remote(dkv.at[to], tkv.at[:, :, cols], s_kv.at[e], r_kv.at[e], to)

    own_loc(0).wait()
    own_loc(1).wait()
    gy_copy(0).start()
    wo_copy(0).start()
    att[:, cols] = o_s[rows(me), :]
    raw[0] = jnp.zeros((t_all, HEAD), f32)

    def delta(j):
        qs = ds(j, blk)
        dl[0:1, qs] = as_row(jnp.sum(raw[2, qs, :] * do_s[qs, :].astype(f32), axis=1, keepdims=True))

    with scope('delta'):
        loop(0, nb, delta)

    def bwd_step(s):
        kb = chip(s)
        ks = ds(kb, blk)
        k = k_s[ks, :]
        v = v_s[ks, :]

        def unit(qb, carry, masked):
            dk, dv = carry
            qs = ds(qb, blk)
            q = q_s[qs, :]
            do = do_s[qs, :]
            p = jnp.exp2(dotf(k, q, NT) * cexp - lse[0:1, qs])
            if masked:
                r = lax.broadcasted_iota(jnp.int32, (blk, blk), 0)
                cc = lax.broadcasted_iota(jnp.int32, (blk, blk), 1)
                p = jnp.where(cc >= r, p, 0.0)
            g = (p * (dotf(v, do, NT) - dl[0:1, qs])).astype(bf16)
            dv = dv + dotf(p.astype(bf16), do, NN)
            dk = dk + dotf(g, q, NN)
            raw[0, qs, :] = raw[0, qs, :] + dotf(g, k, TN)
            return dk, dv

        zk = jnp.zeros((blk, HEAD), f32)
        carry = unit(kb, (zk, zk), True)
        dk, dv = lax.fori_loop(kb + 1, nb, functools.partial(unit, masked=False), carry)
        dk = (dk * scale).astype(bf16)
        dv = dv.astype(bf16)
        for u in range(2):
            dkv[2 * kb + u, 0] = dk[u * t_loc:(u + 1) * t_loc]
            dkv[2 * kb + u, 1] = dv[u * t_loc:(u + 1) * t_loc]

        @pl.when(kb != z)
        def _():
            for u in range(2):
                kv_send(2 * kb + u).start()

        @pl.when(kb == z)
        def _():
            kv_send(mate).start()

    with scope('bwd'):
        loop(0, nb, bwd_step)
        dq_s[...] = (raw[0] * scale).astype(bf16)
    for e in far:
        q_send(e).start()
    tq[:, cols] = dq_s[rows(me), :]
    tkv[:, :, cols] = dkv[me]

    def flip_o(i):
        dt[:, rows(i)] = o_s[rows(i), :].T

    def flip_v(i):
        dt[:, rows(i)] = dkv[i, 1].T

    def dwo_step(t):
        gy_copy(t).wait()

        @pl.when(t + 1 < nt)
        def _():
            gy_copy(t + 1).start()

        @pl.when(t + 1 == nt)
        def _():
            h_copy(t + 1).start()
        dwo_s[:, ds(t, cw)] = dotf(dt[...], tile[lax.rem(t, 2)], NN)

    def dwv_step(t):
        h_copy(t).wait()

        @pl.when(t + 1 < 2 * nt)
        def _():
            h_copy(t + 1).start()

        @pl.when(t + 1 == 2 * nt)
        def _():
            h2_copy(0).start()
        r = dotf(dt[...], tile[lax.rem(t, 2)], NN)
        for u in range(cw // HEAD):
            bv[(t - nt) * (cw // HEAD) + u] = r[:, u * HEAD:(u + 1) * HEAD].T

    def y_step(t):
        wo_copy(t).wait()

        @pl.when(t + 1 < nt)
        def _():
            wo_copy(t + 1).start()
        cs = ds(t, cw)
        y_s[:, cs] = (x_ref[:, cs].astype(f32) + dotf(att[...], wtile[lax.rem(t, 2)], NN)).astype(bf16)

    def v_send(e):
        to = peer(e)
        return remote(bv.at[to], dwv_out.at[:, cols], s_v.at[e], r_v.at[e], to)

    def out(i):
        src, dst = ((y_s, y_out), (dwo_s, dwo_out), (gx_s, gx_out), (bv.at[me], dwv_out.at[:, cols]),
                    (raw.at[1, rows_f(0, me), :], dwq_out.at[:, cols]), (raw.at[1, rows_f(1, me), :], dwk_out.at[:, cols]))[i]
        return pltpu.make_async_copy(src, dst, s_out.at[i])

    def rows_f(w, to):
        return ds(w * n + to, HEAD)

    with scope('dwo'):
        loop(0, n, flip_o)
        loop(0, nt, dwo_step)
        out(1).start()
    with scope('dwv'):
        loop(0, n, flip_v)
        loop(nt, 2 * nt, dwv_step)
        out(3).start()
    for e in early:
        v_send(e).start()
    with scope('y'):
        for e in range(1, n):
            o_send(e).wait()
        loop(0, nt, y_step)
        out(0).start()

    def w_copies(t):
        slot = lax.rem(t, 2)
        return [pltpu.make_async_copy(w.at[ds(t, wr), :], wrow.at[slot, i], s_x.at[4 + 3 * slot + i]) for i, w in enumerate((wq_ref, wk_ref, wv_ref))]

    for cp in w_copies(0):
        cp.start()
    with scope('waitkv'):
        for e in range(1, n):
            kv_send(peer(e)).wait()
    with scope('waitq'):
        for e in range(1, n):
            q_send(e).wait()

    cl = cl_s[...]
    sl = sl_s[...]

    def back_rope(a):
        a = a.astype(f32)
        return a * cl + pltpu.roll(a, half, 1) * sl

    def mean_step(i, carry):
        a, b = carry
        a = a + back_rope(tq[:, hs(i)]) * g_ref[0:1, hs(i)] * qkl[0, :, hs(i)]
        b = b + back_rope(tkv[0, :, hs(i)]) * g_ref[1:2, hs(i)] * qkl[1, :, hs(i)]
        return a, b

    def m_send(e):
        return remote(mine2, mall.at[me], s_m.at[e], r_m.at[e], peer(e))

    with scope('mean'):
        a, b = lax.fori_loop(0, nd, mean_step, (zero, zero))
        mq = jnp.sum(a, axis=1, keepdims=True) * inv[0] * (1.0 / d)
        mk = jnp.sum(b, axis=1, keepdims=True) * inv[1] * (1.0 / d)
        mine2[0:1, :] = mq.T[0:1, :]
        mine2[1:2, :] = mk.T[0:1, :]
    for e in range(1, n):
        m_send(e).start()
    for e in far:
        if e not in early:
            v_send(e).start()
    mall[me] = mine2[...]

    def loc_step(i):
        tq[:, hs(i)] = (inv[0] * (back_rope(tq[:, hs(i)]) * g_ref[0:1, hs(i)] - qkl[0, :, hs(i)] * inv[0] * mq)).astype(bf16)
        tkv[0, :, hs(i)] = (inv[1] * (back_rope(tkv[0, :, hs(i)]) * g_ref[1:2, hs(i)] - qkl[1, :, hs(i)] * inv[1] * mk)).astype(bf16)

    with scope('mwait'):
        for e in range(1, n):
            m_send(e).wait()

    gcol = [g_ref[w:w + 1, cols] for w in range(2)]
    gcol = [spread_col(g)[:, 0:1] for g in gcol]

    def head_step(j, carry):
        js = rows(j)
        ct = csT[0, :, js]
        sn = csT[1, :, js]
        res = []
        for w, src in enumerate((dq_s[js, :], dkv[j, 0])):
            t = src.astype(f32).T
            p, r = t[:half], t[half:]
            t = jnp.concatenate([p * ct + r * sn, r * ct - p * sn], axis=0)
            hat = hatT[w, :, js]
            res.append(carry[w] + t * hat)
            rawT[w * HEAD:(w + 1) * HEAD, js] = (sall[j, w:w + 1, :] * (t * gcol[w] - hat * mall[j, w:w + 1, :])).astype(bf16)
        return tuple(res)

    with scope('head'):
        zt = jnp.zeros((HEAD, t_loc), f32)
        sums = lax.fori_loop(0, n, head_step, (zt, zt))
        for w in range(2):
            gg_ref[w] = jnp.broadcast_to(jnp.sum(sums[w], axis=1, keepdims=True), (HEAD, HEAD)).T[0:8, :]

    def a_send(to):
        e = lax.rem(to + n - me, n)
        return remote(raw.at[1, rows_f(0, to), :], dwq_out.at[:, cols], s_a.at[e], r_a.at[e], to)

    def b_send(to):
        e = lax.rem(to + n - me, n)
        return remote(raw.at[1, rows_f(1, to), :], dwk_out.at[:, cols], s_b.at[e], r_b.at[e], to)

    def dw_step(t):
        h2_copy(t).wait()

        @pl.when(t + 1 < nt)
        def _():
            h2_copy(t + 1).start()
        nn = chip(t)
        r = dotf(rawT[...], tile[lax.rem(t, 2)], NN)
        for u in range(cw // HEAD):
            to = nn * (cw // HEAD) + u
            for w in range(2):
                raw[1, rows_f(w, to), :] = r[w * HEAD:(w + 1) * HEAD, u * HEAD:(u + 1) * HEAD].T

            @pl.when(to != me)
            def _():
                a_send(to).start()
                b_send(to).start()

    with scope('dw'):
        loop(0, nt, dw_step)
    out(4).start()
    out(5).start()
    with scope('loc'):
        loop(0, nd, loc_step)

    def dh_step(t):
        for cp in w_copies(t):
            cp.wait()

        @pl.when(t + 1 < nw)
        def _():
            for cp in w_copies(t + 1):
                cp.start()
        slot = lax.rem(t, 2)
        r = dotf(tq[...], wrow[slot, 0], NT) + dotf(tkv[0], wrow[slot, 1], NT) + dotf(tkv[1], wrow[slot, 2], NT)
        dh[:, ds(t, wr)] = r.astype(bf16).astype(f32)

    with scope('dh'):
        loop(0, nw, dh_step)

    def mx_step(i, acc):
        return acc + dh[:, hs(i)] * g_ref[2:3, hs(i)] * x_ref[:, hs(i)].astype(f32)

    def g_send(e):
        return remote(gpart.at[peer(e)], gall.at[me], s_g.at[e], r_g.at[e], peer(e))

    with scope('gx'):
        mx = jnp.sum(lax.fori_loop(0, nd, mx_step, zero), axis=1, keepdims=True) * x_inv * (1.0 / d)

        def gx_step(i):
            xh = x_ref[:, hs(i)].astype(f32) * x_inv
            dhh = dh[:, hs(i)]
            gpart[i] = jnp.broadcast_to(jnp.sum(dhh * xh, axis=0, keepdims=True), (8, HEAD))
            gx_s[:, hs(i)] = (gy_ref[:, hs(i)].astype(f32) + x_inv * (dhh * g_ref[2:3, hs(i)] - xh * mx)).astype(bf16)

        loop(0, nd, gx_step)
        out(2).start()
    with scope('end_v'):
        for e in range(1, n):
            g_send(e).start()
        gall[me] = gpart[me]
        for e in range(1, n):
            v_send(e).wait()
    with scope('end_g'):
        for e in range(1, n):
            g_send(e).wait()
        gn_ref[...] = jnp.sum(gall[...], axis=0)

        def drain(i):
            s = i // 2
            u = lax.rem(i, 2)
            for a in range(2):
                for direction in range(2):
                    ring(a, direction, s, u).wait_send()
                    par(a, direction, s, u).wait_send()

        loop(0, ticks, drain)
        for a in range(2):
            own_par(a).wait_send()
        for i in range(6):
            out(i).wait()
    with scope('end_ab'):
        for e in range(1, n):
            a_send(peer(e)).wait()
            b_send(peer(e)).wait()


def block(n, x, gy, pos, gains, freq, wq, wk, wv, wo):
    t_loc, d = x.shape
    t_all = t_loc * n
    vm = pl.BlockSpec(memory_space=pltpu.VMEM)
    hb = pl.BlockSpec(memory_space=pl.ANY)
    S = jax.ShapeDtypeStruct
    V = pltpu.VMEM
    sem = pltpu.SemaphoreType.DMA
    hd = (t_all, HEAD)
    tok = (t_loc, d)
    nz = n // 2
    return pl.pallas_call(functools.partial(block_kernel, n),
        in_specs=[hb] * 2 + [vm] * 3 + [hb] * 4,
        out_specs=[hb, hb, vm, hb, hb, hb, hb, vm, hb, hb],
        out_shape=[S(tok, bf16), S(tok, bf16), S((8, d // n), f32)] + [S((d // n, d), f32)] * 4 + [S((2, 8, HEAD), f32), S((t_all, d), bf16), S((t_all, d), bf16)],
        scratch_shapes=[V(tok, bf16), V(tok, bf16), V(tok, bf16), V((d, 3 * HEAD), bf16), V((HEAD, d), bf16), V((3,) + hd, f32), V((2,) + tok, bf16), V((2, d, 2 * HEAD), bf16), V((2, t_all, 2 * HEAD), bf16), V((2, 3, 2 * HEAD, d), bf16),
            V((2,) + tok, f32), V((2, HEAD, t_all), f32), V((2, HEAD // 2, t_all), f32)] + [V(hd, bf16)] * 5 + [V((8, t_all), f32)] * 2
        + [V(hd, bf16), V((n, 2, t_loc, HEAD), bf16), V(tok, bf16), V((2,) + tok, bf16), V(tok, bf16), V((HEAD, t_all), bf16), V((n, d // n, HEAD), f32), V((2 * HEAD, t_all), bf16), V(tok, bf16), V((HEAD, d), f32), V(tok, bf16), V(tok, f32),
            V((2, t_loc, HEAD), f32), V((t_loc, HEAD), f32), V((t_loc, HEAD), f32), V((2, t_loc, HEAD), f32), V((8, t_loc), f32), V((n, 8, t_loc), f32), V((8, t_loc), f32), V((n, 8, t_loc), f32), V((n, 8, d // n), f32), V((n, 8, d // n), f32)]
        + [sem((2, 2, nz - 1, 2))] * 4 + [sem((2,))] * 2 + [sem((n,))] * 18
        + [sem((2, 4)), sem((2,)), sem((2,)), sem((10,)), sem((2,)), sem((6,))],
        compiler_params=pltpu.CompilerParams(collective_id=1, has_side_effects=True, vmem_limit_bytes=67043328), name='block')(x, gy, pos, gains, freq, wq, wk, wv, wo)


def copy_kernel(*refs):
    k = (len(refs) - 1) // 3
    src, dst, buf, si, so = list(refs[:k - 1]), refs[k - 1:2 * k - 1], refs[2 * k - 1:3 * k - 1], refs[-2], refs[-1]
    src[k - 3:] = [src[k - 3].at[0:1, :], src[k - 2].at[0, 0:1, :], src[k - 2].at[1, 0:1, :]]
    ins = [pltpu.make_async_copy(src[i], buf[i], si.at[i]) for i in range(k)]
    outs = [pltpu.make_async_copy(buf[i], dst[i], so.at[i]) for i in range(k)]
    for cp in ins:
        cp.start()
    for i in range(k):
        ins[i].wait()
        outs[i].start()
    for cp in outs:
        cp.wait()


def copy_out(arrays):
    hb = pl.BlockSpec(memory_space=pl.ANY)
    shapes = [(a.shape, a.dtype) for a in arrays[:-2]] + [((1, HEAD), f32)] * 3
    k = len(shapes)
    return pl.pallas_call(copy_kernel, in_specs=[hb] * len(arrays), out_specs=[hb] * k, out_shape=[jax.ShapeDtypeStruct(*a) for a in shapes],
        scratch_shapes=[pltpu.VMEM(*a) for a in shapes] + [pltpu.SemaphoreType.DMA((k,))] * 2, name='copy_out')(*arrays)


def solution(mesh):
    n = mesh.shape['sp']

    def device_step(x_in, grad_y, positions, g_norm, wq, wk, wv, wo, gq, gk):
        gains = jnp.concatenate([gq, gk, g_norm]).astype(f32).reshape(3, -1)
        half = HEAD // 2
        inv_freq = ROPE_BASE ** (-np.arange(half) * (2.0 / HEAD))
        freq = jnp.asarray(np.tile(inv_freq, (8, 2)), f32)
        y, gx, gn, dwq, dwk, dwv, dwo, gg, _, _ = block(n, x_in[0], grad_y[0], positions, gains, freq, wq, wk, wv, wo)
        y, gx, dwq, dwk, dwv, dwo, gn, ggq, ggk = copy_out([y, gx, dwq, dwk, dwv, dwo, gn, gg])
        return (y[None], gx[None], gn[0], dwq, dwk, dwv, dwo, ggq[0], ggk[0])

    seq_spec = P('dp', 'sp', None)
    rep2, rep1 = P(None, None), P(None)
    row_spec, vec_spec = P(('dp', 'sp'), None), P(('dp', 'sp'))
    return jax.shard_map(device_step, mesh=mesh, in_specs=(seq_spec, seq_spec, P('dp', 'sp'), rep1, rep2, rep2, rep2, rep2, rep1, rep1), out_specs=(seq_spec, seq_spec, vec_spec, row_spec, row_spec, row_spec, row_spec, vec_spec, vec_spec), check_vma=False)
```

```python
import contextlib
import functools
import jax
import jax.numpy as jnp
import numpy as np
from jax import lax
from jax.experimental import pallas as pl
from jax.experimental.pallas import tpu as pltpu
from jax.sharding import PartitionSpec as P

HEAD = 128
NORM_EPS = 1e-5
ROPE_BASE = 10000.0
LOG2E = 1.4426950408889634
f32 = jnp.float32
bf16 = jnp.bfloat16
MESH = pl.DeviceIdType.MESH
NN = (((1,), (0,)), ((), ()))
NT = (((1,), (1,)), ((), ()))
TN = (((0,), (0,)), ((), ()))
PROF = 0
scope = jax.named_scope if PROF else (lambda name: contextlib.nullcontext())


def dotf(a, b, dims):
    return lax.dot_general(a, b, dims, preferred_element_type=f32)


def remote(src, dst, ss, rs, to):
    return pltpu.make_async_remote_copy(src_ref=src, dst_ref=dst, send_sem=ss, recv_sem=rs, device_id={'sp': to}, device_id_type=MESH)


def ds(i, size):
    return pl.ds(pl.multiple_of(i * size, size), size)


def settle(ref, *sems):
    for sem in sems:
        pltpu.make_async_copy(ref, ref, sem).wait()


def as_row(col):
    return jnp.broadcast_to(col, (col.shape[0], HEAD)).T[0:1, :]


def loop(lo, hi, body):
    def step(i, carry):
        body(i)
        return carry
    lax.fori_loop(lo, hi, step, 0)


def block_kernel(n, x_hbm, gy_hbm, pos_ref, gq_ref, gk_ref, gn1_ref, fr_ref, wq_ref, wk_ref, wv_ref, wo_ref,
                 y_out, gx_out, gall, dwq_out, dwk_out, dwv_out, dwo_out, gg_out, h_all, gy_all,
                 x_ref, gy_ref, g_ref, hid, wh, woh, raw, xbuf, wtile, tile, wrow, qkl, hatT, csT, q_s, k_s, v_s, do_s, o_s, lse, dl,
                 dq_s, dkv, tq, tkv, att, dt, bv, rawT, y_s, dwo_s, gx_s, dh, ssq, cl_s, sl_s, inv, xinv, mine, sall, mine2, mall, pm, pall, gpart, gg_s,
                 s_ring, r_ring, s_par, r_par, r_own, s_st, r_st, s_o, r_o, s_kv, r_kv, s_q, r_q, s_v, r_v, s_a, r_a, s_b, r_b, s_m, r_m, s_g, r_g, s_p, r_p,
                 s_ld, s_t, s_w, s_x, s_wr, s_loc, s_out):
    me = lax.axis_index('sp')
    t_loc, d = x_hbm.shape
    t_all = t_loc * n
    z = me // 2
    c = lax.rem(me, 2)
    nz = n // 2
    mate = me + 1 - 2 * c
    up = lax.rem(z + 1, nz) * 2 + c
    down = lax.rem(z + nz - 1, nz) * 2 + c
    nd = d // HEAD
    half = HEAD // 2
    sub = t_loc // 4
    last = nz - 2
    ticks = 2 * (nz - 1)
    blk = 2 * t_loc
    nb = t_all // blk
    cexp = HEAD ** -0.5 * LOG2E
    scale = HEAD ** -0.5
    cw = tile.shape[2]
    nt = d // cw
    wr = wrow.shape[2]
    nw = d // wr
    cols = ds(me, HEAD)
    far = sorted(range(1, n), key=lambda e: -min(e, n - e))
    alls = (h_all, gy_all)
    own_src = (hid, gy_ref)

    def peer(e):
        return lax.rem(me + e, n)

    def rows(i):
        return ds(i, t_loc)

    def hs(i):
        return ds(i, HEAD)

    def chip(s):
        k = nz // 2 - (s + 1) // 2
        return lax.rem(z + nz + jnp.where(lax.rem(s, 2) == 0, -k, k), nz)

    def piece(core, direction, s, u):
        bz = lax.rem(z + nz - 1 - s, nz) if direction == 0 else lax.rem(z + 1 + s, nz)
        return ds((bz * 2 + core) * 4 + 2 * direction + u, sub)

    def ring(a, direction, s, u):
        ref = alls[a]
        bz = lax.rem(z + nz - s, nz) if direction == 0 else lax.rem(z + s, nz)
        rs = ds((bz * 2 + c) * 4 + 2 * direction + u, sub)
        return remote(ref.at[rs, :], ref.at[rs, :], s_ring.at[a], r_ring.at[a, direction, s, u], up if direction == 0 else down)

    def ring0(a, direction, u):
        rs = ds(me * 4 + 2 * direction + u, sub)
        return remote(own_src[a].at[pl.ds((2 * direction + u) * sub, sub), :], alls[a].at[rs, :], s_ring.at[a], r_ring.at[a, direction, 0, u], up if direction == 0 else down)

    def par(a, direction, s, u):
        rs = piece(c, direction, s, u)
        return remote(alls[a].at[rs, :], alls[a].at[rs, :], s_par.at[a], r_par.at[a, 2 * s + u], mate)

    def own_par(a):
        return remote(own_src[a], alls[a].at[rows(me), :], s_par.at[a], r_own.at[a], mate)

    def own_loc(a):
        return pltpu.make_async_copy(own_src[a], alls[a].at[rows(me), :], s_loc.at[0])

    def comm(a, t):
        s = t // 2
        u = lax.rem(t, 2)
        for direction in range(2):
            ring(a, direction, s, u).wait_recv()

            @pl.when(s < last)
            def _():
                ring(a, direction, s + 1, u).start()
            par(a, direction, s, u).start()

    def loads(a, t):
        s = t // 2
        u = lax.rem(t, 2)
        slot = lax.rem(t, 2)
        out = []
        for i, (core, direction) in enumerate(((c, 0), (c, 1), (1 - c, 0), (1 - c, 1))):
            out.append(pltpu.make_async_copy(alls[a].at[piece(core, direction, s, u), :], xbuf.at[slot, pl.ds(i * sub, sub), :], s_ld.at[slot]))
        return out

    def mate_load(a):
        return pltpu.make_async_copy(alls[a].at[rows(mate), :], xbuf.at[1], s_ld.at[1])

    def spots(t):
        s = t // 2
        u = lax.rem(t, 2)
        return [piece(c, 0, s, u), piece(c, 1, s, u), piece(1 - c, 0, s, u), piece(1 - c, 1, s, u)]

    def gather(a, t, work, put):
        @pl.when(t < ticks)
        def _():
            with scope('comm'):
                comm(a, t)

        @pl.when(t == 0)
        def _():
            own_par(a).wait_recv()
            mate_load(a).start()
            put(work(own_src[a][...]), [rows(me)])

        @pl.when(t == 1)
        def _():
            mate_load(a).wait()
            put(work(xbuf[1]), [rows(mate)])

        @pl.when(t >= 2)
        def _():
            settle(xbuf.at[lax.rem(t, 2)], s_ld.at[lax.rem(t, 2)])
            put(work(xbuf[lax.rem(t, 2)]), spots(t - 2))

        @pl.when((t >= 1) & (t < ticks + 1))
        def _():
            settle(alls[a].at[pl.ds(0, 2 * sub), :], r_par.at[a, t - 1])
            for cp in loads(a, t - 1):
                cp.start()

    def stat_tile(i, act):
        slot = lax.rem(i, 2)
        cs = ds(lax.rem(i, nt), cw)

        @pl.when(i < nt)
        def _():
            act(pltpu.make_async_copy(wq_ref.at[:, cs], wtile.at[slot], s_w.at[slot]))

        @pl.when(i >= nt)
        def _():
            act(pltpu.make_async_copy(wk_ref.at[:, cs], wtile.at[slot], s_w.at[slot]))

    def start(cp):
        cp.start()

    def wait(cp):
        cp.wait()

    def stat_step(i):
        stat_tile(i, wait)

        @pl.when(i + 1 < 2 * nt)
        def _():
            stat_tile(i + 1, start)
        r = dotf(hid[...], wtile[lax.rem(i, 2)], NN)
        w = i // nt
        qkl[w, :, ds(lax.rem(i, nt), cw)] = r
        acc = r[:, :HEAD] * r[:, :HEAD]
        for j in range(1, cw // HEAD):
            acc = acc + r[:, j * HEAD:(j + 1) * HEAD] * r[:, j * HEAD:(j + 1) * HEAD]
        ssq[w] = ssq[w] + acc

    def st_send(e):
        return remote(mine.at[pl.ds(0, 3)], sall.at[me, pl.ds(0, 3)], s_st.at[0], r_st.at[0], peer(e))

    sgn = jnp.where(lax.broadcasted_iota(jnp.int32, (1, HEAD), 1) < half, -1.0, 1.0).astype(f32)

    def stat_done():
        for w in range(2):
            iv = lax.rsqrt(jnp.sum(ssq[w], axis=1, keepdims=True) * (1.0 / d) + NORM_EPS)
            inv[w] = jnp.broadcast_to(iv, (t_loc, HEAD))
            mine[w:w + 1, :] = as_row(iv)
        mine[2:3, :] = pos_ref[...].astype(f32)
        for e in range(1, n):
            st_send(e).start()
        sall[me, 0:3, :] = mine[0:3, :]
        ang = spread_col(pos_ref[...].astype(f32)) * fr_ref[0:1, :]
        cl_s[...] = jnp.cos(ang)
        sl_s[...] = jnp.sin(ang) * (-sgn)

    def spread_col(row):
        return jnp.broadcast_to(row, (HEAD, row.shape[1])).T

    def head_w(i):
        w = (wq_ref, wk_ref, wv_ref)[i]
        return pltpu.make_async_copy(w.at[:, cols], wh.at[:, pl.ds(i * HEAD, HEAD)], s_x.at[0])

    def wo_load():
        return pltpu.make_async_copy(wo_ref.at[cols, :], woh, s_x.at[1])

    with scope('begin'):
        barrier = pltpu.get_barrier_semaphore()
        for e in range(1, n):
            pl.semaphore_signal(barrier, inc=1, device_id={'sp': peer(e)}, device_id_type=MESH)
        def x_piece(p):
            rs = pl.ds(p * sub, sub)
            return pltpu.make_async_copy(x_hbm.at[rs, :], x_ref.at[rs, :], s_x.at[2 + p])

        gy_load = pltpu.make_async_copy(gy_hbm, gy_ref, s_x.at[6])
        for p in (0, 2, 1, 3):
            x_piece(p).start()
        gy_load.start()
        for i in range(3):
            head_w(i).start()
        wo_load().start()
        stat_tile(0, start)
        for w, src in enumerate((gq_ref, gk_ref, gn1_ref)):
            g_ref[w:w + 1, :] = src[...].astype(f32).reshape(1, d)
        def norm_piece(p):
            rs = pl.ds(p * sub, sub)
            x_piece(p).wait()

            def sq_step(i, acc):
                xf = x_ref[rs, hs(i)].astype(f32)
                return acc + xf * xf

            acc = lax.fori_loop(0, nd, sq_step, jnp.zeros((sub, HEAD), f32))
            xi = lax.rsqrt(jnp.sum(acc, axis=1, keepdims=True) * (1.0 / d) + NORM_EPS)
            xinv[rs, :] = jnp.broadcast_to(xi, (sub, HEAD))

            def hid_step(i):
                hid[rs, hs(i)] = (x_ref[rs, hs(i)].astype(f32) * xi * g_ref[2:3, hs(i)]).astype(bf16)

            loop(0, nd, hid_step)

        norm_piece(0)
        norm_piece(2)
        pl.semaphore_wait(barrier, n - 1)
        ring0(0, 0, 0).start()
        ring0(0, 1, 0).start()
        norm_piece(1)
        ring0(0, 0, 1).start()
        norm_piece(3)
        ring0(0, 1, 1).start()
        zero = jnp.zeros((t_loc, HEAD), f32)
        ssq[...] = jnp.zeros_like(ssq)
        gy_load.wait()
        own_loc(1).start()
    own_par(0).start()
    own_par(1).start()
    own_loc(0).start()
    settle(wh, s_x.at[0])
    wo_load().wait()

    hb = t_loc // 2

    def finish(s):
        for direction in range(2):
            bz = lax.rem(z + nz - 1 - s, nz) if direction == 0 else lax.rem(z + 1 + s, nz)

            def one(core):
                b = bz * 2 + core
                rs = ds(b * 2 + direction, hb)
                st = sall[b, 0:3, direction * hb:(direction + 1) * hb]
                ang = spread_col(st[2:3, :]) * fr_ref[0:1, :]
                co = jnp.cos(ang)
                si = jnp.sin(ang)
                csT[0, :, rs] = co.T[:half, :]
                csT[1, :, rs] = si.T[:half, :]
                si = si * sgn
                for w, dst in enumerate((q_s, k_s)):
                    hat = raw[w, rs, :] * spread_col(st[w:w + 1, :])
                    hatT[w, :, rs] = hat.T
                    hat = hat * g_ref[w:w + 1, cols]
                    dst[rs, :] = (hat * co + pltpu.roll(hat, half, 1) * si).astype(bf16)
                v_s[rs, :] = raw[2, rs, :].astype(bf16)

            loop(0, 2, one)

    def qkv_work(xv):
        return dotf(xv, wh[...], NN)

    def qkv_put(r, where):
        step = r.shape[0] // len(where)
        for i, rs in enumerate(where):
            for w in range(3):
                raw[w, rs, :] = r[i * step:(i + 1) * step, w * HEAD:(w + 1) * HEAD]

    spt = 2 * nt // 4

    def x_tick(t):
        gather(0, t, qkv_work, qkv_put)

        @pl.when(t == 2 * last - 1)
        def _():
            for u in range(2):
                for direction in range(2):
                    ring0(1, direction, u).start()

        @pl.when(t < 4)
        def _():
            with scope('stat'):
                loop(t * spt, (t + 1) * spt, stat_step)

        @pl.when(t == 4)
        def _():
            with scope('statdone'):
                stat_done()

        @pl.when(t == 6)
        def _():
            settle(sall.at[pl.ds(0, n - 1), pl.ds(0, 3)], s_st.at[0], r_st.at[0])

        @pl.when(((t >= 6) & (t <= 11)) | (t == 13))
        def _():
            with scope('finish'):
                finish(jnp.where(t == 13, last - 1, t - 7))

    with scope('gather_x'):
        loop(0, ticks + 2, x_tick)

    def attend(j):
        qs = ds(j, blk)
        q = q_s[qs, :]

        def unit(kb, carry, masked):
            m, l, acc = carry
            ks = ds(kb, blk)
            s = dotf(q, k_s[ks, :], NT)
            if masked:
                r = lax.broadcasted_iota(jnp.int32, (blk, blk), 0)
                cc = lax.broadcasted_iota(jnp.int32, (blk, blk), 1)
                s = jnp.where(r >= cc, s, -1e30)
            mn = jnp.maximum(m, jnp.max(s, axis=1, keepdims=True))
            al = jnp.exp2((m - mn) * cexp)
            p = jnp.exp2((s - mn) * cexp)
            l = l * al + jnp.sum(p, axis=1, keepdims=True)
            acc = acc * al + dotf(p.astype(bf16), v_s[ks, :], NN)
            return mn, l, acc

        init = (jnp.full((blk, 1), -1e30, f32), jnp.zeros((blk, 1), f32), jnp.zeros((blk, HEAD), f32))
        carry = lax.fori_loop(0, j, functools.partial(unit, masked=False), init)
        m, l, acc = unit(j, carry, True)
        o = acc / l
        raw[2, qs, :] = o
        o_s[qs, :] = o.astype(bf16)
        lse[0:1, qs] = as_row(m * cexp + jnp.log2(l))

    def o_send(e):
        to = peer(e)
        return remote(o_s.at[rows(to), :], att.at[:, cols], s_o.at[0], r_o.at[0], to)

    def do_work(xv):
        return dotf(xv, woh[...], NT).astype(bf16)

    def do_put(r, where):
        step = r.shape[0] // len(where)
        for i, rs in enumerate(where):
            do_s[rs, :] = r[i * step:(i + 1) * step]

    def y_tick(t):
        gather(1, t, do_work, do_put)

        @pl.when(t == 0)
        def _():
            with scope('finish'):
                finish(last)
        lo = jnp.where(t == 0, 0, jnp.where(t <= 4, t + 1, jnp.where(t <= 6, 6, 7)))
        hi = jnp.where(t == 0, 2, jnp.where(t <= 4, t + 2, jnp.where(t == 5, 6, jnp.where(t == 8, 8, 7))))
        with scope('attend'):
            loop(lo, hi, attend)

        @pl.when(t == ticks - 2)
        def _():
            for e in far:
                o_send(e).start()

    with scope('gather_y'):
        loop(0, ticks + 2, y_tick)

    def gy_copy(t):
        return pltpu.make_async_copy(gy_all.at[:, ds(t, cw)], tile.at[lax.rem(t, 2)], s_t.at[lax.rem(t, 2)])

    def h_copy(t):
        return pltpu.make_async_copy(h_all.at[:, ds(lax.rem(t, nt), cw)], tile.at[lax.rem(t, 2)], s_t.at[lax.rem(t, 2)])

    def h2_copy(t):
        return pltpu.make_async_copy(h_all.at[:, ds(chip(t), cw)], tile.at[lax.rem(t, 2)], s_t.at[lax.rem(t, 2)])

    def wo_copy(t):
        return pltpu.make_async_copy(wo_ref.at[:, ds(t, cw)], wtile.at[lax.rem(t, 2)], s_w.at[lax.rem(t, 2)])

    def q_send(e):
        to = peer(e)
        return remote(dq_s.at[rows(to), :], tq.at[:, cols], s_q.at[0], r_q.at[0], to)

    def kv_send(to):
        return remote(dkv.at[to], tkv.at[:, :, cols], s_kv.at[0], r_kv.at[0], to)

    settle(h_all.at[pl.ds(0, 2 * t_loc), :], s_loc.at[0])
    gy_copy(0).start()
    wo_copy(0).start()
    att[:, cols] = o_s[rows(me), :]
    raw[0] = jnp.zeros((t_all, HEAD), f32)

    def delta(j):
        qs = ds(j, blk)
        dl[0:1, qs] = as_row(jnp.sum(raw[2, qs, :] * do_s[qs, :].astype(f32), axis=1, keepdims=True))

    with scope('delta'):
        loop(0, nb, delta)

    def bwd_step(s):
        kb = chip(s)
        ks = ds(kb, blk)
        k = k_s[ks, :]
        v = v_s[ks, :]

        def unit(qb, carry, masked):
            dk, dv = carry
            qs = ds(qb, blk)
            q = q_s[qs, :]
            do = do_s[qs, :]
            p = jnp.exp2(dotf(k, q, NT) * cexp - lse[0:1, qs])
            if masked:
                r = lax.broadcasted_iota(jnp.int32, (blk, blk), 0)
                cc = lax.broadcasted_iota(jnp.int32, (blk, blk), 1)
                p = jnp.where(cc >= r, p, 0.0)
            g = (p * (dotf(v, do, NT) - dl[0:1, qs])).astype(bf16)
            dv = dv + dotf(p.astype(bf16), do, NN)
            dk = dk + dotf(g, q, NN)
            raw[0, qs, :] = raw[0, qs, :] + dotf(g, k, TN)
            return dk, dv

        zk = jnp.zeros((blk, HEAD), f32)
        carry = unit(kb, (zk, zk), True)
        dk, dv = lax.fori_loop(kb + 1, nb, functools.partial(unit, masked=False), carry)
        dk = (dk * scale).astype(bf16)
        dv = dv.astype(bf16)
        for u in range(2):
            dkv[2 * kb + u, 0] = dk[u * t_loc:(u + 1) * t_loc]
            dkv[2 * kb + u, 1] = dv[u * t_loc:(u + 1) * t_loc]

        @pl.when(kb != z)
        def _():
            for u in range(2):
                kv_send(2 * kb + u).start()

        @pl.when(kb == z)
        def _():
            kv_send(mate).start()

    with scope('bwd'):
        loop(0, nb, bwd_step)
        dq_s[...] = (raw[0] * scale).astype(bf16)
    gcol = [spread_col(g_ref[w:w + 1, cols])[:, 0:1] for w in range(2)]

    def unroped(src, js):
        ct = csT[0, :, js]
        sn = csT[1, :, js]
        t = src.astype(f32).T
        p, r = t[:half], t[half:]
        return jnp.concatenate([p * ct + r * sn, r * ct - p * sn], axis=0)

    def share_step(j, carry):
        js = rows(j)
        res = []
        for w, src in enumerate((dq_s[js, :], dkv[j, 0])):
            th = unroped(src, js) * hatT[w, :, js]
            res.append(carry[w] + th)
            pm[j, w:w + 1, :] = jnp.sum(th * gcol[w], axis=0, keepdims=True)
        return tuple(res)

    def p_send(e):
        to = peer(e)
        return remote(pm.at[to, pl.ds(0, 2)], pall.at[me, pl.ds(0, 2)], s_p.at[0], r_p.at[0], to)

    with scope('share'):
        zt = jnp.zeros((HEAD, t_loc), f32)
        sums = lax.fori_loop(0, n, share_step, (zt, zt))
    for e in far:
        p_send(e).start()
    for e in far:
        q_send(e).start()
    pall[me, 0:2, :] = pm[me, 0:2, :]
    for w in range(2):
        gg_s[w] = jnp.broadcast_to(jnp.sum(sums[w], axis=1, keepdims=True), (HEAD, HEAD)).T[0:8, :]
    tq[:, cols] = dq_s[rows(me), :]
    tkv[:, :, cols] = dkv[me]

    def flip_o(i):
        dt[:, rows(i)] = o_s[rows(i), :].T

    def flip_v(i):
        dt[:, rows(i)] = dkv[i, 1].T

    def dwo_step(t):
        gy_copy(t).wait()

        @pl.when(t + 1 < nt)
        def _():
            gy_copy(t + 1).start()

        @pl.when(t + 1 == nt)
        def _():
            h_copy(t + 1).start()
        dwo_s[:, ds(t, cw)] = dotf(dt[...], tile[lax.rem(t, 2)], NN)

    def dwv_step(t):
        h_copy(t).wait()

        @pl.when(t + 1 < 2 * nt)
        def _():
            h_copy(t + 1).start()

        @pl.when(t + 1 == 2 * nt)
        def _():
            h2_copy(0).start()
        r = dotf(dt[...], tile[lax.rem(t, 2)], NN)
        for u in range(cw // HEAD):
            bv[(t - nt) * (cw // HEAD) + u] = r[:, u * HEAD:(u + 1) * HEAD].T

    def y_step(t):
        wo_copy(t).wait()

        @pl.when(t + 1 < nt)
        def _():
            wo_copy(t + 1).start()
        cs = ds(t, cw)
        y_s[:, cs] = (x_ref[:, cs].astype(f32) + dotf(att[...], wtile[lax.rem(t, 2)], NN)).astype(bf16)

    def v_send(e):
        to = peer(e)
        return remote(bv.at[to], dwv_out.at[:, cols], s_v.at[0], r_v.at[0], to)

    def out(i):
        src, dst, k = ((y_s, y_out, 0), (dwo_s, dwo_out, 1), (gx_s, gx_out, 0), (bv.at[me], dwv_out.at[:, cols], 2),
                       (raw.at[1, rows_f(0, me), :], dwq_out.at[:, cols], 2), (raw.at[1, rows_f(1, me), :], dwk_out.at[:, cols], 2),
                       (gg_s, gg_out, 3), (gpart.at[me], gall.at[me], 4))[i]
        return pltpu.make_async_copy(src, dst, s_out.at[k])

    def rows_f(w, to):
        return ds(w * n + to, HEAD)

    with scope('dwo'):
        loop(0, n, flip_o)
        loop(0, nt, dwo_step)
        out(1).start()

    def m_send(e):
        return remote(mine2.at[pl.ds(0, 2)], mall.at[me, pl.ds(0, 2)], s_m.at[0], r_m.at[0], peer(e))

    with scope('dwv'):
        loop(0, n, flip_v)
        loop(nt, 2 * nt, dwv_step)
        out(3).start()
    with scope('pwait'):
        settle(pall.at[pl.ds(0, n - 1), pl.ds(0, 2)], s_p.at[0], r_p.at[0])
        tot = pall[0, 0:2, :]
        for j in range(1, n):
            tot = tot + pall[j, 0:2, :]
        mine2[0:2, :] = tot * (1.0 / d)
    for e in far:
        m_send(e).start()
    mall[me, 0:2, :] = mine2[0:2, :]
    for e in far:
        v_send(e).start()
    with scope('y'):
        settle(att.at[pl.ds(0, t_loc - t_loc // n), :], s_o.at[0], r_o.at[0])
        loop(0, nt, y_step)
        out(0).start()

    def w_copies(t):
        slot = lax.rem(t, 2)
        return [pltpu.make_async_copy(w.at[ds(t, wr), :], wrow.at[slot, i], s_wr.at[slot]) for i, w in enumerate((wq_ref, wk_ref, wv_ref))]

    for cp in w_copies(0):
        cp.start()
    cl = cl_s[...]
    sl = sl_s[...]

    def back_rope(a):
        a = a.astype(f32)
        return a * cl + pltpu.roll(a, half, 1) * sl

    def loc_step(i):
        tq[:, hs(i)] = (inv[0] * (back_rope(tq[:, hs(i)]) * g_ref[0:1, hs(i)] - qkl[0, :, hs(i)] * inv[0] * mq)).astype(bf16)
        tkv[0, :, hs(i)] = (inv[1] * (back_rope(tkv[0, :, hs(i)]) * g_ref[1:2, hs(i)] - qkl[1, :, hs(i)] * inv[1] * mk)).astype(bf16)

    with scope('mwait'):
        settle(mall.at[pl.ds(0, n - 1), pl.ds(0, 2)], s_m.at[0], r_m.at[0])

    def head_step(j):
        js = rows(j)
        for w, src in enumerate((dq_s[js, :], dkv[j, 0])):
            rawT[w * HEAD:(w + 1) * HEAD, js] = (sall[j, w:w + 1, :] * (unroped(src, js) * gcol[w] - hatT[w, :, js] * mall[j, w:w + 1, :])).astype(bf16)

    with scope('head'):
        loop(0, n, head_step)

    def a_send(to):
        return remote(raw.at[1, rows_f(0, to), :], dwq_out.at[:, cols], s_a.at[0], r_a.at[0], to)

    def b_send(to):
        return remote(raw.at[1, rows_f(1, to), :], dwk_out.at[:, cols], s_b.at[0], r_b.at[0], to)

    def dw_step(t):
        h2_copy(t).wait()

        @pl.when(t + 1 < nt)
        def _():
            h2_copy(t + 1).start()
        nn = chip(t)
        r = dotf(rawT[...], tile[lax.rem(t, 2)], NN)
        for u in range(cw // HEAD):
            to = nn * (cw // HEAD) + u
            for w in range(2):
                raw[1, rows_f(w, to), :] = r[w * HEAD:(w + 1) * HEAD, u * HEAD:(u + 1) * HEAD].T

            @pl.when(to != me)
            def _():
                a_send(to).start()
                b_send(to).start()

    with scope('dw'):
        loop(0, nt, dw_step)
    out(4).start()
    out(5).start()
    with scope('waitkv'):
        settle(tkv.at[:, pl.ds(0, t_loc - t_loc // n), :], s_kv.at[0], r_kv.at[0])
    with scope('waitq'):
        settle(tq.at[pl.ds(0, t_loc - t_loc // n), :], s_q.at[0], r_q.at[0])

    mq = spread_col(mine2[0:1, :])
    mk = spread_col(mine2[1:2, :])
    with scope('loc'):
        loop(0, nd, loc_step)

    def dh_step(t):
        settle(wrow.at[lax.rem(t, 2)], s_wr.at[lax.rem(t, 2)])

        @pl.when(t + 1 < nw)
        def _():
            for cp in w_copies(t + 1):
                cp.start()
        slot = lax.rem(t, 2)
        r = dotf(tq[...], wrow[slot, 0], NT) + dotf(tkv[0], wrow[slot, 1], NT) + dotf(tkv[1], wrow[slot, 2], NT)
        dh[:, ds(t, wr)] = r.astype(bf16).astype(f32)

    with scope('dh'):
        loop(0, nw, dh_step)

    def mx_step(i, acc):
        return acc + dh[:, hs(i)] * g_ref[2:3, hs(i)] * x_ref[:, hs(i)].astype(f32)

    def g_send(e):
        return remote(gpart.at[peer(e), pl.ds(0, 1)], gall.at[me, pl.ds(0, 1)], s_g.at[0], r_g.at[0], peer(e))

    with scope('gx'):
        mx = jnp.sum(lax.fori_loop(0, nd, mx_step, zero), axis=1, keepdims=True) * (1.0 / d) * xinv[...]

        def gx_step(i):
            xh = x_ref[:, hs(i)].astype(f32) * xinv[...]
            dhh = dh[:, hs(i)]
            gpart[i] = jnp.broadcast_to(jnp.sum(dhh * xh, axis=0, keepdims=True), (8, HEAD))
            gx_s[:, hs(i)] = (gy_ref[:, hs(i)].astype(f32) + xinv[...] * (dhh * g_ref[2:3, hs(i)] - xh * mx)).astype(bf16)

        loop(0, nd, gx_step)
        out(2).start()
    for e in far:
        g_send(e).start()
    out(7).start()
    out(6).start()
    with scope('end_drain'):
        for a in range(2):
            settle(alls[a].at[pl.ds(0, (nz - 1) * t_loc), :], s_ring.at[a])
            settle(alls[a].at[pl.ds(0, nz * t_loc), :], s_par.at[a])
        settle(tkv, s_out.at[0])
        settle(dwo_s, s_out.at[1])
        settle(bv.at[pl.ds(0, 3)], s_out.at[2])
        settle(gg_s, s_out.at[3])
        settle(gpart.at[0], s_out.at[4])
    most = pl.ds(0, HEAD - HEAD // n)
    with scope('end_v'):
        settle(dwv_out.at[most, :], s_v.at[0], r_v.at[0])
    with scope('end_a'):
        settle(dwq_out.at[most, :], s_a.at[0], r_a.at[0])
    with scope('end_b'):
        settle(dwk_out.at[most, :], s_b.at[0], r_b.at[0])
    with scope('end_g'):
        settle(gall.at[pl.ds(0, n - 1), pl.ds(0, 1)], s_g.at[0], r_g.at[0])


def block(n, x, gy, pos, gq, gk, gn, freq, wq, wk, wv, wo):
    t_loc, d = x.shape
    t_all = t_loc * n
    vm = pl.BlockSpec(memory_space=pltpu.VMEM)
    hb = pl.BlockSpec(memory_space=pl.ANY)
    S = jax.ShapeDtypeStruct
    V = pltpu.VMEM
    sem = pltpu.SemaphoreType.DMA
    hd = (t_all, HEAD)
    tok = (t_loc, d)
    nz = n // 2
    return pl.pallas_call(functools.partial(block_kernel, n),
        in_specs=[hb] * 2 + [vm] * 5 + [hb] * 4,
        out_specs=[hb] * 10,
        out_shape=[S(tok, bf16), S(tok, bf16), S((n, 8, d // n), f32)] + [S((d // n, d), f32)] * 4 + [S((2, 8, HEAD), f32), S((t_all, d), bf16), S((t_all, d), bf16)],
        scratch_shapes=[V(tok, bf16), V(tok, bf16), V((8, d), f32), V(tok, bf16), V((d, 3 * HEAD), bf16), V((HEAD, d), bf16), V((3,) + hd, f32), V((2,) + tok, bf16), V((2, d, 2 * HEAD), bf16), V((2, t_all, 2 * HEAD), bf16), V((2, 3, 2 * HEAD, d), bf16),
            V((2,) + tok, f32), V((2, HEAD, t_all), f32), V((2, HEAD // 2, t_all), f32)] + [V(hd, bf16)] * 5 + [V((8, t_all), f32)] * 2
        + [V(hd, bf16), V((n, 2, t_loc, HEAD), bf16), V(tok, bf16), V((2,) + tok, bf16), V(tok, bf16), V((HEAD, t_all), bf16), V((n, d // n, HEAD), f32), V((2 * HEAD, t_all), bf16), V(tok, bf16), V((HEAD, d), f32), V(tok, bf16), V(tok, f32),
            V((2, t_loc, HEAD), f32), V((t_loc, HEAD), f32), V((t_loc, HEAD), f32), V((2, t_loc, HEAD), f32), V((t_loc, HEAD), f32), V((8, t_loc), f32), V((n, 8, t_loc), f32), V((8, t_loc), f32), V((n, 8, t_loc), f32), V((n, 8, t_loc), f32), V((n, 8, t_loc), f32), V((n, 8, d // n), f32), V((2, 8, HEAD), f32)]
        + [sem((2,)), sem((2, 2, nz - 1, 2)), sem((2,)), sem((2, 2 * (nz - 1))), sem((2,))] + [sem((1,))] * 20
        + [sem((2,)), sem((2,)), sem((2,)), sem((7,)), sem((2,)), sem((1,)), sem((5,))],
        compiler_params=pltpu.CompilerParams(collective_id=1, has_side_effects=True, vmem_limit_bytes=67043328), name='block')(x, gy, pos, gq, gk, gn, freq, wq, wk, wv, wo)


def copy_kernel(*refs):
    k = (len(refs) - 2) // 3
    src, dst, buf, si, so = list(refs[:k - 1]), refs[k - 1:2 * k - 1], refs[2 * k - 1:3 * k - 1], refs[-2], refs[-1]
    parts = src[k - 3]
    src[k - 3:] = [parts, src[k - 2].at[0, 0:1, :], src[k - 2].at[1, 0:1, :]]
    buf = list(buf)
    total = buf[k - 3]
    buf[k - 3] = refs[-3]
    ins = [pltpu.make_async_copy(src[i], buf[i], si.at[i]) for i in range(k)]
    outs = [pltpu.make_async_copy(buf[i], dst[i], so.at[i]) if i != k - 3 else None for i in range(k)]
    for cp in ins:
        cp.start()
    outs[k - 3] = pltpu.make_async_copy(total, dst[k - 3], so.at[k - 3])
    for i in range(k):
        ins[i].wait()
        if i == k - 3:
            total[...] = jnp.sum(refs[-3][:, 0:1, :], axis=0)
        outs[i].start()
    for cp in outs:
        cp.wait()


def copy_out(arrays):
    hb = pl.BlockSpec(memory_space=pl.ANY)
    shapes = [(a.shape, a.dtype) for a in arrays[:-2]] + [((1, HEAD), f32)] * 3
    k = len(shapes)
    return pl.pallas_call(copy_kernel, in_specs=[hb] * len(arrays), out_specs=[hb] * k, out_shape=[jax.ShapeDtypeStruct(*a) for a in shapes],
        scratch_shapes=[pltpu.VMEM(*a) for a in shapes] + [pltpu.VMEM(arrays[-2].shape, f32)] + [pltpu.SemaphoreType.DMA((k,))] * 2, name='copy_out')(*arrays)


def solution(mesh):
    n = mesh.shape['sp']

    def device_step(x_in, grad_y, positions, g_norm, wq, wk, wv, wo, gq, gk):
        half = HEAD // 2
        inv_freq = ROPE_BASE ** (-np.arange(half) * (2.0 / HEAD))
        freq = jnp.asarray(np.tile(inv_freq, (8, 2)), f32)
        y, gx, gn, dwq, dwk, dwv, dwo, gg, _, _ = block(n, x_in[0], grad_y[0], positions, gq, gk, g_norm, freq, wq, wk, wv, wo)
        y, gx, dwq, dwk, dwv, dwo, gn, ggq, ggk = copy_out([y, gx, dwq, dwk, dwv, dwo, gn, gg])
        return (y[None], gx[None], gn[0], dwq, dwk, dwv, dwo, ggq[0], ggk[0])

    seq_spec = P('dp', 'sp', None)
    rep2, rep1 = P(None, None), P(None)
    row_spec, vec_spec = P(('dp', 'sp'), None), P(('dp', 'sp'))
    return jax.shard_map(device_step, mesh=mesh, in_specs=(seq_spec, seq_spec, P('dp', 'sp'), rep1, rep2, rep2, rep2, rep2, rep1, rep1), out_specs=(seq_spec, seq_spec, vec_spec, row_spec, row_spec, row_spec, row_spec, vec_spec, vec_spec), check_vma=False)
```

```python
import contextlib
import functools
import jax
import jax.numpy as jnp
import numpy as np
from jax import lax
from jax.experimental import pallas as pl
from jax.experimental.pallas import tpu as pltpu
from jax.sharding import PartitionSpec as P

HEAD = 128
NORM_EPS = 1e-5
ROPE_BASE = 10000.0
LOG2E = 1.4426950408889634
f32 = jnp.float32
bf16 = jnp.bfloat16
MESH = pl.DeviceIdType.MESH
NN = (((1,), (0,)), ((), ()))
NT = (((1,), (1,)), ((), ()))
TN = (((0,), (0,)), ((), ()))
PROF = 0
scope = jax.named_scope if PROF else (lambda name: contextlib.nullcontext())


def dotf(a, b, dims):
    return lax.dot_general(a, b, dims, preferred_element_type=f32)


def remote(src, dst, ss, rs, to):
    return pltpu.make_async_remote_copy(src_ref=src, dst_ref=dst, send_sem=ss, recv_sem=rs, device_id={'sp': to}, device_id_type=MESH)


def ds(i, size):
    return pl.ds(pl.multiple_of(i * size, size), size)


def settle(ref, *sems):
    for sem in sems:
        pltpu.make_async_copy(ref, ref, sem).wait()


def as_row(col):
    return jnp.broadcast_to(col, (col.shape[0], HEAD)).T[0:1, :]


def loop(lo, hi, body):
    def step(i, carry):
        body(i)
        return carry
    lax.fori_loop(lo, hi, step, 0)


def block_kernel(n, x_hbm, gy_hbm, pos_hbm, gq_hbm, gk_hbm, gn1_hbm, fr_hbm, wq_ref, wk_ref, wv_ref, wo_ref,
                 y_out, gx_out, gall, dwq_out, dwk_out, dwv_out, dwo_out, gg_out, h_all, gy_all,
                 pos_ref, gq_ref, gk_ref, gn1_ref, fr_ref, x_ref, gy_ref, g_ref, hid, wh, woh, raw, xbuf, wtile, tile, wrow, qkl, hatT, csT, q_s, k_s, v_s, do_s, o_s, lse, dl,
                 dq_s, dkv, tq, tkv, att, dt, bv, rawT, y_s, dwo_s, gx_s, dh, ssq, cl_s, sl_s, inv, xinv, mine, sall, mine2, mall, pm, pall, gpart, gg_s,
                 s_ring, r_ring, s_par, r_par, r_own, s_st, r_st, s_o, r_o, s_kv, r_kv, s_q, r_q, s_v, r_v, s_a, r_a, s_b, r_b, s_m, r_m, s_g, r_g, s_p, r_p,
                 s_ld, s_t, s_w, s_x, s_wr, s_loc, s_out, s_in):
    me = lax.axis_index('sp')
    t_loc, d = x_hbm.shape
    t_all = t_loc * n
    z = me // 2
    c = lax.rem(me, 2)
    nz = n // 2
    mate = me + 1 - 2 * c
    up = lax.rem(z + 1, nz) * 2 + c
    down = lax.rem(z + nz - 1, nz) * 2 + c
    nd = d // HEAD
    half = HEAD // 2
    sub = t_loc // 4
    last = nz - 2
    ticks = 2 * (nz - 1)
    blk = 2 * t_loc
    nb = t_all // blk
    cexp = HEAD ** -0.5 * LOG2E
    scale = HEAD ** -0.5
    cw = tile.shape[2]
    nt = d // cw
    wr = wrow.shape[2]
    nw = d // wr
    cols = ds(me, HEAD)
    far = sorted(range(1, n), key=lambda e: -min(e, n - e))
    alls = (h_all, gy_all)
    own_src = (hid, gy_hbm)

    def peer(e):
        return lax.rem(me + e, n)

    def rows(i):
        return ds(i, t_loc)

    def hs(i):
        return ds(i, HEAD)

    def chip(s):
        k = nz // 2 - (s + 1) // 2
        return lax.rem(z + nz + jnp.where(lax.rem(s, 2) == 0, -k, k), nz)

    def piece(core, direction, s, u):
        bz = lax.rem(z + nz - 1 - s, nz) if direction == 0 else lax.rem(z + 1 + s, nz)
        return ds((bz * 2 + core) * 4 + 2 * direction + u, sub)

    def ring(a, direction, s, u):
        ref = alls[a]
        bz = lax.rem(z + nz - s, nz) if direction == 0 else lax.rem(z + s, nz)
        rs = ds((bz * 2 + c) * 4 + 2 * direction + u, sub)
        return remote(ref.at[rs, :], ref.at[rs, :], s_ring.at[a], r_ring.at[a, direction, s, u], up if direction == 0 else down)

    def ring0(a, direction, u):
        rs = ds(me * 4 + 2 * direction + u, sub)
        return remote(own_src[a].at[pl.ds((2 * direction + u) * sub, sub), :], alls[a].at[rs, :], s_ring.at[a], r_ring.at[a, direction, 0, u], up if direction == 0 else down)

    def par(a, direction, s, u):
        rs = piece(c, direction, s, u)
        return remote(alls[a].at[rs, :], alls[a].at[rs, :], s_par.at[a], r_par.at[a, 2 * s + u], mate)

    def own_par(a):
        return remote((hid, gy_ref)[a], alls[a].at[rows(me), :], s_par.at[a], r_own.at[a], mate)

    def own_loc(a):
        return pltpu.make_async_copy((hid, gy_ref)[a], alls[a].at[rows(me), :], s_loc.at[0])

    def comm(a, t):
        s = t // 2
        u = lax.rem(t, 2)
        for direction in range(2):
            ring(a, direction, s, u).wait_recv()

            @pl.when(s < last)
            def _():
                ring(a, direction, s + 1, u).start()
            par(a, direction, s, u).start()

    def loads(a, t):
        s = t // 2
        u = lax.rem(t, 2)
        slot = lax.rem(t, 2)
        out = []
        for i, (core, direction) in enumerate(((c, 0), (c, 1), (1 - c, 0), (1 - c, 1))):
            out.append(pltpu.make_async_copy(alls[a].at[piece(core, direction, s, u), :], xbuf.at[slot, pl.ds(i * sub, sub), :], s_ld.at[slot]))
        return out

    def mate_load(a):
        return pltpu.make_async_copy(alls[a].at[rows(mate), :], xbuf.at[1], s_ld.at[1])

    def spots(t):
        s = t // 2
        u = lax.rem(t, 2)
        return [piece(c, 0, s, u), piece(c, 1, s, u), piece(1 - c, 0, s, u), piece(1 - c, 1, s, u)]

    def gather(a, t, work, put):
        @pl.when((t >= a) & (t < ticks))
        def _():
            with scope('comm'):
                comm(a, t)

        @pl.when(t == 0)
        def _():
            own_par(a).wait_recv()
            mate_load(a).start()
            put(work((hid, gy_ref)[a][...]), [rows(me)])

        @pl.when(t == 1)
        def _():
            mate_load(a).wait()
            put(work(xbuf[1]), [rows(mate)])

        @pl.when(t >= 2)
        def _():
            settle(xbuf.at[lax.rem(t, 2)], s_ld.at[lax.rem(t, 2)])
            put(work(xbuf[lax.rem(t, 2)]), spots(t - 2))

        @pl.when((t >= 1) & (t < ticks + 1))
        def _():
            settle(alls[a].at[pl.ds(0, 2 * sub), :], r_par.at[a, t - 1])
            for cp in loads(a, t - 1):
                cp.start()

    def stat_tile(i, act):
        slot = lax.rem(i, 2)
        cs = ds(lax.rem(i, nt), cw)

        @pl.when(i < nt)
        def _():
            act(pltpu.make_async_copy(wq_ref.at[:, cs], wtile.at[slot], s_w.at[slot]))

        @pl.when(i >= nt)
        def _():
            act(pltpu.make_async_copy(wk_ref.at[:, cs], wtile.at[slot], s_w.at[slot]))

    def start(cp):
        cp.start()

    def wait(cp):
        cp.wait()

    def stat_step(i):
        stat_tile(i, wait)

        @pl.when(i + 1 < 2 * nt)
        def _():
            stat_tile(i + 1, start)
        r = dotf(hid[...], wtile[lax.rem(i, 2)], NN)
        w = i // nt
        qkl[w, :, ds(lax.rem(i, nt), cw)] = r
        acc = r[:, :HEAD] * r[:, :HEAD]
        for j in range(1, cw // HEAD):
            acc = acc + r[:, j * HEAD:(j + 1) * HEAD] * r[:, j * HEAD:(j + 1) * HEAD]
        ssq[w] = ssq[w] + acc

    def st_send(e):
        return remote(mine.at[pl.ds(0, 3)], sall.at[me, pl.ds(0, 3)], s_st.at[0], r_st.at[0], peer(e))

    sgn = jnp.where(lax.broadcasted_iota(jnp.int32, (1, HEAD), 1) < half, -1.0, 1.0).astype(f32)

    def stat_done():
        for w in range(2):
            iv = lax.rsqrt(jnp.sum(ssq[w], axis=1, keepdims=True) * (1.0 / d) + NORM_EPS)
            inv[w] = jnp.broadcast_to(iv, (t_loc, HEAD))
            mine[w:w + 1, :] = as_row(iv)
        mine[2:3, :] = pos_ref[...].astype(f32)
        sall[me, 0:3, :] = mine[0:3, :]
        ang = spread_col(pos_ref[...].astype(f32)) * fr_ref[0:1, :]
        cl_s[...] = jnp.cos(ang)
        sl_s[...] = jnp.sin(ang) * (-sgn)

    def spread_col(row):
        return jnp.broadcast_to(row, (HEAD, row.shape[1])).T

    def head_w(i):
        w = (wq_ref, wk_ref, wv_ref)[i]
        return pltpu.make_async_copy(w.at[:, cols], wh.at[:, pl.ds(i * HEAD, HEAD)], s_x.at[0])

    def wo_load():
        return pltpu.make_async_copy(wo_ref.at[cols, :], woh, s_x.at[1])

    with scope('begin'):
        barrier = pltpu.get_barrier_semaphore()
        for to in (up, down, mate):
            pl.semaphore_signal(barrier, inc=1, device_id={'sp': to}, device_id_type=MESH)

        def x_piece(p):
            rs = pl.ds(p * sub, sub)
            return pltpu.make_async_copy(x_hbm.at[rs, :], x_ref.at[rs, :], s_x.at[2 + p])

        smalls = [pltpu.make_async_copy(src, dst, s_in.at[i]) for i, (src, dst) in enumerate(((gn1_hbm, gn1_ref), (gq_hbm, gq_ref), (gk_hbm, gk_ref), (pos_hbm, pos_ref), (fr_hbm, fr_ref)))]
        smalls[0].start()
        for p in (0, 2, 1, 3):
            x_piece(p).start()
        for cp in smalls[1:]:
            cp.start()
        gy_load = pltpu.make_async_copy(gy_hbm, gy_ref, s_x.at[6])
        gy_load.start()
        for i in range(3):
            head_w(i).start()
        wo_load().start()
        stat_tile(0, start)
        pl.semaphore_wait(barrier, 3)
        ring0(1, 0, 0).start()
        ring0(1, 1, 0).start()
        smalls[0].wait()
        g_ref[2:3, :] = gn1_ref[...].astype(f32).reshape(1, d)

        def norm_piece(p):
            rs = pl.ds(p * sub, sub)
            x_piece(p).wait()

            def sq_step(i, acc):
                xf = x_ref[rs, hs(i)].astype(f32)
                return acc + xf * xf

            acc = lax.fori_loop(0, nd, sq_step, jnp.zeros((sub, HEAD), f32))
            xi = lax.rsqrt(jnp.sum(acc, axis=1, keepdims=True) * (1.0 / d) + NORM_EPS)
            xinv[rs, :] = jnp.broadcast_to(xi, (sub, HEAD))

            def hid_step(i):
                hid[rs, hs(i)] = (x_ref[rs, hs(i)].astype(f32) * xi * g_ref[2:3, hs(i)]).astype(bf16)

            loop(0, nd, hid_step)

        for p in (0, 2, 1, 3):
            norm_piece(p)
            ring0(0, p // 2, p % 2).start()
        for cp in smalls[1:]:
            cp.wait()
        for w, src in enumerate((gq_ref, gk_ref)):
            g_ref[w:w + 1, :] = src[...].astype(f32).reshape(1, d)
        zero = jnp.zeros((t_loc, HEAD), f32)
        ssq[...] = jnp.zeros_like(ssq)
        gy_load.wait()
        own_loc(1).start()
    own_par(0).start()
    own_par(1).start()
    own_loc(0).start()
    settle(wh, s_x.at[0])
    wo_load().wait()

    hb = t_loc // 2

    def finish(s):
        for direction in range(2):
            bz = lax.rem(z + nz - 1 - s, nz) if direction == 0 else lax.rem(z + 1 + s, nz)

            def one(core):
                b = bz * 2 + core
                rs = ds(b * 2 + direction, hb)
                st = sall[b, 0:3, direction * hb:(direction + 1) * hb]
                ang = spread_col(st[2:3, :]) * fr_ref[0:1, :]
                co = jnp.cos(ang)
                si = jnp.sin(ang)
                csT[0, :, rs] = co.T[:half, :]
                csT[1, :, rs] = si.T[:half, :]
                si = si * sgn
                for w, dst in enumerate((q_s, k_s)):
                    hat = raw[w, rs, :] * spread_col(st[w:w + 1, :])
                    hatT[w, :, rs] = hat.T
                    hat = hat * g_ref[w:w + 1, cols]
                    dst[rs, :] = (hat * co + pltpu.roll(hat, half, 1) * si).astype(bf16)
                v_s[rs, :] = raw[2, rs, :].astype(bf16)

            loop(0, 2, one)

    def qkv_work(xv):
        return dotf(xv, wh[...], NN)

    def qkv_put(r, where):
        step = r.shape[0] // len(where)
        for i, rs in enumerate(where):
            for w in range(3):
                raw[w, rs, :] = r[i * step:(i + 1) * step, w * HEAD:(w + 1) * HEAD]

    spt = 2 * nt // 4

    def x_tick(t):
        gather(0, t, qkv_work, qkv_put)

        @pl.when(t == 2 * last - 1)
        def _():
            for direction in range(2):
                ring0(1, direction, 1).start()
            comm(1, 0)

        @pl.when(t < 4)
        def _():
            with scope('stat'):
                loop(t * spt, (t + 1) * spt, stat_step)

        @pl.when(t == 4)
        def _():
            with scope('statdone'):
                stat_done()

        @pl.when(t == 8)
        def _():
            for e in far:
                st_send(e).start()

        @pl.when(t == 10)
        def _():
            settle(sall.at[pl.ds(0, n - 1), pl.ds(0, 3)], s_st.at[0], r_st.at[0])
        lo = jnp.where(t == 10, -1, jnp.where(t == 11, 1, jnp.where(t >= 12, t - 9, 0)))
        hi = jnp.where(t == 10, 1, jnp.where(t == 11, 3, jnp.where((t >= 12) & (t <= 14), t - 8, -1)))
        with scope('finish'):
            loop(lo, hi, finish)

    with scope('gather_x'):
        loop(0, ticks + 2, x_tick)

    def attend(j):
        qs = ds(j, blk)
        q = q_s[qs, :]

        def unit(kb, carry, masked):
            m, l, acc = carry
            ks = ds(kb, blk)
            s = dotf(q, k_s[ks, :], NT)
            if masked:
                r = lax.broadcasted_iota(jnp.int32, (blk, blk), 0)
                cc = lax.broadcasted_iota(jnp.int32, (blk, blk), 1)
                s = jnp.where(r >= cc, s, -1e30)
            mn = jnp.maximum(m, jnp.max(s, axis=1, keepdims=True))
            al = jnp.exp2((m - mn) * cexp)
            p = jnp.exp2((s - mn) * cexp)
            l = l * al + jnp.sum(p, axis=1, keepdims=True)
            acc = acc * al + dotf(p.astype(bf16), v_s[ks, :], NN)
            return mn, l, acc

        init = (jnp.full((blk, 1), -1e30, f32), jnp.zeros((blk, 1), f32), jnp.zeros((blk, HEAD), f32))
        carry = lax.fori_loop(0, j, functools.partial(unit, masked=False), init)
        m, l, acc = unit(j, carry, True)
        o = acc / l
        raw[2, qs, :] = o
        o_s[qs, :] = o.astype(bf16)
        lse[0:1, qs] = as_row(m * cexp + jnp.log2(l))

    def o_send(e):
        to = peer(e)
        return remote(o_s.at[rows(to), :], att.at[:, cols], s_o.at[0], r_o.at[0], to)

    def do_work(xv):
        return dotf(xv, woh[...], NT).astype(bf16)

    def do_put(r, where):
        step = r.shape[0] // len(where)
        for i, rs in enumerate(where):
            do_s[rs, :] = r[i * step:(i + 1) * step]

    def y_tick(t):
        gather(1, t, do_work, do_put)

        @pl.when(t == 1)
        def _():
            with scope('finish'):
                finish(last)
        t = t - 1
        lo = jnp.where(t == 0, 0, jnp.where(t <= 4, t + 1, jnp.where(t <= 6, 6, 7)))
        hi = jnp.where(t == 0, 2, jnp.where(t <= 4, t + 2, jnp.where(t == 5, 6, jnp.where(t == 8, 8, 7))))
        hi = jnp.where(t < 0, 0, hi)
        with scope('attend'):
            loop(lo, hi, attend)

        @pl.when(t == ticks - 3)
        def _():
            for e in far[-5:]:
                o_send(e).start()

        @pl.when(t == ticks - 2)
        def _():
            for e in far[:-5]:
                o_send(e).start()

    with scope('gather_y'):
        loop(0, ticks + 2, y_tick)

    def gy_copy(t):
        return pltpu.make_async_copy(gy_all.at[:, ds(t, cw)], tile.at[lax.rem(t, 2)], s_t.at[lax.rem(t, 2)])

    def h_copy(t):
        return pltpu.make_async_copy(h_all.at[:, ds(lax.rem(t, nt), cw)], tile.at[lax.rem(t, 2)], s_t.at[lax.rem(t, 2)])

    def h2_copy(t):
        return pltpu.make_async_copy(h_all.at[:, ds(chip(t), cw)], tile.at[lax.rem(t, 2)], s_t.at[lax.rem(t, 2)])

    def wo_copy(t):
        return pltpu.make_async_copy(wo_ref.at[:, ds(t, cw)], wtile.at[lax.rem(t, 2)], s_w.at[lax.rem(t, 2)])

    def q_send(e):
        to = peer(e)
        return remote(dq_s.at[rows(to), :], tq.at[:, cols], s_q.at[0], r_q.at[0], to)

    def kv_send(to):
        return remote(dkv.at[to], tkv.at[:, :, cols], s_kv.at[0], r_kv.at[0], to)

    settle(h_all.at[pl.ds(0, 2 * t_loc), :], s_loc.at[0])
    gy_copy(0).start()
    wo_copy(0).start()
    att[:, cols] = o_s[rows(me), :]
    raw[0] = jnp.zeros((t_all, HEAD), f32)

    def delta(j):
        qs = ds(j, blk)
        dl[0:1, qs] = as_row(jnp.sum(raw[2, qs, :] * do_s[qs, :].astype(f32), axis=1, keepdims=True))

    with scope('delta'):
        loop(0, nb, delta)

    def bwd_step(s):
        kb = chip(s)
        ks = ds(kb, blk)
        k = k_s[ks, :]
        v = v_s[ks, :]

        def unit(qb, carry, masked):
            dk, dv = carry
            qs = ds(qb, blk)
            q = q_s[qs, :]
            do = do_s[qs, :]
            p = jnp.exp2(dotf(k, q, NT) * cexp - lse[0:1, qs])
            if masked:
                r = lax.broadcasted_iota(jnp.int32, (blk, blk), 0)
                cc = lax.broadcasted_iota(jnp.int32, (blk, blk), 1)
                p = jnp.where(cc >= r, p, 0.0)
            g = (p * (dotf(v, do, NT) - dl[0:1, qs])).astype(bf16)
            dv = dv + dotf(p.astype(bf16), do, NN)
            dk = dk + dotf(g, q, NN)
            raw[0, qs, :] = raw[0, qs, :] + dotf(g, k, TN)
            return dk, dv

        zk = jnp.zeros((blk, HEAD), f32)
        carry = unit(kb, (zk, zk), True)
        dk, dv = lax.fori_loop(kb + 1, nb, functools.partial(unit, masked=False), carry)
        dk = (dk * scale).astype(bf16)
        dv = dv.astype(bf16)
        for u in range(2):
            dkv[2 * kb + u, 0] = dk[u * t_loc:(u + 1) * t_loc]
            dkv[2 * kb + u, 1] = dv[u * t_loc:(u + 1) * t_loc]

        @pl.when(kb != z)
        def _():
            for u in range(2):
                kv_send(2 * kb + u).start()

        @pl.when(kb == z)
        def _():
            kv_send(mate).start()

    with scope('bwd'):
        loop(0, nb, bwd_step)
        dq_s[...] = (raw[0] * scale).astype(bf16)
    gcol = [spread_col(g_ref[w:w + 1, cols])[:, 0:1] for w in range(2)]

    def unroped(src, js):
        ct = csT[0, :, js]
        sn = csT[1, :, js]
        t = src.astype(f32).T
        p, r = t[:half], t[half:]
        return jnp.concatenate([p * ct + r * sn, r * ct - p * sn], axis=0)

    def share_step(j, carry):
        js = rows(j)
        res = []
        for w, src in enumerate((dq_s[js, :], dkv[j, 0])):
            th = unroped(src, js) * hatT[w, :, js]
            res.append(carry[w] + th)
            pm[j, w:w + 1, :] = jnp.sum(th * gcol[w], axis=0, keepdims=True)
        return tuple(res)

    def p_send(e):
        to = peer(e)
        return remote(pm.at[to, pl.ds(0, 2)], pall.at[me, pl.ds(0, 2)], s_p.at[0], r_p.at[0], to)

    with scope('share'):
        zt = jnp.zeros((HEAD, t_loc), f32)
        sums = lax.fori_loop(0, n, share_step, (zt, zt))
    for e in far:
        p_send(e).start()
    for e in far:
        q_send(e).start()
    pall[me, 0:2, :] = pm[me, 0:2, :]
    for w in range(2):
        gg_s[w] = jnp.broadcast_to(jnp.sum(sums[w], axis=1, keepdims=True), (HEAD, HEAD)).T[0:8, :]
    tq[:, cols] = dq_s[rows(me), :]
    tkv[:, :, cols] = dkv[me]

    def flip_o(i):
        dt[:, rows(i)] = o_s[rows(i), :].T

    def flip_v(i):
        dt[:, rows(i)] = dkv[i, 1].T

    def dwo_step(t):
        gy_copy(t).wait()

        @pl.when(t + 1 < nt)
        def _():
            gy_copy(t + 1).start()

        @pl.when(t + 1 == nt)
        def _():
            h_copy(t + 1).start()
        dwo_s[:, ds(t, cw)] = dotf(dt[...], tile[lax.rem(t, 2)], NN)

    def dwv_step(t):
        h_copy(t).wait()

        @pl.when(t + 1 < 2 * nt)
        def _():
            h_copy(t + 1).start()

        @pl.when(t + 1 == 2 * nt)
        def _():
            h2_copy(0).start()
        r = dotf(dt[...], tile[lax.rem(t, 2)], NN)
        for u in range(cw // HEAD):
            bv[(t - nt) * (cw // HEAD) + u] = r[:, u * HEAD:(u + 1) * HEAD].T

    def y_step(t):
        wo_copy(t).wait()

        @pl.when(t + 1 < nt)
        def _():
            wo_copy(t + 1).start()
        cs = ds(t, cw)
        y_s[:, cs] = (x_ref[:, cs].astype(f32) + dotf(att[...], wtile[lax.rem(t, 2)], NN)).astype(bf16)

    def v_send(e):
        to = peer(e)
        return remote(bv.at[to], dwv_out.at[:, cols], s_v.at[0], r_v.at[0], to)

    def out(i):
        src, dst, k = ((y_s, y_out, 0), (dwo_s, dwo_out, 1), (gx_s, gx_out, 0), (bv.at[me], dwv_out.at[:, cols], 2),
                       (raw.at[1, rows_f(0, me), :], dwq_out.at[:, cols], 2), (raw.at[1, rows_f(1, me), :], dwk_out.at[:, cols], 2),
                       (gg_s, gg_out, 3), (gpart.at[me], gall.at[me], 4))[i]
        return pltpu.make_async_copy(src, dst, s_out.at[k])

    def rows_f(w, to):
        return ds(w * n + to, HEAD)

    with scope('dwo'):
        loop(0, n, flip_o)
        loop(0, nt, dwo_step)
        out(1).start()

    def m_send(e):
        return remote(mine2.at[pl.ds(0, 2)], mall.at[me, pl.ds(0, 2)], s_m.at[0], r_m.at[0], peer(e))

    with scope('dwv'):
        loop(0, n, flip_v)
        loop(nt, 2 * nt, dwv_step)
        out(3).start()
    with scope('pwait'):
        settle(pall.at[pl.ds(0, n - 1), pl.ds(0, 2)], s_p.at[0], r_p.at[0])
        tot = pall[0, 0:2, :]
        for j in range(1, n):
            tot = tot + pall[j, 0:2, :]
        mine2[0:2, :] = tot * (1.0 / d)
    for e in far:
        m_send(e).start()
    mall[me, 0:2, :] = mine2[0:2, :]
    for e in far:
        v_send(e).start()
    with scope('y'):
        settle(att.at[pl.ds(0, t_loc - t_loc // n), :], s_o.at[0], r_o.at[0])
        loop(0, nt, y_step)
        out(0).start()

    def w_copies(t):
        slot = lax.rem(t, 2)
        return [pltpu.make_async_copy(w.at[ds(t, wr), :], wrow.at[slot, i], s_wr.at[slot]) for i, w in enumerate((wq_ref, wk_ref, wv_ref))]

    for cp in w_copies(0):
        cp.start()
    cl = cl_s[...]
    sl = sl_s[...]

    def back_rope(a):
        a = a.astype(f32)
        return a * cl + pltpu.roll(a, half, 1) * sl

    def loc_step(i):
        tq[:, hs(i)] = (inv[0] * (back_rope(tq[:, hs(i)]) * g_ref[0:1, hs(i)] - qkl[0, :, hs(i)] * inv[0] * mq)).astype(bf16)
        tkv[0, :, hs(i)] = (inv[1] * (back_rope(tkv[0, :, hs(i)]) * g_ref[1:2, hs(i)] - qkl[1, :, hs(i)] * inv[1] * mk)).astype(bf16)

    with scope('mwait'):
        settle(mall.at[pl.ds(0, n - 1), pl.ds(0, 2)], s_m.at[0], r_m.at[0])

    def head_step(j):
        js = rows(j)
        for w, src in enumerate((dq_s[js, :], dkv[j, 0])):
            rawT[w * HEAD:(w + 1) * HEAD, js] = (sall[j, w:w + 1, :] * (unroped(src, js) * gcol[w] - hatT[w, :, js] * mall[j, w:w + 1, :])).astype(bf16)

    with scope('head'):
        loop(0, n, head_step)

    def a_send(to):
        return remote(raw.at[1, rows_f(0, to), :], dwq_out.at[:, cols], s_a.at[0], r_a.at[0], to)

    def b_send(to):
        return remote(raw.at[1, rows_f(1, to), :], dwk_out.at[:, cols], s_b.at[0], r_b.at[0], to)

    def dw_step(t):
        h2_copy(t).wait()

        @pl.when(t + 1 < nt)
        def _():
            h2_copy(t + 1).start()
        nn = chip(t)
        r = dotf(rawT[...], tile[lax.rem(t, 2)], NN)
        for u in range(cw // HEAD):
            to = nn * (cw // HEAD) + u
            for w in range(2):
                raw[1, rows_f(w, to), :] = r[w * HEAD:(w + 1) * HEAD, u * HEAD:(u + 1) * HEAD].T

            @pl.when(to != me)
            def _():
                a_send(to).start()
                b_send(to).start()

    with scope('dw'):
        loop(0, nt // 2, dw_step)
    with scope('waitkv'):
        settle(tkv.at[:, pl.ds(0, t_loc - t_loc // n), :], s_kv.at[0], r_kv.at[0])
    with scope('waitq'):
        settle(tq.at[pl.ds(0, t_loc - t_loc // n), :], s_q.at[0], r_q.at[0])

    mq = spread_col(mine2[0:1, :])
    mk = spread_col(mine2[1:2, :])
    with scope('loc'):
        loop(0, nd, loc_step)

    def dh_step(t):
        settle(wrow.at[lax.rem(t, 2)], s_wr.at[lax.rem(t, 2)])

        @pl.when(t + 1 < nw)
        def _():
            for cp in w_copies(t + 1):
                cp.start()
        slot = lax.rem(t, 2)
        r = dotf(tq[...], wrow[slot, 0], NT) + dotf(tkv[0], wrow[slot, 1], NT) + dotf(tkv[1], wrow[slot, 2], NT)
        dh[:, ds(t, wr)] = r.astype(bf16).astype(f32)

    with scope('dh'):
        loop(0, nw, dh_step)

    def mx_step(i, acc):
        return acc + dh[:, hs(i)] * g_ref[2:3, hs(i)] * x_ref[:, hs(i)].astype(f32)

    def g_send(e):
        return remote(gpart.at[peer(e), pl.ds(0, 1)], gall.at[me, pl.ds(0, 1)], s_g.at[0], r_g.at[0], peer(e))

    with scope('gx'):
        mx = jnp.sum(lax.fori_loop(0, nd, mx_step, zero), axis=1, keepdims=True) * (1.0 / d) * xinv[...]

        def gx_step(i):
            xh = x_ref[:, hs(i)].astype(f32) * xinv[...]
            dhh = dh[:, hs(i)]
            gpart[i] = jnp.broadcast_to(jnp.sum(dhh * xh, axis=0, keepdims=True), (8, HEAD))
            gx_s[:, hs(i)] = (gy_ref[:, hs(i)].astype(f32) + xinv[...] * (dhh * g_ref[2:3, hs(i)] - xh * mx)).astype(bf16)

        loop(0, nd, gx_step)
        out(2).start()
    for e in far:
        g_send(e).start()
    out(7).start()
    out(6).start()
    with scope('dw2'):
        loop(nt // 2, nt, dw_step)
        out(4).start()
        out(5).start()
    with scope('end_drain'):
        for a in range(2):
            settle(alls[a].at[pl.ds(0, (nz - 1) * t_loc), :], s_ring.at[a])
            settle(alls[a].at[pl.ds(0, nz * t_loc), :], s_par.at[a])
        settle(tkv, s_out.at[0])
        settle(dwo_s, s_out.at[1])
        settle(bv.at[pl.ds(0, 3)], s_out.at[2])
        settle(gg_s, s_out.at[3])
        settle(gpart.at[0], s_out.at[4])
    most = pl.ds(0, HEAD - HEAD // n)
    with scope('end_v'):
        settle(dwv_out.at[most, :], s_v.at[0], r_v.at[0])
    with scope('end_a'):
        settle(dwq_out.at[most, :], s_a.at[0], r_a.at[0])
    with scope('end_b'):
        settle(dwk_out.at[most, :], s_b.at[0], r_b.at[0])
    with scope('end_g'):
        settle(gall.at[pl.ds(0, n - 1), pl.ds(0, 1)], s_g.at[0], r_g.at[0])


def block(n, x, gy, pos, gq, gk, gn, freq, wq, wk, wv, wo):
    t_loc, d = x.shape
    t_all = t_loc * n
    hb = pl.BlockSpec(memory_space=pl.ANY)
    S = jax.ShapeDtypeStruct
    V = pltpu.VMEM
    sem = pltpu.SemaphoreType.DMA
    hd = (t_all, HEAD)
    tok = (t_loc, d)
    nz = n // 2
    return pl.pallas_call(functools.partial(block_kernel, n),
        in_specs=[hb] * 11,
        out_specs=[hb] * 10,
        out_shape=[S(tok, bf16), S(tok, bf16), S((n, 8, d // n), f32)] + [S((d // n, d), f32)] * 4 + [S((2, 8, HEAD), f32), S((t_all, d), bf16), S((t_all, d), bf16)],
        scratch_shapes=[V((1, t_loc), jnp.int32), V((d,), bf16), V((d,), bf16), V((d,), bf16), V((8, HEAD), f32), V(tok, bf16), V(tok, bf16), V((8, d), f32), V(tok, bf16), V((d, 3 * HEAD), bf16), V((HEAD, d), bf16), V((3,) + hd, f32), V((2,) + tok, bf16), V((2, d, 2 * HEAD), bf16), V((2, t_all, 2 * HEAD), bf16), V((2, 3, 2 * HEAD, d), bf16),
            V((2,) + tok, f32), V((2, HEAD, t_all), f32), V((2, HEAD // 2, t_all), f32)] + [V(hd, bf16)] * 5 + [V((8, t_all), f32)] * 2
        + [V(hd, bf16), V((n, 2, t_loc, HEAD), bf16), V(tok, bf16), V((2,) + tok, bf16), V(tok, bf16), V((HEAD, t_all), bf16), V((n, d // n, HEAD), f32), V((2 * HEAD, t_all), bf16), V(tok, bf16), V((HEAD, d), f32), V(tok, bf16), V(tok, f32),
            V((2, t_loc, HEAD), f32), V((t_loc, HEAD), f32), V((t_loc, HEAD), f32), V((2, t_loc, HEAD), f32), V((t_loc, HEAD), f32), V((8, t_loc), f32), V((n, 8, t_loc), f32), V((8, t_loc), f32), V((n, 8, t_loc), f32), V((n, 8, t_loc), f32), V((n, 8, t_loc), f32), V((n, 8, d // n), f32), V((2, 8, HEAD), f32)]
        + [sem((2,)), sem((2, 2, nz - 1, 2)), sem((2,)), sem((2, 2 * (nz - 1))), sem((2,))] + [sem((1,))] * 20
        + [sem((2,)), sem((2,)), sem((2,)), sem((7,)), sem((2,)), sem((1,)), sem((5,)), sem((5,))],
        compiler_params=pltpu.CompilerParams(collective_id=1, has_side_effects=True, vmem_limit_bytes=67043328), name='block')(x, gy, pos, gq, gk, gn, freq, wq, wk, wv, wo)


def copy_kernel(*refs):
    k = (len(refs) - 2) // 3
    src, dst, buf, si, so = list(refs[:k - 1]), refs[k - 1:2 * k - 1], refs[2 * k - 1:3 * k - 1], refs[-2], refs[-1]
    parts = src[k - 3]
    src[k - 3:] = [parts, src[k - 2].at[0, 0:1, :], src[k - 2].at[1, 0:1, :]]
    buf = list(buf)
    total = buf[k - 3]
    buf[k - 3] = refs[-3]
    ins = [pltpu.make_async_copy(src[i], buf[i], si.at[i]) for i in range(k)]
    outs = [pltpu.make_async_copy(buf[i], dst[i], so.at[i]) if i != k - 3 else None for i in range(k)]
    for cp in ins:
        cp.start()
    outs[k - 3] = pltpu.make_async_copy(total, dst[k - 3], so.at[k - 3])
    for i in range(k):
        ins[i].wait()
        if i == k - 3:
            total[...] = jnp.sum(refs[-3][:, 0:1, :], axis=0)
        outs[i].start()
    for cp in outs:
        cp.wait()


def copy_out(arrays):
    hb = pl.BlockSpec(memory_space=pl.ANY)
    shapes = [(a.shape, a.dtype) for a in arrays[:-2]] + [((1, HEAD), f32)] * 3
    k = len(shapes)
    return pl.pallas_call(copy_kernel, in_specs=[hb] * len(arrays), out_specs=[hb] * k, out_shape=[jax.ShapeDtypeStruct(*a) for a in shapes],
        scratch_shapes=[pltpu.VMEM(*a) for a in shapes] + [pltpu.VMEM(arrays[-2].shape, f32)] + [pltpu.SemaphoreType.DMA((k,))] * 2, name='copy_out')(*arrays)


def solution(mesh):
    n = mesh.shape['sp']

    def device_step(x_in, grad_y, positions, g_norm, wq, wk, wv, wo, gq, gk):
        half = HEAD // 2
        inv_freq = ROPE_BASE ** (-np.arange(half) * (2.0 / HEAD))
        freq = jnp.asarray(np.tile(inv_freq, (8, 2)), f32)
        y, gx, gn, dwq, dwk, dwv, dwo, gg, _, _ = block(n, x_in[0], grad_y[0], positions, gq, gk, g_norm, freq, wq, wk, wv, wo)
        y, gx, dwq, dwk, dwv, dwo, gn, ggq, ggk = copy_out([y, gx, dwq, dwk, dwv, dwo, gn, gg])
        return (y[None], gx[None], gn[0], dwq, dwk, dwv, dwo, ggq[0], ggk[0])

    seq_spec = P('dp', 'sp', None)
    rep2, rep1 = P(None, None), P(None)
    row_spec, vec_spec = P(('dp', 'sp'), None), P(('dp', 'sp'))
    return jax.shard_map(device_step, mesh=mesh, in_specs=(seq_spec, seq_spec, P('dp', 'sp'), rep1, rep2, rep2, rep2, rep2, rep1, rep1), out_specs=(seq_spec, seq_spec, vec_spec, row_spec, row_spec, row_spec, row_spec, vec_spec, vec_spec), check_vma=False)
```

```python
import contextlib
import functools
import jax
import jax.numpy as jnp
import numpy as np
from jax import lax
from jax.experimental import pallas as pl
from jax.experimental.pallas import tpu as pltpu
from jax.sharding import PartitionSpec as P

HEAD = 128
NORM_EPS = 1e-5
ROPE_BASE = 10000.0
LOG2E = 1.4426950408889634
f32 = jnp.float32
bf16 = jnp.bfloat16
MESH = pl.DeviceIdType.MESH
NN = (((1,), (0,)), ((), ()))
NT = (((1,), (1,)), ((), ()))
TN = (((0,), (0,)), ((), ()))
PROF = 0
scope = jax.named_scope if PROF else (lambda name: contextlib.nullcontext())


def dotf(a, b, dims):
    return lax.dot_general(a, b, dims, preferred_element_type=f32)


def remote(src, dst, ss, rs, to):
    return pltpu.make_async_remote_copy(src_ref=src, dst_ref=dst, send_sem=ss, recv_sem=rs, device_id={'sp': to}, device_id_type=MESH)


def ds(i, size):
    return pl.ds(pl.multiple_of(i * size, size), size)


def settle(ref, *sems):
    for sem in sems:
        pltpu.make_async_copy(ref, ref, sem).wait()


def as_row(col):
    return jnp.broadcast_to(col, (col.shape[0], HEAD)).T[0:1, :]


def loop(lo, hi, body):
    def step(i, carry):
        body(i)
        return carry
    lax.fori_loop(lo, hi, step, 0)


def block_kernel(n, x_hbm, gy_hbm, pos_hbm, gq_hbm, gk_hbm, gn1_hbm, fr_hbm, wq_ref, wk_ref, wv_ref, wo_ref,
                 y_out, gx_out, gall, dwq_out, dwk_out, dwv_out, dwo_out, gg_out, h_all, gy_all,
                 pos_ref, gq_ref, gk_ref, gn1_ref, fr_ref, x_ref, gy_ref, g_ref, hid, wh, woh, raw, xbuf, wtile, tile, wrow, qkl, hatT, csT, q_s, k_s, v_s, do_s, o_s, lse, ld2,
                 dq_s, dkv, tq, tkv, att, rawT, dh, cl_s, sl_s, inv, xinv, mine, sall, mine2, mall, pm, pall, gpart, gg_s, k2, v2, q2, do2, o2, dq2, dkv2,
                 s_ring, r_ring, s_par, r_par, r_own, s_st, r_st, s_o, r_o, s_kv, r_kv, s_q, r_q, s_v, r_v, s_a, r_a, s_b, r_b, s_m, r_m, s_g, r_g, s_p, r_p,
                 s_ld, s_t, s_w, s_x, s_wr, s_loc, s_out, s_in, s_r2, s_hu, s_o2, r_o2, s_q2, r_q2, s_kv2, r_kv2, s_ld2, r_ld2):
    me = lax.axis_index('sp')
    t_loc, d = x_hbm.shape
    t_all = t_loc * n
    z = me // 2
    c = lax.rem(me, 2)
    nz = n // 2
    mate = me + 1 - 2 * c
    up = lax.rem(z + 1, nz) * 2 + c
    down = lax.rem(z + nz - 1, nz) * 2 + c
    nd = d // HEAD
    half = HEAD // 2
    sub = t_loc // 4
    last = nz - 2
    ticks = 2 * (nz - 1)
    blk = 2 * t_loc
    nb = t_all // blk
    cexp = HEAD ** -0.5 * LOG2E
    scale = HEAD ** -0.5
    cw = tile.shape[2]
    nt = d // cw
    wr = wrow.shape[2]
    nw = d // wr
    cols = ds(me, HEAD)
    far = sorted(range(1, n), key=lambda e: -min(e, n - e))
    alls = (h_all, gy_all)
    own_src = (hid, gy_hbm)

    again = lax.rem(me, 4) == 0
    sent = lax.rem(me, 4) != 0
    n_sent = n - n // 4
    msg = t_loc // n

    def h2(i):
        return c * (n // 2) + 4 * i

    def w2(act):
        for i in range(2):
            act(pltpu.make_async_copy(wk_ref.at[:, hs(h2(i))], wtile.at[0, :, pl.ds(i * HEAD, HEAD)], s_r2.at[0]))
            act(pltpu.make_async_copy(wv_ref.at[:, hs(h2(i))], wtile.at[1, :, pl.ds(i * HEAD, HEAD)], s_r2.at[0]))
            act(pltpu.make_async_copy(wq_ref.at[:, hs(h2(i))], tile.at[0, pl.ds(0, d), pl.ds(i * HEAD, HEAD)], s_r2.at[1]))
            act(pltpu.make_async_copy(wo_ref.at[hs(h2(i)), :], wrow.at[0, 0, pl.ds(i * HEAD, HEAD), :], s_r2.at[2]))

    def peer(e):
        return lax.rem(me + e, n)

    def rows(i):
        return ds(i, t_loc)

    def hs(i):
        return ds(i, HEAD)

    def chip(s):
        k = nz // 2 - (s + 1) // 2
        return lax.rem(z + nz + jnp.where(lax.rem(s, 2) == 0, -k, k), nz)

    def piece(core, direction, s, u):
        bz = lax.rem(z + nz - 1 - s, nz) if direction == 0 else lax.rem(z + 1 + s, nz)
        return ds((bz * 2 + core) * 4 + 2 * direction + u, sub)

    def ring(a, direction, s, u):
        ref = alls[a]
        bz = lax.rem(z + nz - s, nz) if direction == 0 else lax.rem(z + s, nz)
        rs = ds((bz * 2 + c) * 4 + 2 * direction + u, sub)
        return remote(ref.at[rs, :], ref.at[rs, :], s_ring.at[a], r_ring.at[a, direction, s, u], up if direction == 0 else down)

    def ring0(a, direction, u):
        rs = ds(me * 4 + 2 * direction + u, sub)
        return remote(own_src[a].at[pl.ds((2 * direction + u) * sub, sub), :], alls[a].at[rs, :], s_ring.at[a], r_ring.at[a, direction, 0, u], up if direction == 0 else down)

    def par(a, direction, s, u):
        rs = piece(c, direction, s, u)
        return remote(alls[a].at[rs, :], alls[a].at[rs, :], s_par.at[a], r_par.at[a, 2 * s + u], mate)

    def own_par(a):
        return remote((hid, gy_ref)[a], alls[a].at[rows(me), :], s_par.at[a], r_own.at[a], mate)

    def own_loc(a):
        return pltpu.make_async_copy((hid, gy_ref)[a], alls[a].at[rows(me), :], s_loc.at[0])

    def comm(a, t):
        s = t // 2
        u = lax.rem(t, 2)
        for direction in range(2):
            ring(a, direction, s, u).wait_recv()

            @pl.when(s < last)
            def _():
                ring(a, direction, s + 1, u).start()
            par(a, direction, s, u).start()

    def loads(a, t):
        s = t // 2
        u = lax.rem(t, 2)
        slot = lax.rem(t, 2)
        out = []
        for i, (core, direction) in enumerate(((c, 0), (c, 1), (1 - c, 0), (1 - c, 1))):
            out.append(pltpu.make_async_copy(alls[a].at[piece(core, direction, s, u), :], xbuf.at[slot, pl.ds(i * sub, sub), :], s_ld.at[slot]))
        return out

    def mate_load(a):
        return pltpu.make_async_copy(alls[a].at[rows(mate), :], xbuf.at[1], s_ld.at[1])

    def spots(t):
        s = t // 2
        u = lax.rem(t, 2)
        return [piece(c, 0, s, u), piece(c, 1, s, u), piece(1 - c, 0, s, u), piece(1 - c, 1, s, u)]

    def gather(a, t, work, put):
        @pl.when((t >= a) & (t < ticks))
        def _():
            with scope('comm'):
                comm(a, t)

        @pl.when(t == 0)
        def _():
            own_par(a).wait_recv()
            mate_load(a).start()
            put(work((hid, gy_ref)[a][...]), [rows(me)])

        @pl.when(t == 1)
        def _():
            mate_load(a).wait()
            put(work(xbuf[1]), [rows(mate)])

        @pl.when(t >= 2)
        def _():
            settle(xbuf.at[lax.rem(t, 2)], s_ld.at[lax.rem(t, 2)])
            put(work(xbuf[lax.rem(t, 2)]), spots(t - 2))

        @pl.when((t >= 1) & (t < ticks + 1))
        def _():
            settle(alls[a].at[pl.ds(0, 2 * sub), :], r_par.at[a, t - 1])
            for cp in loads(a, t - 1):
                cp.start()

    def stat_tile(i, act):
        slot = lax.rem(i, 2)
        cs = ds(lax.rem(i, nt), cw)

        @pl.when(i < nt)
        def _():
            act(pltpu.make_async_copy(wq_ref.at[:, cs], wtile.at[slot], s_w.at[slot]))

        @pl.when(i >= nt)
        def _():
            act(pltpu.make_async_copy(wk_ref.at[:, cs], wtile.at[slot], s_w.at[slot]))

    def start(cp):
        cp.start()

    def wait(cp):
        cp.wait()

    def stat_step(i):
        stat_tile(i, wait)

        @pl.when(i + 1 < 2 * nt)
        def _():
            stat_tile(i + 1, start)
        r = dotf(hid[...], wtile[lax.rem(i, 2)], NN)
        w = i // nt
        qkl[w, :, ds(lax.rem(i, nt), cw)] = r
        acc = r[:, :HEAD] * r[:, :HEAD]
        for j in range(1, cw // HEAD):
            acc = acc + r[:, j * HEAD:(j + 1) * HEAD] * r[:, j * HEAD:(j + 1) * HEAD]
        inv[w] = inv[w] + acc

    def st_send(e):
        return remote(mine.at[pl.ds(0, 3)], sall.at[me, pl.ds(0, 3)], s_st.at[0], r_st.at[0], peer(e))

    sgn = jnp.where(lax.broadcasted_iota(jnp.int32, (1, HEAD), 1) < half, -1.0, 1.0).astype(f32)

    def stat_done():
        for w in range(2):
            iv = lax.rsqrt(jnp.sum(inv[w], axis=1, keepdims=True) * (1.0 / d) + NORM_EPS)
            inv[w] = jnp.broadcast_to(iv, (t_loc, HEAD))
            mine[w:w + 1, :] = as_row(iv)
        mine[2:3, :] = pos_ref[...].astype(f32)
        sall[me, 0:3, :] = mine[0:3, :]
        ang = spread_col(pos_ref[...].astype(f32)) * fr_ref[0:1, :]
        cl_s[...] = jnp.cos(ang)
        sl_s[...] = jnp.sin(ang) * (-sgn)

    def spread_col(row):
        return jnp.broadcast_to(row, (HEAD, row.shape[1])).T

    def head_w(i):
        w = (wq_ref, wk_ref, wv_ref)[i]
        return pltpu.make_async_copy(w.at[:, cols], wh.at[:, pl.ds(i * HEAD, HEAD)], s_x.at[0])

    def wo_load():
        return pltpu.make_async_copy(wo_ref.at[cols, :], woh, s_x.at[1])

    with scope('begin'):
        barrier = pltpu.get_barrier_semaphore()
        for to in (up, down, mate):
            pl.semaphore_signal(barrier, inc=1, device_id={'sp': to}, device_id_type=MESH)

        def x_piece(p):
            rs = pl.ds(p * sub, sub)
            return pltpu.make_async_copy(x_hbm.at[rs, :], x_ref.at[rs, :], s_x.at[2 + p])

        smalls = [pltpu.make_async_copy(src, dst, s_in.at[i]) for i, (src, dst) in enumerate(((gn1_hbm, gn1_ref), (gq_hbm, gq_ref), (gk_hbm, gk_ref), (pos_hbm, pos_ref), (fr_hbm, fr_ref)))]
        smalls[0].start()
        for p in (0, 2, 1, 3):
            x_piece(p).start()
        for cp in smalls[1:]:
            cp.start()
        gy_load = pltpu.make_async_copy(gy_hbm, gy_ref, s_x.at[6])
        gy_load.start()
        for i in range(3):
            head_w(i).start()
        wo_load().start()
        stat_tile(0, start)
        pl.semaphore_wait(barrier, 3)
        ring0(1, 0, 0).start()
        ring0(1, 1, 0).start()
        smalls[0].wait()
        g_ref[2:3, :] = gn1_ref[...].astype(f32).reshape(1, d)

        def norm_piece(p):
            rs = pl.ds(p * sub, sub)
            x_piece(p).wait()

            def sq_step(i, acc):
                xf = x_ref[rs, hs(i)].astype(f32)
                return acc + xf * xf

            acc = lax.fori_loop(0, nd, sq_step, jnp.zeros((sub, HEAD), f32))
            xi = lax.rsqrt(jnp.sum(acc, axis=1, keepdims=True) * (1.0 / d) + NORM_EPS)
            xinv[rs, :] = jnp.broadcast_to(xi, (sub, HEAD))

            def hid_step(i):
                hid[rs, hs(i)] = (x_ref[rs, hs(i)].astype(f32) * xi * g_ref[2:3, hs(i)]).astype(bf16)

            loop(0, nd, hid_step)

        for p in (0, 2, 1, 3):
            norm_piece(p)
            ring0(0, p // 2, p % 2).start()
        for cp in smalls[1:]:
            cp.wait()
        for w, src in enumerate((gq_ref, gk_ref)):
            g_ref[w:w + 1, :] = src[...].astype(f32).reshape(1, d)
        zero = jnp.zeros((t_loc, HEAD), f32)
        inv[...] = jnp.zeros_like(inv)
        gy_load.wait()
        own_loc(1).start()
    own_par(0).start()
    own_par(1).start()
    own_loc(0).start()
    settle(wh, s_x.at[0])
    wo_load().wait()

    hb = t_loc // 2

    def finish(s):
        for direction in range(2):
            bz = lax.rem(z + nz - 1 - s, nz) if direction == 0 else lax.rem(z + 1 + s, nz)

            def one(core):
                b = bz * 2 + core
                rs = ds(b * 2 + direction, hb)
                st = sall[b, 0:3, direction * hb:(direction + 1) * hb]
                ang = spread_col(st[2:3, :]) * fr_ref[0:1, :]
                co = jnp.cos(ang)
                si = jnp.sin(ang)
                csT[0, :, rs] = co.T[:half, :]
                csT[1, :, rs] = si.T[:half, :]
                si = si * sgn
                for w, dst in enumerate((q_s, k_s)):
                    hat = raw[w, rs, :] * spread_col(st[w:w + 1, :])
                    hatT[w, :, rs] = hat.T
                    hat = hat * g_ref[w:w + 1, cols]
                    dst[rs, :] = (hat * co + pltpu.roll(hat, half, 1) * si).astype(bf16)
                v_s[rs, :] = raw[2, rs, :].astype(bf16)

            loop(0, 2, one)

    def qkv_work(xv):
        return dotf(xv, wh[...], NN)

    def qkv_put(r, where):
        step = r.shape[0] // len(where)
        for i, rs in enumerate(where):
            for w in range(3):
                raw[w, rs, :] = r[i * step:(i + 1) * step, w * HEAD:(w + 1) * HEAD]

    spt = 2 * nt // 4

    def x_tick(t):
        gather(0, t, qkv_work, qkv_put)

        @pl.when(t == 2 * last - 1)
        def _():
            for direction in range(2):
                ring0(1, direction, 1).start()
            comm(1, 0)

        @pl.when(t < 4)
        def _():
            with scope('stat'):
                loop(t * spt, (t + 1) * spt, stat_step)

        @pl.when(t == 4)
        def _():
            with scope('statdone'):
                stat_done()

        @pl.when(t == 8)
        def _():
            for e in far:
                st_send(e).start()
            w2(start)

        @pl.when(t == 10)
        def _():
            settle(sall.at[pl.ds(0, n - 1), pl.ds(0, 3)], s_st.at[0], r_st.at[0])
        lo = jnp.where(t == 10, -1, jnp.where(t == 11, 1, jnp.where(t >= 12, t - 9, 0)))
        hi = jnp.where(t == 10, 1, jnp.where(t == 11, 3, jnp.where((t >= 12) & (t <= 14), t - 8, -1)))
        with scope('finish'):
            loop(lo, hi, finish)

    with scope('gather_x'):
        loop(0, ticks + 2, x_tick)

    def attend(j):
        qs = ds(j, blk)
        q = q_s[qs, :]

        def unit(kb, carry, masked):
            m, l, acc = carry
            ks = ds(kb, blk)
            s = dotf(q, k_s[ks, :], NT)
            if masked:
                r = lax.broadcasted_iota(jnp.int32, (blk, blk), 0)
                cc = lax.broadcasted_iota(jnp.int32, (blk, blk), 1)
                s = jnp.where(r >= cc, s, -1e30)
            mn = jnp.maximum(m, jnp.max(s, axis=1, keepdims=True))
            al = jnp.exp2((m - mn) * cexp)
            p = jnp.exp2((s - mn) * cexp)
            l = l * al + jnp.sum(p, axis=1, keepdims=True)
            acc = acc * al + dotf(p.astype(bf16), v_s[ks, :], NN)
            return mn, l, acc

        init = (jnp.full((blk, 1), -1e30, f32), jnp.zeros((blk, 1), f32), jnp.zeros((blk, HEAD), f32))
        carry = lax.fori_loop(0, j, functools.partial(unit, masked=False), init)
        m, l, acc = unit(j, carry, True)
        o = acc / l
        raw[2, qs, :] = o
        o_s[qs, :] = o.astype(bf16)
        lse[0:1, qs] = as_row(m * cexp + jnp.log2(l))

    def o_send(e):
        to = peer(e)
        return remote(o_s.at[rows(to), :], att.at[:, cols], s_o.at[0], r_o.at[0], to)

    def h_unit(u):
        return pltpu.make_async_copy(h_all.at[rows(u), :], wrow.at[1, lax.rem(u, 2)], s_hu.at[lax.rem(u, 2)])

    def kv_unit(u):
        h_unit(u).wait()

        @pl.when(u < n - 1)
        def _():
            h_unit(u + 1).start()
        xv = wrow[1, lax.rem(u, 2)]
        rs = rows(u)
        st = sall[u, 0:3, :]
        ang = spread_col(st[2:3, :]) * fr_ref[0:1, :]
        co = jnp.cos(ang)
        si = jnp.sin(ang) * sgn

        def turned(r, w, i):
            hat = r[:, i * HEAD:(i + 1) * HEAD] * spread_col(st[w:w + 1, :]) * g_ref[w:w + 1, hs(h2(i))]
            return (hat * co + pltpu.roll(hat, half, 1) * si).astype(bf16)

        @pl.when(u < 2 * z + 2)
        def _():
            rk = dotf(xv, wtile[0], NN)
            rv = dotf(xv, wtile[1], NN).astype(bf16)
            for i in range(2):
                k2[i, rs, :] = turned(rk, 1, i)
                v2[i, rs, :] = rv[:, i * HEAD:(i + 1) * HEAD]

        @pl.when(u >= 2 * z)
        def _():
            rq = dotf(xv, tile[0, 0:d, :], NN)
            for i in range(2):
                @pl.when(u < 2 * z + 2)
                def _():
                    q2[i, rows(u - 2 * z), :] = turned(rq, 0, i)

                @pl.when(u >= 2 * z + 2)
                def _():
                    k2[i, rs, :] = turned(rq, 0, i)

    def do_again(gv, core):
        r = dotf(gv, wrow[0, 0], NT).astype(bf16)
        for i in range(2):
            do2[i, rows(core), :] = r[:, i * HEAD:(i + 1) * HEAD]

    def do_work(xv):
        return dotf(xv, woh[...], NT).astype(bf16), xv

    def do_put(r, where):
        r, xv = r
        step = r.shape[0] // len(where)
        for i, rs in enumerate(where):
            do_s[rs, :] = r[i * step:(i + 1) * step]
        if len(where) == 4:
            w = dotf(xv, wrow[0, 0], NT).astype(bf16)
            for j, rs in enumerate(where):
                @pl.when(rs.start >= 2 * t_loc * (z + 1))
                def _():
                    for i in range(2):
                        v2[i, rs, :] = w[j * step:(j + 1) * step, i * HEAD:(i + 1) * HEAD]

    def y_tick(t):
        gather(1, t, do_work, do_put)

        @pl.when(t == 1)
        def _():
            with scope('finish'):
                finish(last)
        t = t - 1
        lo = jnp.where(t == 0, 0, jnp.where(t <= 4, t + 1, jnp.where(t <= 6, 6, 7)))
        hi = jnp.where(t == 0, 2, jnp.where(t <= 4, t + 2, jnp.where(t == 5, 6, jnp.where(t == 8, 8, 7))))
        hi = jnp.where(t < 0, 0, hi)
        with scope('attend'):
            loop(lo, hi, attend)

        @pl.when((t == ticks - 3) & sent)
        def _():
            for e in far[-5:]:
                o_send(e).start()

        @pl.when((t == ticks - 2) & sent)
        def _():
            for e in far[:-5]:
                o_send(e).start()

        @pl.when(t == -1)
        def _():
            settle(wrow.at[0, 0], s_r2.at[2])
            do_again(gy_ref[...], c)
            settle(h_all.at[pl.ds(0, 2 * t_loc), :], s_loc.at[0])
            h_unit(0).start()
            settle(wtile, s_r2.at[0])
            settle(tile.at[0, pl.ds(0, d), :], s_r2.at[1])

        @pl.when(t == 0)
        def _():
            do_again(xbuf[1], 1 - c)
        first = jnp.where(t == 1, 0, jnp.where(t == 2, 1, jnp.where(t == 5, 2, jnp.where(t == 7, 5, jnp.where(t == 9, 8, jnp.where(t == 10, 11, jnp.where(t == 11, 14, 16)))))))
        count = jnp.where((t == 1) | (t == 2), 1, jnp.where((t == 5) | (t == 7) | (t == 9) | (t == 10), 3, jnp.where(t == 11, 2, 0)))
        with scope('again_kv'):
            loop(first, first + count, kv_unit)

    with scope('gather_y'):
        loop(0, ticks + 2, y_tick)

    def gy_copy(t):
        return pltpu.make_async_copy(gy_all.at[:, ds(t, cw)], tile.at[lax.rem(t, 2)], s_t.at[lax.rem(t, 2)])

    def h_copy(t):
        return pltpu.make_async_copy(h_all.at[:, ds(lax.rem(t, nt), cw)], tile.at[lax.rem(t, 2)], s_t.at[lax.rem(t, 2)])

    def h2_copy(t):
        return pltpu.make_async_copy(h_all.at[:, ds(chip(t), cw)], tile.at[lax.rem(t, 2)], s_t.at[lax.rem(t, 2)])

    def wo_copy(t):
        return pltpu.make_async_copy(wo_ref.at[:, ds(t, cw)], wtile.at[lax.rem(t, 2)], s_w.at[lax.rem(t, 2)])

    def q_send(e):
        to = peer(e)
        return remote(dq_s.at[rows(to), :], tq.at[:, cols], s_q.at[0], r_q.at[0], to)

    def kv_send(to):
        return remote(dkv.at[to], tkv.at[:, :, cols], s_kv.at[0], r_kv.at[0], to)

    gy_copy(0).start()
    wo_copy(0).start()
    settle(h_all.at[pl.ds(0, (nz - 1) * t_loc), :], s_ring.at[0])
    settle(h_all.at[pl.ds(0, nz * t_loc), :], s_par.at[0])

    @pl.when(sent)
    def _():
        att[:, cols] = o_s[rows(me), :]
    raw[0] = jnp.zeros((t_all, HEAD), f32)

    def delta(j):
        qs = ds(j, blk)
        lse[1:2, qs] = as_row(jnp.sum(raw[2, qs, :] * do_s[qs, :].astype(f32), axis=1, keepdims=True))

    with scope('delta'):
        loop(0, nb, delta)

    home = me // (n // 2)
    slot2 = lax.rem(me, n // 2) // 4
    mine_too = again & (home == c)

    def ld_send(k):
        to = lax.rem(z + k, nz) * 2 + home
        return remote(lse.at[pl.ds(0, 2)], ld2.at[slot2, pl.ds(0, 2)], s_ld2.at[0], r_ld2.at[0], to)

    @pl.when(again)
    def _():
        for k in (4, 3, 5, 2, 6, 1, 7):
            ld_send(k).start()

    @pl.when(again & (home != c))
    def _():
        ld_send(0).start()

    @pl.when(mine_too)
    def _():
        ld2[slot2, 0:2, :] = lse[0:2, :]

    def bwd_step(s):
        kb = chip(s)
        ks = ds(kb, blk)
        k = k_s[ks, :]
        v = v_s[ks, :]

        def unit(qb, carry, masked):
            dk, dv = carry
            qs = ds(qb, blk)
            q = q_s[qs, :]
            do = do_s[qs, :]
            p = jnp.exp2(dotf(k, q, NT) * cexp - lse[0:1, qs])
            if masked:
                r = lax.broadcasted_iota(jnp.int32, (blk, blk), 0)
                cc = lax.broadcasted_iota(jnp.int32, (blk, blk), 1)
                p = jnp.where(cc >= r, p, 0.0)
            g = (p * (dotf(v, do, NT) - lse[1:2, qs])).astype(bf16)
            dv = dv + dotf(p.astype(bf16), do, NN)
            dk = dk + dotf(g, q, NN)
            raw[0, qs, :] = raw[0, qs, :] + dotf(g, k, TN)
            return dk, dv

        zk = jnp.zeros((blk, HEAD), f32)
        carry = unit(kb, (zk, zk), True)
        dk, dv = lax.fori_loop(kb + 1, nb, functools.partial(unit, masked=False), carry)
        dk = (dk * scale).astype(bf16)
        dv = dv.astype(bf16)
        for u in range(2):
            dkv[2 * kb + u, 0] = dk[u * t_loc:(u + 1) * t_loc]
            dkv[2 * kb + u, 1] = dv[u * t_loc:(u + 1) * t_loc]

        @pl.when((kb != z) & sent)
        def _():
            for u in range(2):
                kv_send(2 * kb + u).start()

        @pl.when((kb == z) & sent)
        def _():
            kv_send(mate).start()

    with scope('bwd'):
        loop(0, nb, bwd_step)
        dq_s[...] = (raw[0] * scale).astype(bf16)
    gcol = [spread_col(g_ref[w:w + 1, cols])[:, 0:1] for w in range(2)]

    def unroped(src, js):
        ct = csT[0, :, js]
        sn = csT[1, :, js]
        t = src.astype(f32).T
        p, r = t[:half], t[half:]
        return jnp.concatenate([p * ct + r * sn, r * ct - p * sn], axis=0)

    def share_step(j, carry):
        js = rows(j)
        res = []
        for w, src in enumerate((dq_s[js, :], dkv[j, 0])):
            th = unroped(src, js) * hatT[w, :, js]
            res.append(carry[w] + th)
            pm[j, w:w + 1, :] = jnp.sum(th * gcol[w], axis=0, keepdims=True)
        return tuple(res)

    def p_send(e):
        to = peer(e)
        return remote(pm.at[to, pl.ds(0, 2)], pall.at[me, pl.ds(0, 2)], s_p.at[0], r_p.at[0], to)

    with scope('share'):
        zt = jnp.zeros((HEAD, t_loc), f32)
        sums = lax.fori_loop(0, n, share_step, (zt, zt))
    for e in far:
        p_send(e).start()
    @pl.when(sent)
    def _():
        for e in far:
            q_send(e).start()
        tq[:, cols] = dq_s[rows(me), :]
        tkv[:, :, cols] = dkv[me]

    pall[me, 0:2, :] = pm[me, 0:2, :]
    for w in range(2):
        gg_s[w] = jnp.broadcast_to(jnp.sum(sums[w], axis=1, keepdims=True), (HEAD, HEAD)).T[0:8, :]

    def flip_o(i):
        rawT[0:HEAD, rows(i)] = o_s[rows(i), :].T

    def flip_v(i):
        rawT[0:HEAD, rows(i)] = dkv[i, 1].T

    def dwo_step(t):
        gy_copy(t).wait()

        @pl.when(t + 1 < nt)
        def _():
            gy_copy(t + 1).start()

        @pl.when(t + 1 == nt)
        def _():
            h_copy(t + 1).start()
        r = dotf(rawT[0:HEAD, :], tile[lax.rem(t, 2)], NN)
        for u in range(cw // HEAD):
            raw[2, hs(n + t * (cw // HEAD) + u), :] = r[:, u * HEAD:(u + 1) * HEAD]

    def dwv_step(t):
        h_copy(t).wait()

        @pl.when(t + 1 < 2 * nt)
        def _():
            h_copy(t + 1).start()

        @pl.when(t + 1 == 2 * nt)
        def _():
            h2_copy(0).start()
        r = dotf(rawT[0:HEAD, :], tile[lax.rem(t, 2)], NN)
        for u in range(cw // HEAD):
            raw[2, hs((t - nt) * (cw // HEAD) + u), :] = r[:, u * HEAD:(u + 1) * HEAD].T

    def y_step(t):
        wo_copy(t).wait()

        @pl.when(t + 1 < nt)
        def _():
            wo_copy(t + 1).start()
        cs = ds(t, cw)
        hid[:, cs] = (x_ref[:, cs].astype(f32) + dotf(att[...], wtile[lax.rem(t, 2)], NN)).astype(bf16)

    def v_send(e):
        to = peer(e)
        return remote(raw.at[2, hs(to), :], dwv_out.at[:, cols], s_v.at[0], r_v.at[0], to)

    def out(i):
        src, dst, k = ((hid, y_out, 0), None, (xbuf.at[0], gx_out, 0), (raw.at[2, hs(me), :], dwv_out.at[:, cols], 2),
                       (raw.at[1, rows_f(0, me), :], dwq_out.at[:, cols], 2), (raw.at[1, rows_f(1, me), :], dwk_out.at[:, cols], 2),
                       (gg_s, gg_out, 3), (gpart.at[me], gall.at[me], 4))[i]
        return pltpu.make_async_copy(src, dst, s_out.at[k])

    def rows_f(w, to):
        return ds(w * n + to, HEAD)

    with scope('dwo'):
        loop(0, n, flip_o)
        loop(0, nt, dwo_step)
        for j in range(n):
            pltpu.make_async_copy(raw.at[2, pl.ds((n + j) * HEAD, HEAD), :], dwo_out.at[:, pl.ds(j * HEAD, HEAD)], s_out.at[1]).start()

    def m_send(e):
        return remote(mine2.at[pl.ds(0, 2)], mall.at[me, pl.ds(0, 2)], s_m.at[0], r_m.at[0], peer(e))

    with scope('dwv'):
        loop(0, n, flip_v)
        loop(nt, 2 * nt, dwv_step)
        out(3).start()
    with scope('pwait'):
        settle(pall.at[pl.ds(0, n - 1), pl.ds(0, 2)], s_p.at[0], r_p.at[0])
        tot = pall[0, 0:2, :]
        for j in range(1, n):
            tot = tot + pall[j, 0:2, :]
        mine2[0:2, :] = tot * (1.0 / d)
    for e in far:
        m_send(e).start()
    mall[me, 0:2, :] = mine2[0:2, :]
    for e in far:
        v_send(e).start()
    def got(buf, s_sem, r_sem):
        @pl.when(sent)
        def _():
            settle(buf.at[pl.ds(0, (n - 1) * msg), :], s_sem.at[0])
            settle(buf.at[pl.ds(0, (n_sent - 1) * msg), :], r_sem.at[0])

        @pl.when(again)
        def _():
            settle(buf.at[pl.ds(0, n_sent * msg), :], r_sem.at[0])

    def o2_send(i):
        return remote(o2.at[i, rows(1 - c), :], att.at[:, hs(h2(i))], s_o2.at[0], r_o2.at[0], mate)

    def q2_send(i):
        return remote(dq2.at[i, rows(1 - c), :], tq.at[:, hs(h2(i))], s_q2.at[0], r_q2.at[0], mate)

    def again_head(i):
        q = q2[i]
        do = do2[i]
        r0 = lax.broadcasted_iota(jnp.int32, (blk, blk), 0)
        c0 = lax.broadcasted_iota(jnp.int32, (blk, blk), 1)

        def unit(kb, carry, masked):
            m, l, acc = carry
            ks = ds(kb, blk)
            s = dotf(q, k2[i, ks, :], NT)
            if masked:
                s = jnp.where(r0 >= c0, s, -1e30)
            mn = jnp.maximum(m, jnp.max(s, axis=1, keepdims=True))
            al = jnp.exp2((m - mn) * cexp)
            p = jnp.exp2((s - mn) * cexp)
            l = l * al + jnp.sum(p, axis=1, keepdims=True)
            acc = acc * al + dotf(p.astype(bf16), v2[i, ks, :], NN)
            return mn, l, acc

        init = (jnp.full((blk, 1), -1e30, f32), jnp.zeros((blk, 1), f32), jnp.zeros((blk, HEAD), f32))
        m, l, acc = unit(z, lax.fori_loop(0, z, functools.partial(unit, masked=False), init), True)
        o = acc / l
        o2[i] = o.astype(bf16)
        ls = m * cexp + jnp.log2(l)
        de = jnp.sum(o * do.astype(f32), axis=1, keepdims=True)

        def unit2(kb, dq, masked):
            ks = ds(kb, blk)
            k = k2[i, ks, :]
            p = jnp.exp2(dotf(q, k, NT) * cexp - ls)
            if masked:
                p = jnp.where(r0 >= c0, p, 0.0)
            g = (p * (dotf(do, v2[i, ks, :], NT) - de)).astype(bf16)
            return dq + dotf(g, k, NN)

        dq = unit2(z, lax.fori_loop(0, z, functools.partial(unit2, masked=False), jnp.zeros((blk, HEAD), f32)), True)
        dq2[i] = (dq * scale).astype(bf16)

        k = k2[i, ds(z, blk), :]
        v = v2[i, ds(z, blk), :]

        def unit3(carry, qq, dd, qb, masked):
            dk, dv = carry
            qs = ds(qb, blk)
            p = jnp.exp2(dotf(k, qq, NT) * cexp - ld2[i, 0:1, qs])
            if masked:
                p = jnp.where(c0 >= r0, p, 0.0)
            g = (p * (dotf(v, dd, NT) - ld2[i, 1:2, qs])).astype(bf16)
            return dk + dotf(g, qq, NN), dv + dotf(p.astype(bf16), dd, NN)

        def later(qb, carry):
            qs = ds(qb, blk)
            return unit3(carry, k2[i, qs, :], v2[i, qs, :], qb, False)

        zk = jnp.zeros((blk, HEAD), f32)
        dk, dv = lax.fori_loop(z + 1, nb, later, unit3((zk, zk), q, do, z, True))
        dkv2[i, 0] = (dk * scale).astype(bf16)
        dkv2[i, 1] = dv.astype(bf16)
        for w in range(2):
            tkv[w, :, hs(h2(i))] = dkv2[i, w, rows(c), :]
        att[:, hs(h2(i))] = o2[i, rows(c), :]
        tq[:, hs(h2(i))] = dq2[i, rows(c), :]

    def kv2_send(i):
        return remote(dkv2.at[i, :, rows(1 - c), :], tkv.at[:, :, hs(h2(i))], s_kv2.at[0], r_kv2.at[0], mate)

    pair = ld2.at[pl.ds(0, 1), pl.ds(0, 2)]
    with scope('ldwait'):
        @pl.when(mine_too)
        def _():
            settle(pair, r_ld2.at[0])
            settle(ld2.at[:, pl.ds(0, nz - 1)], s_ld2.at[0])

        @pl.when(jnp.logical_not(mine_too))
        def _():
            settle(ld2.at[:, pl.ds(0, 2)], r_ld2.at[0])

        @pl.when(again & (home != c))
        def _():
            settle(ld2.at[:, pl.ds(0, nz)], s_ld2.at[0])
    with scope('again'):
        loop(0, 2, again_head)
        for i in range(2):
            o2_send(i).start()
            q2_send(i).start()
            kv2_send(i).start()

    def w_copies(t):
        slot = lax.rem(t, 2)
        return [pltpu.make_async_copy(w.at[ds(t, wr), :], wrow.at[slot, i], s_wr.at[slot]) for i, w in enumerate((wq_ref, wk_ref, wv_ref))]

    for cp in w_copies(0):
        cp.start()
    cl = cl_s[...]
    sl = sl_s[...]

    def back_rope(a):
        a = a.astype(f32)
        return a * cl + pltpu.roll(a, half, 1) * sl

    def loc_step(i):
        tq[:, hs(i)] = (inv[0] * (back_rope(tq[:, hs(i)]) * g_ref[0:1, hs(i)] - qkl[0, :, hs(i)] * inv[0] * mq)).astype(bf16)
        tkv[0, :, hs(i)] = (inv[1] * (back_rope(tkv[0, :, hs(i)]) * g_ref[1:2, hs(i)] - qkl[1, :, hs(i)] * inv[1] * mk)).astype(bf16)

    with scope('mwait'):
        settle(mall.at[pl.ds(0, n - 1), pl.ds(0, 2)], s_m.at[0], r_m.at[0])

    def head_step(j):
        js = rows(j)
        for w, src in enumerate((dq_s[js, :], dkv[j, 0])):
            rawT[w * HEAD:(w + 1) * HEAD, js] = (sall[j, w:w + 1, :] * (unroped(src, js) * gcol[w] - hatT[w, :, js] * mall[j, w:w + 1, :])).astype(bf16)

    with scope('head'):
        loop(0, n, head_step)

    def a_send(to):
        return remote(raw.at[1, rows_f(0, to), :], dwq_out.at[:, cols], s_a.at[0], r_a.at[0], to)

    def b_send(to):
        return remote(raw.at[1, rows_f(1, to), :], dwk_out.at[:, cols], s_b.at[0], r_b.at[0], to)

    def dw_step(t):
        h2_copy(t).wait()

        @pl.when(t + 1 < nt)
        def _():
            h2_copy(t + 1).start()
        nn = chip(t)
        r = dotf(rawT[...], tile[lax.rem(t, 2)], NN)
        for u in range(cw // HEAD):
            to = nn * (cw // HEAD) + u
            for w in range(2):
                raw[1, rows_f(w, to), :] = r[w * HEAD:(w + 1) * HEAD, u * HEAD:(u + 1) * HEAD].T

            @pl.when(to != me)
            def _():
                a_send(to).start()
                b_send(to).start()

    with scope('dw'):
        loop(0, nt // 2, dw_step)
    with scope('waitkv'):
        @pl.when(sent)
        def _():
            settle(tkv.at[:, pl.ds(0, (n - 1) * msg), :], s_kv.at[0])
            settle(tkv.at[:, pl.ds(0, (n_sent - 1) * msg), :], r_kv.at[0])

        @pl.when(again)
        def _():
            settle(tkv.at[:, pl.ds(0, n_sent * msg), :], r_kv.at[0])
        settle(tkv.at[:, pl.ds(0, 2 * msg), :], s_kv2.at[0], r_kv2.at[0])
    with scope('waitq'):
        got(tq, s_q, r_q)
        settle(tq.at[pl.ds(0, 2 * msg), :], s_q2.at[0], r_q2.at[0])

    mq = spread_col(mine2[0:1, :])
    mk = spread_col(mine2[1:2, :])
    with scope('loc'):
        loop(0, nd, loc_step)

    def dh_step(t):
        settle(wrow.at[lax.rem(t, 2)], s_wr.at[lax.rem(t, 2)])

        @pl.when(t + 1 < nw)
        def _():
            for cp in w_copies(t + 1):
                cp.start()
        slot = lax.rem(t, 2)
        r = dotf(tq[...], wrow[slot, 0], NT) + dotf(tkv[0], wrow[slot, 1], NT) + dotf(tkv[1], wrow[slot, 2], NT)
        dh[:, ds(t, wr)] = r.astype(bf16).astype(f32)

    with scope('dh'):
        loop(0, nw, dh_step)

    def mx_step(i, acc):
        return acc + dh[:, hs(i)] * g_ref[2:3, hs(i)] * x_ref[:, hs(i)].astype(f32)

    def g_send(e):
        return remote(gpart.at[peer(e), pl.ds(0, 1)], gall.at[me, pl.ds(0, 1)], s_g.at[0], r_g.at[0], peer(e))

    with scope('gx'):
        mx = jnp.sum(lax.fori_loop(0, nd, mx_step, zero), axis=1, keepdims=True) * (1.0 / d) * xinv[...]

        def gx_step(i):
            xh = x_ref[:, hs(i)].astype(f32) * xinv[...]
            dhh = dh[:, hs(i)]
            gpart[i] = jnp.broadcast_to(jnp.sum(dhh * xh, axis=0, keepdims=True), (8, HEAD))
            xbuf[0, :, hs(i)] = (gy_ref[:, hs(i)].astype(f32) + xinv[...] * (dhh * g_ref[2:3, hs(i)] - xh * mx)).astype(bf16)

        loop(0, nd, gx_step)
        out(2).start()
    for e in far:
        g_send(e).start()
    out(7).start()
    out(6).start()
    with scope('dw2'):
        loop(nt // 2, nt, dw_step)
        out(4).start()
        out(5).start()
    with scope('y'):
        got(att, s_o, r_o)
        settle(att.at[pl.ds(0, 2 * msg), :], s_o2.at[0], r_o2.at[0])
        loop(0, nt, y_step)
        out(0).start()
    with scope('end_drain'):
        settle(gy_all.at[pl.ds(0, (nz - 1) * t_loc), :], s_ring.at[1])
        settle(gy_all.at[pl.ds(0, nz * t_loc), :], s_par.at[1])
        settle(tkv, s_out.at[0])
        settle(raw.at[2, pl.ds(0, n * HEAD), :], s_out.at[1])
        settle(raw.at[2, pl.ds(0, 3 * HEAD), :], s_out.at[2])
        settle(gg_s, s_out.at[3])
        settle(gpart.at[0], s_out.at[4])
    most = pl.ds(0, HEAD - HEAD // n)
    with scope('end_v'):
        settle(dwv_out.at[most, :], s_v.at[0], r_v.at[0])
    with scope('end_a'):
        settle(dwq_out.at[most, :], s_a.at[0], r_a.at[0])
    with scope('end_b'):
        settle(dwk_out.at[most, :], s_b.at[0], r_b.at[0])
    with scope('end_g'):
        settle(gall.at[pl.ds(0, n - 1), pl.ds(0, 1)], s_g.at[0], r_g.at[0])


def block(n, x, gy, pos, gq, gk, gn, freq, wq, wk, wv, wo):
    t_loc, d = x.shape
    t_all = t_loc * n
    hb = pl.BlockSpec(memory_space=pl.ANY)
    S = jax.ShapeDtypeStruct
    V = pltpu.VMEM
    sem = pltpu.SemaphoreType.DMA
    hd = (t_all, HEAD)
    tok = (t_loc, d)
    nz = n // 2
    return pl.pallas_call(functools.partial(block_kernel, n),
        in_specs=[hb] * 11,
        out_specs=[hb] * 10,
        out_shape=[S(tok, bf16), S(tok, bf16), S((n, 8, d // n), f32)] + [S((d // n, d), f32)] * 4 + [S((2, 8, HEAD), f32), S((t_all, d), bf16), S((t_all, d), bf16)],
        scratch_shapes=[V((1, t_loc), jnp.int32), V((d,), bf16), V((d,), bf16), V((d,), bf16), V((8, HEAD), f32), V(tok, bf16), V(tok, bf16), V((8, d), f32), V(tok, bf16), V((d, 3 * HEAD), bf16), V((HEAD, d), bf16), V((3,) + hd, f32), V((2,) + tok, bf16), V((2, d, 2 * HEAD), bf16), V((2, t_all, 2 * HEAD), bf16), V((2, 3, 2 * HEAD, d), bf16),
            V((2,) + tok, f32), V((2, HEAD, t_all), f32), V((2, HEAD // 2, t_all), f32)] + [V(hd, bf16)] * 5 + [V((8, t_all), f32), V((2, 8, t_all), f32)]
        + [V(hd, bf16), V((n, 2, t_loc, HEAD), bf16), V(tok, bf16), V((2,) + tok, bf16), V(tok, bf16), V((2 * HEAD, t_all), bf16), V(tok, f32),
            V((t_loc, HEAD), f32), V((t_loc, HEAD), f32), V((2, t_loc, HEAD), f32), V((t_loc, HEAD), f32), V((8, t_loc), f32), V((n, 8, t_loc), f32), V((8, t_loc), f32), V((n, 8, t_loc), f32), V((n, 8, t_loc), f32), V((n, 8, t_loc), f32), V((n, 8, d // n), f32), V((2, 8, HEAD), f32)] + [V((2, t_all, HEAD), bf16)] * 2 + [V((2, 2 * t_loc, HEAD), bf16)] * 4 + [V((2, 2, 2 * t_loc, HEAD), bf16)]
        + [sem((2,)), sem((2, 2, nz - 1, 2)), sem((2,)), sem((2, 2 * (nz - 1))), sem((2,))] + [sem((1,))] * 20
        + [sem((2,)), sem((2,)), sem((2,)), sem((7,)), sem((2,)), sem((1,)), sem((5,)), sem((5,)), sem((3,)), sem((2,))] + [sem((1,))] * 8,
        compiler_params=pltpu.CompilerParams(collective_id=1, has_side_effects=True, vmem_limit_bytes=67043328), name='block')(x, gy, pos, gq, gk, gn, freq, wq, wk, wv, wo)


def copy_kernel(*refs):
    k = (len(refs) - 2) // 3
    src, dst, buf, si, so = list(refs[:k - 1]), refs[k - 1:2 * k - 1], refs[2 * k - 1:3 * k - 1], refs[-2], refs[-1]
    parts = src[k - 3]
    src[k - 3:] = [parts, src[k - 2].at[0, 0:1, :], src[k - 2].at[1, 0:1, :]]
    buf = list(buf)
    total = buf[k - 3]
    buf[k - 3] = refs[-3]
    ins = [pltpu.make_async_copy(src[i], buf[i], si.at[i]) for i in range(k)]
    outs = [pltpu.make_async_copy(buf[i], dst[i], so.at[i]) if i != k - 3 else None for i in range(k)]
    for cp in ins:
        cp.start()
    outs[k - 3] = pltpu.make_async_copy(total, dst[k - 3], so.at[k - 3])
    for i in range(k):
        ins[i].wait()
        if i == k - 3:
            total[...] = jnp.sum(refs[-3][:, 0:1, :], axis=0)
        outs[i].start()
    for cp in outs:
        cp.wait()


def copy_out(arrays):
    hb = pl.BlockSpec(memory_space=pl.ANY)
    shapes = [(a.shape, a.dtype) for a in arrays[:-2]] + [((1, HEAD), f32)] * 3
    k = len(shapes)
    return pl.pallas_call(copy_kernel, in_specs=[hb] * len(arrays), out_specs=[hb] * k, out_shape=[jax.ShapeDtypeStruct(*a) for a in shapes],
        scratch_shapes=[pltpu.VMEM(*a) for a in shapes] + [pltpu.VMEM(arrays[-2].shape, f32)] + [pltpu.SemaphoreType.DMA((k,))] * 2, name='copy_out')(*arrays)


def solution(mesh):
    n = mesh.shape['sp']

    def device_step(x_in, grad_y, positions, g_norm, wq, wk, wv, wo, gq, gk):
        half = HEAD // 2
        inv_freq = ROPE_BASE ** (-np.arange(half) * (2.0 / HEAD))
        freq = jnp.asarray(np.tile(inv_freq, (8, 2)), f32)
        y, gx, gn, dwq, dwk, dwv, dwo, gg, _, _ = block(n, x_in[0], grad_y[0], positions, gq, gk, g_norm, freq, wq, wk, wv, wo)
        y, gx, dwq, dwk, dwv, dwo, gn, ggq, ggk = copy_out([y, gx, dwq, dwk, dwv, dwo, gn, gg])
        return (y[None], gx[None], gn[0], dwq, dwk, dwv, dwo, ggq[0], ggk[0])

    seq_spec = P('dp', 'sp', None)
    rep2, rep1 = P(None, None), P(None)
    row_spec, vec_spec = P(('dp', 'sp'), None), P(('dp', 'sp'))
    return jax.shard_map(device_step, mesh=mesh, in_specs=(seq_spec, seq_spec, P('dp', 'sp'), rep1, rep2, rep2, rep2, rep2, rep1, rep1), out_specs=(seq_spec, seq_spec, vec_spec, row_spec, row_spec, row_spec, row_spec, vec_spec, vec_spec), check_vma=False)
```

```python
import contextlib
import functools
import jax
import jax.numpy as jnp
import numpy as np
from jax import lax
from jax.experimental import pallas as pl
from jax.experimental.pallas import tpu as pltpu
from jax.sharding import PartitionSpec as P

HEAD = 128
NORM_EPS = 1e-5
ROPE_BASE = 10000.0
LOG2E = 1.4426950408889634
f32 = jnp.float32
bf16 = jnp.bfloat16
MESH = pl.DeviceIdType.MESH
NN = (((1,), (0,)), ((), ()))
NT = (((1,), (1,)), ((), ()))
TN = (((0,), (0,)), ((), ()))
PROF = 0
scope = jax.named_scope if PROF else (lambda name: contextlib.nullcontext())


def dotf(a, b, dims):
    return lax.dot_general(a, b, dims, preferred_element_type=f32)


def remote(src, dst, ss, rs, to):
    return pltpu.make_async_remote_copy(src_ref=src, dst_ref=dst, send_sem=ss, recv_sem=rs, device_id={'sp': to}, device_id_type=MESH)


def ds(i, size):
    return pl.ds(pl.multiple_of(i * size, size), size)


def settle(ref, *sems):
    for sem in sems:
        pltpu.make_async_copy(ref, ref, sem).wait()


def as_row(col):
    return jnp.broadcast_to(col, (col.shape[0], HEAD)).T[0:1, :]


def loop(lo, hi, body):
    def step(i, carry):
        body(i)
        return carry
    lax.fori_loop(lo, hi, step, 0)


def block_kernel(n, x_hbm, gy_hbm, pos_hbm, gq_hbm, gk_hbm, gn1_hbm, fr_hbm, wq_ref, wk_ref, wv_ref, wo_ref,
                 y_out, gx_out, gall, dwq_out, dwk_out, dwv_out, dwo_out, gg_out, h_all, gy_all,
                 pos_ref, gq_ref, gk_ref, gn1_ref, fr_ref, x_ref, gy_ref, g_ref, hid, wh, woh, raw, xbuf, wtile, tile, wrow, qkl, hatT, csT, q_s, k_s, v_s, do_s, o_s, lse, ld2,
                 dq_s, dkv, tq, tkv, att, rawT, dh, cl_s, sl_s, inv, xinv, mine, sall, mine2, mall, pm, pall, gpart, gg_s, k2, v2, q2, do2, o2, dq2, dkv2,
                 s_ring, r_ring, s_par, r_par, r_own, s_st, r_st, s_o, r_o, s_kv, r_kv, s_q, r_q, s_v, r_v, s_a, r_a, s_b, r_b, s_m, r_m, s_g, r_g, s_p, r_p,
                 s_ld, s_t, s_w, s_x, s_wr, s_loc, s_out, s_in, s_r2, s_hu, s_o2, r_o2, s_q2, r_q2, s_kv2, r_kv2, s_ld2, r_ld2, s_w4):
    me = lax.axis_index('sp')
    t_loc, d = x_hbm.shape
    t_all = t_loc * n
    z = me // 2
    c = lax.rem(me, 2)
    nz = n // 2
    mate = me + 1 - 2 * c
    up = lax.rem(z + 1, nz) * 2 + c
    down = lax.rem(z + nz - 1, nz) * 2 + c
    nd = d // HEAD
    half = HEAD // 2
    sub = t_loc // 4
    last = nz - 2
    ticks = 2 * (nz - 1)
    blk = 2 * t_loc
    nb = t_all // blk
    cexp = HEAD ** -0.5 * LOG2E
    scale = HEAD ** -0.5
    cw = tile.shape[2]
    nt = d // cw
    wr = wrow.shape[2]
    nw = d // wr
    cols = ds(me, HEAD)
    far = sorted(range(1, n), key=lambda e: -min(e, n - e))
    alls = (h_all, gy_all)
    own_src = (hid, gy_hbm)

    again = c == 0
    sent = c == 1
    n_sent = n - n // 4
    msg = t_loc // n

    def h2(i):
        return 2 * lax.rem(z, 2) + c * (n // 2) + 4 * i

    def to_send(to):
        return sent | (lax.rem(to // 2 + z, 2) == 1)

    def send_all(make, es):
        for e in es:
            @pl.when(to_send(peer(e)))
            def _():
                make(e).start()

    def w2(act):
        for i in range(2):
            act(pltpu.make_async_copy(wk_ref.at[:, hs(h2(i))], wtile.at[0, :, pl.ds(i * HEAD, HEAD)], s_r2.at[0]))
            act(pltpu.make_async_copy(wv_ref.at[:, hs(h2(i))], wtile.at[1, :, pl.ds(i * HEAD, HEAD)], s_r2.at[0]))
            act(pltpu.make_async_copy(wq_ref.at[:, hs(h2(i))], tile.at[0, pl.ds(0, d), pl.ds(i * HEAD, HEAD)], s_r2.at[1]))
            act(pltpu.make_async_copy(wo_ref.at[hs(h2(i)), :], wrow.at[0, 0, pl.ds(i * HEAD, HEAD), :], s_r2.at[2]))

    def peer(e):
        return lax.rem(me + e, n)

    def rows(i):
        return ds(i, t_loc)

    def hs(i):
        return ds(i, HEAD)

    def chip(s):
        k = nz // 2 - (s + 1) // 2
        return lax.rem(z + nz + jnp.where(lax.rem(s, 2) == 0, -k, k), nz)

    def piece(core, direction, s, u):
        bz = lax.rem(z + nz - 1 - s, nz) if direction == 0 else lax.rem(z + 1 + s, nz)
        return ds((bz * 2 + core) * 4 + 2 * direction + u, sub)

    def ring(a, direction, s, u):
        ref = alls[a]
        bz = lax.rem(z + nz - s, nz) if direction == 0 else lax.rem(z + s, nz)
        rs = ds((bz * 2 + c) * 4 + 2 * direction + u, sub)
        return remote(ref.at[rs, :], ref.at[rs, :], s_ring.at[a], r_ring.at[a, direction, s, u], up if direction == 0 else down)

    def ring0(a, direction, u):
        rs = ds(me * 4 + 2 * direction + u, sub)
        return remote(own_src[a].at[pl.ds((2 * direction + u) * sub, sub), :], alls[a].at[rs, :], s_ring.at[a], r_ring.at[a, direction, 0, u], up if direction == 0 else down)

    def par(a, direction, s, u):
        rs = piece(c, direction, s, u)
        return remote(alls[a].at[rs, :], alls[a].at[rs, :], s_par.at[a], r_par.at[a, 2 * s + u], mate)

    def own_par(a):
        return remote((hid, gy_ref)[a], alls[a].at[rows(me), :], s_par.at[a], r_own.at[a], mate)

    def own_loc(a):
        return pltpu.make_async_copy((hid, gy_ref)[a], alls[a].at[rows(me), :], s_loc.at[0])

    def comm(a, t):
        s = t // 2
        u = lax.rem(t, 2)
        for direction in range(2):
            ring(a, direction, s, u).wait_recv()

            @pl.when(s < last)
            def _():
                ring(a, direction, s + 1, u).start()
            par(a, direction, s, u).start()

    def loads(a, t):
        s = t // 2
        u = lax.rem(t, 2)
        slot = lax.rem(t, 2)
        out = []
        for i, (core, direction) in enumerate(((c, 0), (c, 1), (1 - c, 0), (1 - c, 1))):
            out.append(pltpu.make_async_copy(alls[a].at[piece(core, direction, s, u), :], xbuf.at[slot, pl.ds(i * sub, sub), :], s_ld.at[slot]))
        return out

    def mate_load(a):
        return pltpu.make_async_copy(alls[a].at[rows(mate), :], xbuf.at[1], s_ld.at[1])

    def spots(t):
        s = t // 2
        u = lax.rem(t, 2)
        return [piece(c, 0, s, u), piece(c, 1, s, u), piece(1 - c, 0, s, u), piece(1 - c, 1, s, u)]

    def gather(a, t, work, put):
        @pl.when((t >= a) & (t < ticks))
        def _():
            with scope('comm'):
                comm(a, t)

        @pl.when(t == 0)
        def _():
            own_par(a).wait_recv()
            mate_load(a).start()
            put(work((hid, gy_ref)[a][...]), [rows(me)])

        @pl.when(t == 1)
        def _():
            mate_load(a).wait()
            put(work(xbuf[1]), [rows(mate)])

        @pl.when(t >= 2)
        def _():
            settle(xbuf.at[lax.rem(t, 2)], s_ld.at[lax.rem(t, 2)])
            put(work(xbuf[lax.rem(t, 2)]), spots(t - 2))

        @pl.when((t >= 1) & (t < ticks + 1))
        def _():
            settle(alls[a].at[pl.ds(0, 2 * sub), :], r_par.at[a, t - 1])
            for cp in loads(a, t - 1):
                cp.start()

    def stat_tile(i, act):
        slot = lax.rem(i, 2)
        cs = ds(lax.rem(i, nt), cw)

        @pl.when(i < nt)
        def _():
            act(pltpu.make_async_copy(wq_ref.at[:, cs], wtile.at[slot], s_w.at[slot]))

        @pl.when(i >= nt)
        def _():
            act(pltpu.make_async_copy(wk_ref.at[:, cs], wtile.at[slot], s_w.at[slot]))

    def start(cp):
        cp.start()

    def wait(cp):
        cp.wait()

    def stat_step(i):
        stat_tile(i, wait)

        @pl.when(i + 1 < 2 * nt)
        def _():
            stat_tile(i + 1, start)
        r = dotf(hid[...], wtile[lax.rem(i, 2)], NN)
        w = i // nt
        qkl[w, :, ds(lax.rem(i, nt), cw)] = r
        acc = r[:, :HEAD] * r[:, :HEAD]
        for j in range(1, cw // HEAD):
            acc = acc + r[:, j * HEAD:(j + 1) * HEAD] * r[:, j * HEAD:(j + 1) * HEAD]
        inv[w] = inv[w] + acc

    def st_send(e):
        return remote(mine.at[pl.ds(0, 3)], sall.at[me, pl.ds(0, 3)], s_st.at[0], r_st.at[0], peer(e))

    sgn = jnp.where(lax.broadcasted_iota(jnp.int32, (1, HEAD), 1) < half, -1.0, 1.0).astype(f32)

    def stat_done():
        for w in range(2):
            iv = lax.rsqrt(jnp.sum(inv[w], axis=1, keepdims=True) * (1.0 / d) + NORM_EPS)
            inv[w] = jnp.broadcast_to(iv, (t_loc, HEAD))
            mine[w:w + 1, :] = as_row(iv)
        mine[2:3, :] = pos_ref[...].astype(f32)
        sall[me, 0:3, :] = mine[0:3, :]
        ang = spread_col(pos_ref[...].astype(f32)) * fr_ref[0:1, :]
        cl_s[...] = jnp.cos(ang)
        sl_s[...] = jnp.sin(ang) * (-sgn)

    def spread_col(row):
        return jnp.broadcast_to(row, (HEAD, row.shape[1])).T

    def head_w(i):
        w = (wq_ref, wk_ref, wv_ref)[i]
        return pltpu.make_async_copy(w.at[:, cols], wh.at[:, pl.ds(i * HEAD, HEAD)], s_x.at[0])

    def wo_load():
        return pltpu.make_async_copy(wo_ref.at[cols, :], woh, s_x.at[1])

    with scope('begin'):
        barrier = pltpu.get_barrier_semaphore()
        for to in (up, down, mate):
            pl.semaphore_signal(barrier, inc=1, device_id={'sp': to}, device_id_type=MESH)

        def x_piece(p):
            rs = pl.ds(p * sub, sub)
            return pltpu.make_async_copy(x_hbm.at[rs, :], x_ref.at[rs, :], s_x.at[2 + p])

        smalls = [pltpu.make_async_copy(src, dst, s_in.at[i]) for i, (src, dst) in enumerate(((gn1_hbm, gn1_ref), (gq_hbm, gq_ref), (gk_hbm, gk_ref), (pos_hbm, pos_ref), (fr_hbm, fr_ref)))]
        smalls[0].start()
        for p in (0, 2, 1, 3):
            x_piece(p).start()
        for cp in smalls[1:]:
            cp.start()
        gy_load = pltpu.make_async_copy(gy_hbm, gy_ref, s_x.at[6])
        gy_load.start()
        for i in range(3):
            head_w(i).start()
        wo_load().start()
        stat_tile(0, start)
        pl.semaphore_wait(barrier, 3)
        ring0(1, 0, 0).start()
        ring0(1, 1, 0).start()
        smalls[0].wait()
        g_ref[2:3, :] = gn1_ref[...].astype(f32).reshape(1, d)

        def norm_piece(p):
            rs = pl.ds(p * sub, sub)
            x_piece(p).wait()

            def sq_step(i, acc):
                xf = x_ref[rs, hs(i)].astype(f32)
                return acc + xf * xf

            acc = lax.fori_loop(0, nd, sq_step, jnp.zeros((sub, HEAD), f32))
            xi = lax.rsqrt(jnp.sum(acc, axis=1, keepdims=True) * (1.0 / d) + NORM_EPS)
            xinv[rs, :] = jnp.broadcast_to(xi, (sub, HEAD))

            def hid_step(i):
                hid[rs, hs(i)] = (x_ref[rs, hs(i)].astype(f32) * xi * g_ref[2:3, hs(i)]).astype(bf16)

            loop(0, nd, hid_step)

        for p in (0, 2, 1, 3):
            norm_piece(p)
            ring0(0, p // 2, p % 2).start()
        for cp in smalls[1:]:
            cp.wait()
        for w, src in enumerate((gq_ref, gk_ref)):
            g_ref[w:w + 1, :] = src[...].astype(f32).reshape(1, d)
        zero = jnp.zeros((t_loc, HEAD), f32)
        inv[...] = jnp.zeros_like(inv)
        gy_load.wait()
        own_loc(1).start()
    own_par(0).start()
    own_par(1).start()
    own_loc(0).start()
    settle(wh, s_x.at[0])
    wo_load().wait()

    hb = t_loc // 2

    def finish(s):
        for direction in range(2):
            bz = lax.rem(z + nz - 1 - s, nz) if direction == 0 else lax.rem(z + 1 + s, nz)

            def one(core):
                b = bz * 2 + core
                rs = ds(b * 2 + direction, hb)
                st = sall[b, 0:3, direction * hb:(direction + 1) * hb]
                ang = spread_col(st[2:3, :]) * fr_ref[0:1, :]
                co = jnp.cos(ang)
                si = jnp.sin(ang)
                csT[0, :, rs] = co.T[:half, :]
                csT[1, :, rs] = si.T[:half, :]
                si = si * sgn
                for w, dst in enumerate((q_s, k_s)):
                    hat = raw[w, rs, :] * spread_col(st[w:w + 1, :])
                    hatT[w, :, rs] = hat.T
                    hat = hat * g_ref[w:w + 1, cols]
                    dst[rs, :] = (hat * co + pltpu.roll(hat, half, 1) * si).astype(bf16)
                v_s[rs, :] = raw[2, rs, :].astype(bf16)

            loop(0, 2, one)

    def qkv_work(xv):
        return dotf(xv, wh[...], NN)

    def qkv_put(r, where):
        step = r.shape[0] // len(where)
        for i, rs in enumerate(where):
            for w in range(3):
                raw[w, rs, :] = r[i * step:(i + 1) * step, w * HEAD:(w + 1) * HEAD]

    spt = 2 * nt // 4

    def x_tick(t):
        gather(0, t, qkv_work, qkv_put)

        @pl.when(t == 2 * last - 1)
        def _():
            for direction in range(2):
                ring0(1, direction, 1).start()
            comm(1, 0)

        @pl.when(t < 4)
        def _():
            with scope('stat'):
                loop(t * spt, (t + 1) * spt, stat_step)

        @pl.when(t == 4)
        def _():
            with scope('statdone'):
                stat_done()

        @pl.when(t == 8)
        def _():
            for e in far:
                st_send(e).start()
            w2(start)

        @pl.when(t == 10)
        def _():
            settle(sall.at[pl.ds(0, n - 1), pl.ds(0, 3)], s_st.at[0], r_st.at[0])
        lo = jnp.where(t == 10, -1, jnp.where(t == 11, 1, jnp.where(t >= 12, t - 9, 0)))
        hi = jnp.where(t == 10, 1, jnp.where(t == 11, 3, jnp.where((t >= 12) & (t <= 14), t - 8, -1)))
        with scope('finish'):
            loop(lo, hi, finish)

    with scope('gather_x'):
        loop(0, ticks + 2, x_tick)

    def attend(j):
        qs = ds(j, blk)
        q = q_s[qs, :]

        def unit(kb, carry, masked):
            m, l, acc = carry
            ks = ds(kb, blk)
            s = dotf(q, k_s[ks, :], NT)
            if masked:
                r = lax.broadcasted_iota(jnp.int32, (blk, blk), 0)
                cc = lax.broadcasted_iota(jnp.int32, (blk, blk), 1)
                s = jnp.where(r >= cc, s, -1e30)
            mn = jnp.maximum(m, jnp.max(s, axis=1, keepdims=True))
            al = jnp.exp2((m - mn) * cexp)
            p = jnp.exp2((s - mn) * cexp)
            l = l * al + jnp.sum(p, axis=1, keepdims=True)
            acc = acc * al + dotf(p.astype(bf16), v_s[ks, :], NN)
            return mn, l, acc

        init = (jnp.full((blk, 1), -1e30, f32), jnp.zeros((blk, 1), f32), jnp.zeros((blk, HEAD), f32))
        carry = lax.fori_loop(0, j, functools.partial(unit, masked=False), init)
        m, l, acc = unit(j, carry, True)
        o = acc / l
        raw[2, qs, :] = o
        o_s[qs, :] = o.astype(bf16)
        lse[0:1, qs] = as_row(m * cexp + jnp.log2(l))

    def o_send(e):
        to = peer(e)
        return remote(o_s.at[rows(to), :], att.at[:, cols], s_o.at[0], r_o.at[0], to)

    def h_unit(u):
        return pltpu.make_async_copy(h_all.at[rows(u), :], wrow.at[1, lax.rem(u, 2)], s_hu.at[lax.rem(u, 2)])

    def kv_unit(u):
        h_unit(u).wait()

        @pl.when(u < n - 1)
        def _():
            h_unit(u + 1).start()
        xv = wrow[1, lax.rem(u, 2)]
        rs = rows(u)
        st = sall[u, 0:3, :]
        ang = spread_col(st[2:3, :]) * fr_ref[0:1, :]
        co = jnp.cos(ang)
        si = jnp.sin(ang) * sgn

        def turned(r, w, i):
            hat = r[:, i * HEAD:(i + 1) * HEAD] * spread_col(st[w:w + 1, :]) * g_ref[w:w + 1, hs(h2(i))]
            return (hat * co + pltpu.roll(hat, half, 1) * si).astype(bf16)

        @pl.when(u < 2 * z + 2)
        def _():
            rk = dotf(xv, wtile[0], NN)
            rv = dotf(xv, wtile[1], NN).astype(bf16)
            for i in range(2):
                k2[i, rs, :] = turned(rk, 1, i)
                v2[i, rs, :] = rv[:, i * HEAD:(i + 1) * HEAD]

        @pl.when(u >= 2 * z)
        def _():
            rq = dotf(xv, tile[0, 0:d, :], NN)
            for i in range(2):
                @pl.when(u < 2 * z + 2)
                def _():
                    q2[i, rows(u - 2 * z), :] = turned(rq, 0, i)

                @pl.when(u >= 2 * z + 2)
                def _():
                    k2[i, rs, :] = turned(rq, 0, i)

    def do_again(gv, core):
        r = dotf(gv, wrow[0, 0], NT).astype(bf16)
        for i in range(2):
            do2[i, rows(core), :] = r[:, i * HEAD:(i + 1) * HEAD]

    def do_work(xv):
        return dotf(xv, woh[...], NT).astype(bf16), xv

    def do_put(r, where):
        r, xv = r
        step = r.shape[0] // len(where)
        for i, rs in enumerate(where):
            do_s[rs, :] = r[i * step:(i + 1) * step]
        if len(where) == 4:
            w = dotf(xv, wrow[0, 0], NT).astype(bf16)
            for j, rs in enumerate(where):
                @pl.when(rs.start >= 2 * t_loc * (z + 1))
                def _():
                    for i in range(2):
                        v2[i, rs, :] = w[j * step:(j + 1) * step, i * HEAD:(i + 1) * HEAD]

    def y_tick(t):
        gather(1, t, do_work, do_put)

        @pl.when(t == 1)
        def _():
            with scope('finish'):
                finish(last)
        t = t - 1
        lo = jnp.where(t == 0, 0, jnp.where(t <= 4, t + 1, jnp.where(t <= 6, 6, 7)))
        hi = jnp.where(t == 0, 2, jnp.where(t <= 4, t + 2, jnp.where(t == 5, 6, jnp.where(t == 8, 8, 7))))
        hi = jnp.where(t < 0, 0, hi)
        with scope('attend'):
            loop(lo, hi, attend)

        @pl.when(t == ticks - 3)
        def _():
            send_all(o_send, far[-5:])

        @pl.when(t == ticks - 2)
        def _():
            send_all(o_send, far[:-5])

        @pl.when(t == -1)
        def _():
            settle(wrow.at[0, 0], s_r2.at[2])
            do_again(gy_ref[...], c)
            settle(h_all.at[pl.ds(0, 2 * t_loc), :], s_loc.at[0])
            h_unit(0).start()
            settle(wtile, s_r2.at[0])
            settle(tile.at[0, pl.ds(0, d), :], s_r2.at[1])

        @pl.when(t == 0)
        def _():
            do_again(xbuf[1], 1 - c)
        first = jnp.where(t == 1, 0, jnp.where(t == 2, 1, jnp.where(t == 5, 2, jnp.where(t == 7, 5, jnp.where(t == 9, 8, jnp.where(t == 10, 11, jnp.where(t == 11, 14, 16)))))))
        count = jnp.where((t == 1) | (t == 2), 1, jnp.where((t == 5) | (t == 7) | (t == 9) | (t == 10), 3, jnp.where(t == 11, 2, 0)))
        with scope('again_kv'):
            loop(first, first + count, kv_unit)

    with scope('gather_y'):
        loop(0, ticks + 2, y_tick)

    def gy_copy(t):
        return pltpu.make_async_copy(gy_all.at[:, ds(t, cw)], tile.at[lax.rem(t, 2)], s_t.at[lax.rem(t, 2)])

    def h_copy(t):
        return pltpu.make_async_copy(h_all.at[:, ds(lax.rem(t, nt), cw)], tile.at[lax.rem(t, 2)], s_t.at[lax.rem(t, 2)])

    def h2_copy(t):
        return pltpu.make_async_copy(h_all.at[:, ds(chip(t), cw)], tile.at[lax.rem(t, 2)], s_t.at[lax.rem(t, 2)])

    hw = d // 2

    def wo_half(h):
        k = lax.rem(h, 2)
        return pltpu.make_async_copy(wo_ref.at[ds(k, hw), ds(h // 2, cw)], wtile.at[lax.rem(h // 2, 2), ds(k, hw), :], s_w4.at[lax.rem(h, 4)])

    def q_send(e):
        to = peer(e)
        return remote(dq_s.at[rows(to), :], tq.at[:, cols], s_q.at[0], r_q.at[0], to)

    def kv_send(to):
        return remote(dkv.at[to], tkv.at[:, :, cols], s_kv.at[0], r_kv.at[0], to)

    gy_copy(0).start()
    for h in range(4):
        wo_half(h).start()
    settle(h_all.at[pl.ds(0, (nz - 1) * t_loc), :], s_ring.at[0])
    settle(h_all.at[pl.ds(0, nz * t_loc), :], s_par.at[0])

    @pl.when(sent)
    def _():
        att[:, cols] = o_s[rows(me), :]
    raw[0] = jnp.zeros((t_all, HEAD), f32)

    def delta(j):
        qs = ds(j, blk)
        lse[1:2, qs] = as_row(jnp.sum(raw[2, qs, :] * do_s[qs, :].astype(f32), axis=1, keepdims=True))

    with scope('delta'):
        loop(0, nb, delta)

    home = z // (nz // 2)
    slot2 = lax.rem(z // 2, 2)
    mine_too = again & (home == c)

    def ld_send(k):
        to = lax.rem(z + k, nz) * 2 + home
        return remote(lse.at[pl.ds(0, 2)], ld2.at[slot2, pl.ds(0, 2)], s_ld2.at[0], r_ld2.at[0], to)

    @pl.when(again)
    def _():
        for k in (4, 2, 6):
            ld_send(k).start()

    @pl.when(again & (home != c))
    def _():
        ld_send(0).start()

    @pl.when(mine_too)
    def _():
        ld2[slot2, 0:2, :] = lse[0:2, :]

    def bwd_step(s):
        kb = chip(s)
        ks = ds(kb, blk)
        k = k_s[ks, :]
        v = v_s[ks, :]

        def unit(qb, carry, masked):
            dk, dv = carry
            qs = ds(qb, blk)
            q = q_s[qs, :]
            do = do_s[qs, :]
            p = jnp.exp2(dotf(k, q, NT) * cexp - lse[0:1, qs])
            if masked:
                r = lax.broadcasted_iota(jnp.int32, (blk, blk), 0)
                cc = lax.broadcasted_iota(jnp.int32, (blk, blk), 1)
                p = jnp.where(cc >= r, p, 0.0)
            g = (p * (dotf(v, do, NT) - lse[1:2, qs])).astype(bf16)
            dv = dv + dotf(p.astype(bf16), do, NN)
            dk = dk + dotf(g, q, NN)
            raw[0, qs, :] = raw[0, qs, :] + dotf(g, k, TN)
            return dk, dv

        zk = jnp.zeros((blk, HEAD), f32)
        carry = unit(kb, (zk, zk), True)
        dk, dv = lax.fori_loop(kb + 1, nb, functools.partial(unit, masked=False), carry)
        dk = (dk * scale).astype(bf16)
        dv = dv.astype(bf16)
        for u in range(2):
            dkv[2 * kb + u, 0] = dk[u * t_loc:(u + 1) * t_loc]
            dkv[2 * kb + u, 1] = dv[u * t_loc:(u + 1) * t_loc]

        @pl.when((kb != z) & to_send(2 * kb))
        def _():
            for u in range(2):
                kv_send(2 * kb + u).start()

        @pl.when((kb == z) & sent)
        def _():
            kv_send(mate).start()

    with scope('bwd'):
        loop(0, nb, bwd_step)
        dq_s[...] = (raw[0] * scale).astype(bf16)
    gcol = [spread_col(g_ref[w:w + 1, cols])[:, 0:1] for w in range(2)]

    def unroped(src, js):
        ct = csT[0, :, js]
        sn = csT[1, :, js]
        t = src.astype(f32).T
        p, r = t[:half], t[half:]
        return jnp.concatenate([p * ct + r * sn, r * ct - p * sn], axis=0)

    def share_step(j, carry):
        js = rows(j)
        res = []
        for w, src in enumerate((dq_s[js, :], dkv[j, 0])):
            th = unroped(src, js) * hatT[w, :, js]
            res.append(carry[w] + th)
            pm[j, w:w + 1, :] = jnp.sum(th * gcol[w], axis=0, keepdims=True)
        return tuple(res)

    def p_send(e):
        to = peer(e)
        return remote(pm.at[to, pl.ds(0, 2)], pall.at[me, pl.ds(0, 2)], s_p.at[0], r_p.at[0], to)

    with scope('share'):
        zt = jnp.zeros((HEAD, t_loc), f32)
        sums = lax.fori_loop(0, n, share_step, (zt, zt))
    for e in far:
        p_send(e).start()
    send_all(q_send, far)

    @pl.when(sent)
    def _():
        tq[:, cols] = dq_s[rows(me), :]
        tkv[:, :, cols] = dkv[me]

    pall[me, 0:2, :] = pm[me, 0:2, :]
    for w in range(2):
        gg_s[w] = jnp.broadcast_to(jnp.sum(sums[w], axis=1, keepdims=True), (HEAD, HEAD)).T[0:8, :]

    def flip_o(i):
        rawT[0:HEAD, rows(i)] = o_s[rows(i), :].T

    def flip_v(i):
        rawT[0:HEAD, rows(i)] = dkv[i, 1].T

    def dwo_step(t):
        gy_copy(t).wait()

        @pl.when(t + 1 < nt)
        def _():
            gy_copy(t + 1).start()

        @pl.when(t + 1 == nt)
        def _():
            h_copy(t + 1).start()
        r = dotf(rawT[0:HEAD, :], tile[lax.rem(t, 2)], NN)
        for u in range(cw // HEAD):
            raw[2, hs(n + t * (cw // HEAD) + u), :] = r[:, u * HEAD:(u + 1) * HEAD]

    def dwv_step(t):
        h_copy(t).wait()

        @pl.when(t + 1 < 2 * nt)
        def _():
            h_copy(t + 1).start()

        @pl.when(t + 1 == 2 * nt)
        def _():
            h2_copy(0).start()
        r = dotf(rawT[0:HEAD, :], tile[lax.rem(t, 2)], NN)
        for u in range(cw // HEAD):
            raw[2, hs((t - nt) * (cw // HEAD) + u), :] = r[:, u * HEAD:(u + 1) * HEAD].T

    def y_step(t):
        cs = ds(t, cw)
        acc = x_ref[:, cs].astype(f32)
        for k in range(2):
            h = 2 * t + k
            wo_half(h).wait()
            acc = acc + dotf(att[:, k * hw:(k + 1) * hw], wtile[lax.rem(t, 2), k * hw:(k + 1) * hw, :], NN)

            @pl.when(h + 4 < 2 * nt)
            def _():
                wo_half(h + 4).start()
        hid[:, cs] = acc.astype(bf16)

    def v_send(e):
        to = peer(e)
        return remote(raw.at[2, hs(to), :], dwv_out.at[:, cols], s_v.at[0], r_v.at[0], to)

    def out(i):
        src, dst, k = ((hid, y_out, 0), None, (xbuf.at[0], gx_out, 0), (raw.at[2, hs(me), :], dwv_out.at[:, cols], 2),
                       (raw.at[1, rows_f(0, me), :], dwq_out.at[:, cols], 2), (raw.at[1, rows_f(1, me), :], dwk_out.at[:, cols], 2),
                       (gg_s, gg_out, 3), (gpart.at[me], gall.at[me], 4))[i]
        return pltpu.make_async_copy(src, dst, s_out.at[k])

    def rows_f(w, to):
        return ds(w * n + to, HEAD)

    with scope('dwo'):
        loop(0, n, flip_o)
        loop(0, nt, dwo_step)
        for j in range(n):
            pltpu.make_async_copy(raw.at[2, pl.ds((n + j) * HEAD, HEAD), :], dwo_out.at[:, pl.ds(j * HEAD, HEAD)], s_out.at[1]).start()

    def m_send(e):
        return remote(mine2.at[pl.ds(0, 2)], mall.at[me, pl.ds(0, 2)], s_m.at[0], r_m.at[0], peer(e))

    with scope('dwv'):
        loop(0, n, flip_v)
        loop(nt, 2 * nt, dwv_step)
        out(3).start()
    with scope('pwait'):
        settle(pall.at[pl.ds(0, n - 1), pl.ds(0, 2)], s_p.at[0], r_p.at[0])
        tot = pall[0, 0:2, :]
        for j in range(1, n):
            tot = tot + pall[j, 0:2, :]
        mine2[0:2, :] = tot * (1.0 / d)
    for e in far:
        m_send(e).start()
    mall[me, 0:2, :] = mine2[0:2, :]
    for e in far:
        v_send(e).start()
    def got(buf, s_sem, r_sem):
        @pl.when(sent)
        def _():
            settle(buf.at[pl.ds(0, (n - 1) * msg), :], s_sem.at[0])
            settle(buf.at[pl.ds(0, (n_sent - 1) * msg), :], r_sem.at[0])

        @pl.when(again)
        def _():
            settle(buf.at[pl.ds(0, n // 2 * msg), :], s_sem.at[0])
            settle(buf.at[pl.ds(0, n_sent * msg), :], r_sem.at[0])

    def o2_send(i):
        return remote(o2.at[i, rows(1 - c), :], att.at[:, hs(h2(i))], s_o2.at[0], r_o2.at[0], mate)

    def q2_send(i):
        return remote(dq2.at[i, rows(1 - c), :], tq.at[:, hs(h2(i))], s_q2.at[0], r_q2.at[0], mate)

    def again_head(i):
        q = q2[i]
        do = do2[i]
        r0 = lax.broadcasted_iota(jnp.int32, (blk, blk), 0)
        c0 = lax.broadcasted_iota(jnp.int32, (blk, blk), 1)

        def unit(kb, carry, masked):
            m, l, acc = carry
            ks = ds(kb, blk)
            s = dotf(q, k2[i, ks, :], NT)
            if masked:
                s = jnp.where(r0 >= c0, s, -1e30)
            mn = jnp.maximum(m, jnp.max(s, axis=1, keepdims=True))
            al = jnp.exp2((m - mn) * cexp)
            p = jnp.exp2((s - mn) * cexp)
            l = l * al + jnp.sum(p, axis=1, keepdims=True)
            acc = acc * al + dotf(p.astype(bf16), v2[i, ks, :], NN)
            return mn, l, acc

        init = (jnp.full((blk, 1), -1e30, f32), jnp.zeros((blk, 1), f32), jnp.zeros((blk, HEAD), f32))
        m, l, acc = unit(z, lax.fori_loop(0, z, functools.partial(unit, masked=False), init), True)
        o = acc / l
        o2[i] = o.astype(bf16)
        ls = m * cexp + jnp.log2(l)
        de = jnp.sum(o * do.astype(f32), axis=1, keepdims=True)

        def unit2(kb, dq, masked):
            ks = ds(kb, blk)
            k = k2[i, ks, :]
            p = jnp.exp2(dotf(q, k, NT) * cexp - ls)
            if masked:
                p = jnp.where(r0 >= c0, p, 0.0)
            g = (p * (dotf(do, v2[i, ks, :], NT) - de)).astype(bf16)
            return dq + dotf(g, k, NN)

        dq = unit2(z, lax.fori_loop(0, z, functools.partial(unit2, masked=False), jnp.zeros((blk, HEAD), f32)), True)
        dq2[i] = (dq * scale).astype(bf16)

        k = k2[i, ds(z, blk), :]
        v = v2[i, ds(z, blk), :]

        def unit3(carry, qq, dd, qb, masked):
            dk, dv = carry
            qs = ds(qb, blk)
            p = jnp.exp2(dotf(k, qq, NT) * cexp - ld2[i, 0:1, qs])
            if masked:
                p = jnp.where(c0 >= r0, p, 0.0)
            g = (p * (dotf(v, dd, NT) - ld2[i, 1:2, qs])).astype(bf16)
            return dk + dotf(g, qq, NN), dv + dotf(p.astype(bf16), dd, NN)

        def later(qb, carry):
            qs = ds(qb, blk)
            return unit3(carry, k2[i, qs, :], v2[i, qs, :], qb, False)

        zk = jnp.zeros((blk, HEAD), f32)
        dk, dv = lax.fori_loop(z + 1, nb, later, unit3((zk, zk), q, do, z, True))
        dkv2[i, 0] = (dk * scale).astype(bf16)
        dkv2[i, 1] = dv.astype(bf16)
        for w in range(2):
            tkv[w, :, hs(h2(i))] = dkv2[i, w, rows(c), :]
        att[:, hs(h2(i))] = o2[i, rows(c), :]
        tq[:, hs(h2(i))] = dq2[i, rows(c), :]

    def kv2_send(i):
        return remote(dkv2.at[i, :, rows(1 - c), :], tkv.at[:, :, hs(h2(i))], s_kv2.at[0], r_kv2.at[0], mate)

    pair = ld2.at[pl.ds(0, 1), pl.ds(0, 2)]
    with scope('ldwait'):
        @pl.when(mine_too)
        def _():
            settle(pair, r_ld2.at[0])
            settle(ld2.at[:, pl.ds(0, nz // 2 - 1)], s_ld2.at[0])

        @pl.when(jnp.logical_not(mine_too))
        def _():
            settle(ld2.at[:, pl.ds(0, 2)], r_ld2.at[0])

        @pl.when(again & (home != c))
        def _():
            settle(ld2.at[:, pl.ds(0, nz // 2)], s_ld2.at[0])
    def again_both(i):
        again_head(i)
        o2_send(i).start()
        q2_send(i).start()
        kv2_send(i).start()


    def w_copies(t):
        slot = lax.rem(t, 2)
        return [pltpu.make_async_copy(w.at[ds(t, wr), :], wrow.at[slot, i], s_wr.at[slot]) for i, w in enumerate((wq_ref, wk_ref, wv_ref))]

    for cp in w_copies(0):
        cp.start()
    cl = cl_s[...]
    sl = sl_s[...]

    def back_rope(a):
        a = a.astype(f32)
        return a * cl + pltpu.roll(a, half, 1) * sl

    def loc_step(i):
        tq[:, hs(i)] = (inv[0] * (back_rope(tq[:, hs(i)]) * g_ref[0:1, hs(i)] - qkl[0, :, hs(i)] * inv[0] * mq)).astype(bf16)
        tkv[0, :, hs(i)] = (inv[1] * (back_rope(tkv[0, :, hs(i)]) * g_ref[1:2, hs(i)] - qkl[1, :, hs(i)] * inv[1] * mk)).astype(bf16)

    def head_step(j):
        js = rows(j)
        for w, src in enumerate((dq_s[js, :], dkv[j, 0])):
            rawT[w * HEAD:(w + 1) * HEAD, js] = (sall[j, w:w + 1, :] * (unroped(src, js) * gcol[w] - hatT[w, :, js] * mall[j, w:w + 1, :])).astype(bf16)

    def a_send(to):
        return remote(raw.at[1, rows_f(0, to), :], dwq_out.at[:, cols], s_a.at[0], r_a.at[0], to)

    def b_send(to):
        return remote(raw.at[1, rows_f(1, to), :], dwk_out.at[:, cols], s_b.at[0], r_b.at[0], to)

    def dw_step(t):
        h2_copy(t).wait()

        @pl.when(t + 1 < nt)
        def _():
            h2_copy(t + 1).start()
        nn = chip(t)
        r = dotf(rawT[...], tile[lax.rem(t, 2)], NN)
        for u in range(cw // HEAD):
            to = nn * (cw // HEAD) + u
            for w in range(2):
                raw[1, rows_f(w, to), :] = r[w * HEAD:(w + 1) * HEAD, u * HEAD:(u + 1) * HEAD].T

            @pl.when(to != me)
            def _():
                a_send(to).start()
                b_send(to).start()

    def phase(i):
        with scope('again'):
            again_both(i)

        @pl.when(i == 0)
        def _():
            with scope('mwait'):
                settle(mall.at[pl.ds(0, n - 1), pl.ds(0, 2)], s_m.at[0], r_m.at[0])
            with scope('head'):
                loop(0, n, head_step)
            with scope('dw'):
                loop(0, nt - 2, dw_step)

    loop(0, 2, phase)
    with scope('waitkv'):
        @pl.when(sent)
        def _():
            settle(tkv.at[:, pl.ds(0, (n - 1) * msg), :], s_kv.at[0])
            settle(tkv.at[:, pl.ds(0, (n_sent - 1) * msg), :], r_kv.at[0])

        @pl.when(again)
        def _():
            settle(tkv.at[:, pl.ds(0, n // 2 * msg), :], s_kv.at[0])
            settle(tkv.at[:, pl.ds(0, n_sent * msg), :], r_kv.at[0])
        settle(tkv.at[:, pl.ds(0, 2 * msg), :], s_kv2.at[0], r_kv2.at[0])
    with scope('waitq'):
        got(tq, s_q, r_q)
        settle(tq.at[pl.ds(0, 2 * msg), :], s_q2.at[0], r_q2.at[0])

    mq = spread_col(mine2[0:1, :])
    mk = spread_col(mine2[1:2, :])
    with scope('loc'):
        loop(0, nd, loc_step)

    def dh_step(t):
        settle(wrow.at[lax.rem(t, 2)], s_wr.at[lax.rem(t, 2)])

        @pl.when(t + 1 < nw)
        def _():
            for cp in w_copies(t + 1):
                cp.start()
        slot = lax.rem(t, 2)
        r = dotf(tq[...], wrow[slot, 0], NT) + dotf(tkv[0], wrow[slot, 1], NT) + dotf(tkv[1], wrow[slot, 2], NT)
        dh[:, ds(t, wr)] = r.astype(bf16).astype(f32)

    with scope('dh'):
        loop(0, nw, dh_step)

    def mx_step(i, acc):
        return acc + dh[:, hs(i)] * g_ref[2:3, hs(i)] * x_ref[:, hs(i)].astype(f32)

    def g_send(e):
        return remote(gpart.at[peer(e), pl.ds(0, 1)], gall.at[me, pl.ds(0, 1)], s_g.at[0], r_g.at[0], peer(e))

    with scope('gx'):
        mx = jnp.sum(lax.fori_loop(0, nd, mx_step, zero), axis=1, keepdims=True) * (1.0 / d) * xinv[...]

        def gx_step(i):
            xh = x_ref[:, hs(i)].astype(f32) * xinv[...]
            dhh = dh[:, hs(i)]
            gpart[i] = jnp.broadcast_to(jnp.sum(dhh * xh, axis=0, keepdims=True), (8, HEAD))
            xbuf[0, :, hs(i)] = (gy_ref[:, hs(i)].astype(f32) + xinv[...] * (dhh * g_ref[2:3, hs(i)] - xh * mx)).astype(bf16)

        loop(0, nd, gx_step)
        out(2).start()
    for e in far:
        g_send(e).start()
    out(7).start()
    out(6).start()
    with scope('dw2'):
        loop(nt - 2, nt, dw_step)
        out(4).start()
        out(5).start()
    with scope('y'):
        got(att, s_o, r_o)
        settle(att.at[pl.ds(0, 2 * msg), :], s_o2.at[0], r_o2.at[0])
        loop(0, nt, y_step)
        out(0).start()
    with scope('end_drain'):
        settle(gy_all.at[pl.ds(0, (nz - 1) * t_loc), :], s_ring.at[1])
        settle(gy_all.at[pl.ds(0, nz * t_loc), :], s_par.at[1])
        settle(tkv, s_out.at[0])
        settle(raw.at[2, pl.ds(0, n * HEAD), :], s_out.at[1])
        settle(raw.at[2, pl.ds(0, 3 * HEAD), :], s_out.at[2])
        settle(gg_s, s_out.at[3])
        settle(gpart.at[0], s_out.at[4])
    most = pl.ds(0, HEAD - HEAD // n)
    with scope('end_v'):
        settle(dwv_out.at[most, :], s_v.at[0], r_v.at[0])
    with scope('end_a'):
        settle(dwq_out.at[most, :], s_a.at[0], r_a.at[0])
    with scope('end_b'):
        settle(dwk_out.at[most, :], s_b.at[0], r_b.at[0])
    with scope('end_g'):
        settle(gall.at[pl.ds(0, n - 1), pl.ds(0, 1)], s_g.at[0], r_g.at[0])


def block(n, x, gy, pos, gq, gk, gn, freq, wq, wk, wv, wo):
    t_loc, d = x.shape
    t_all = t_loc * n
    hb = pl.BlockSpec(memory_space=pl.ANY)
    S = jax.ShapeDtypeStruct
    V = pltpu.VMEM
    sem = pltpu.SemaphoreType.DMA
    hd = (t_all, HEAD)
    tok = (t_loc, d)
    nz = n // 2
    return pl.pallas_call(functools.partial(block_kernel, n),
        in_specs=[hb] * 11,
        out_specs=[hb] * 10,
        out_shape=[S(tok, bf16), S(tok, bf16), S((n, 8, d // n), f32)] + [S((d // n, d), f32)] * 4 + [S((2, 8, HEAD), f32), S((t_all, d), bf16), S((t_all, d), bf16)],
        scratch_shapes=[V((1, t_loc), jnp.int32), V((d,), bf16), V((d,), bf16), V((d,), bf16), V((8, HEAD), f32), V(tok, bf16), V(tok, bf16), V((8, d), f32), V(tok, bf16), V((d, 3 * HEAD), bf16), V((HEAD, d), bf16), V((3,) + hd, f32), V((2,) + tok, bf16), V((2, d, 2 * HEAD), bf16), V((2, t_all, 2 * HEAD), bf16), V((2, 3, 2 * HEAD, d), bf16),
            V((2,) + tok, f32), V((2, HEAD, t_all), f32), V((2, HEAD // 2, t_all), f32)] + [V(hd, bf16)] * 5 + [V((8, t_all), f32), V((2, 8, t_all), f32)]
        + [V(hd, bf16), V((n, 2, t_loc, HEAD), bf16), V(tok, bf16), V((2,) + tok, bf16), V(tok, bf16), V((2 * HEAD, t_all), bf16), V(tok, f32),
            V((t_loc, HEAD), f32), V((t_loc, HEAD), f32), V((2, t_loc, HEAD), f32), V((t_loc, HEAD), f32), V((8, t_loc), f32), V((n, 8, t_loc), f32), V((8, t_loc), f32), V((n, 8, t_loc), f32), V((n, 8, t_loc), f32), V((n, 8, t_loc), f32), V((n, 8, d // n), f32), V((2, 8, HEAD), f32)] + [V((2, t_all, HEAD), bf16)] * 2 + [V((2, 2 * t_loc, HEAD), bf16)] * 4 + [V((2, 2, 2 * t_loc, HEAD), bf16)]
        + [sem((2,)), sem((2, 2, nz - 1, 2)), sem((2,)), sem((2, 2 * (nz - 1))), sem((2,))] + [sem((1,))] * 20
        + [sem((2,)), sem((2,)), sem((2,)), sem((7,)), sem((2,)), sem((1,)), sem((5,)), sem((5,)), sem((3,)), sem((2,))] + [sem((1,))] * 8 + [sem((4,))],
        compiler_params=pltpu.CompilerParams(collective_id=1, has_side_effects=True, vmem_limit_bytes=67043328), name='block')(x, gy, pos, gq, gk, gn, freq, wq, wk, wv, wo)


def copy_kernel(*refs):
    k = (len(refs) - 2) // 3
    src, dst, buf, si, so = list(refs[:k - 1]), refs[k - 1:2 * k - 1], refs[2 * k - 1:3 * k - 1], refs[-2], refs[-1]
    parts = src[k - 3]
    src[k - 3:] = [parts, src[k - 2].at[0, 0:1, :], src[k - 2].at[1, 0:1, :]]
    buf = list(buf)
    total = buf[k - 3]
    buf[k - 3] = refs[-3]
    ins = [pltpu.make_async_copy(src[i], buf[i], si.at[i]) for i in range(k)]
    outs = [pltpu.make_async_copy(buf[i], dst[i], so.at[i]) if i != k - 3 else None for i in range(k)]
    for cp in ins:
        cp.start()
    outs[k - 3] = pltpu.make_async_copy(total, dst[k - 3], so.at[k - 3])
    for i in range(k):
        ins[i].wait()
        if i == k - 3:
            total[...] = jnp.sum(refs[-3][:, 0:1, :], axis=0)
        outs[i].start()
    for cp in outs:
        cp.wait()


def copy_out(arrays):
    hb = pl.BlockSpec(memory_space=pl.ANY)
    shapes = [(a.shape, a.dtype) for a in arrays[:-2]] + [((1, HEAD), f32)] * 3
    k = len(shapes)
    return pl.pallas_call(copy_kernel, in_specs=[hb] * len(arrays), out_specs=[hb] * k, out_shape=[jax.ShapeDtypeStruct(*a) for a in shapes],
        scratch_shapes=[pltpu.VMEM(*a) for a in shapes] + [pltpu.VMEM(arrays[-2].shape, f32)] + [pltpu.SemaphoreType.DMA((k,))] * 2, name='copy_out')(*arrays)


def solution(mesh):
    n = mesh.shape['sp']

    def device_step(x_in, grad_y, positions, g_norm, wq, wk, wv, wo, gq, gk):
        half = HEAD // 2
        inv_freq = ROPE_BASE ** (-np.arange(half) * (2.0 / HEAD))
        freq = jnp.asarray(np.tile(inv_freq, (8, 2)), f32)
        y, gx, gn, dwq, dwk, dwv, dwo, gg, _, _ = block(n, x_in[0], grad_y[0], positions, gq, gk, g_norm, freq, wq, wk, wv, wo)
        y, gx, dwq, dwk, dwv, dwo, gn, ggq, ggk = copy_out([y, gx, dwq, dwk, dwv, dwo, gn, gg])
        return (y[None], gx[None], gn[0], dwq, dwk, dwv, dwo, ggq[0], ggk[0])

    seq_spec = P('dp', 'sp', None)
    rep2, rep1 = P(None, None), P(None)
    row_spec, vec_spec = P(('dp', 'sp'), None), P(('dp', 'sp'))
    return jax.shard_map(device_step, mesh=mesh, in_specs=(seq_spec, seq_spec, P('dp', 'sp'), rep1, rep2, rep2, rep2, rep2, rep1, rep1), out_specs=(seq_spec, seq_spec, vec_spec, row_spec, row_spec, row_spec, row_spec, vec_spec, vec_spec), check_vma=False)
```

```python
import contextlib
import functools
import jax
import jax.numpy as jnp
import numpy as np
from jax import lax
from jax.experimental import pallas as pl
from jax.experimental.pallas import tpu as pltpu
from jax.sharding import PartitionSpec as P

HEAD = 128
NORM_EPS = 1e-5
ROPE_BASE = 10000.0
LOG2E = 1.4426950408889634
f32 = jnp.float32
bf16 = jnp.bfloat16
MESH = pl.DeviceIdType.MESH
NN = (((1,), (0,)), ((), ()))
NT = (((1,), (1,)), ((), ()))
TN = (((0,), (0,)), ((), ()))
PROF = 0
scope = jax.named_scope if PROF else (lambda name: contextlib.nullcontext())


def dotf(a, b, dims):
    return lax.dot_general(a, b, dims, preferred_element_type=f32)


def remote(src, dst, ss, rs, to):
    return pltpu.make_async_remote_copy(src_ref=src, dst_ref=dst, send_sem=ss, recv_sem=rs, device_id={'sp': to}, device_id_type=MESH)


def ds(i, size):
    return pl.ds(pl.multiple_of(i * size, size), size)


def settle(ref, *sems):
    for sem in sems:
        pltpu.make_async_copy(ref, ref, sem).wait()


def as_row(col):
    return jnp.broadcast_to(col, (col.shape[0], HEAD)).T[0:1, :]


def loop(lo, hi, body):
    def step(i, carry):
        body(i)
        return carry
    lax.fori_loop(lo, hi, step, 0)


def block_kernel(n, x_hbm, gy_hbm, pos_hbm, gq_hbm, gk_hbm, gn1_hbm, fr_hbm, wq_ref, wk_ref, wv_ref, wo_ref,
                 y_out, gx_out, gall, dwq_out, dwk_out, dwv_out, dwo_out, gg_out, h_all, gy_all,
                 pos_ref, gq_ref, gk_ref, gn1_ref, fr_ref, x_ref, gy_ref, g_ref, hid, wh, woh, raw, xbuf, wtile, tile, wrow, qkl, hatT, csT, q_s, k_s, v_s, do_s, o_s, lse, ld2,
                 dq_s, dkv, tq, tkv, att, rawT, dh, cl_s, sl_s, inv, xinv, mine, sall, mine2, mall, pm, pall, gpart, gg_s, k2, v2, q2, do2, o2, dq2, dkv2,
                 s_ring, r_ring, s_par, r_par, r_own, s_st, r_st, s_o, r_o, s_kv, r_kv, s_q, r_q, s_v, r_v, s_a, r_a, s_b, r_b, s_m, r_m, s_g, r_g, s_p, r_p,
                 s_ld, s_t, s_w, s_x, s_wr, s_loc, s_out, s_in, s_r2, s_hu, s_o2, r_o2, s_q2, r_q2, s_kv2, r_kv2, s_ld2, r_ld2, s_w4):
    me = lax.axis_index('sp')
    t_loc, d = x_hbm.shape
    t_all = t_loc * n
    z = me // 2
    c = lax.rem(me, 2)
    nz = n // 2
    mate = me + 1 - 2 * c
    up = lax.rem(z + 1, nz) * 2 + c
    down = lax.rem(z + nz - 1, nz) * 2 + c
    nd = d // HEAD
    half = HEAD // 2
    sub = t_loc // 4
    last = nz - 2
    ticks = 2 * (nz - 1)
    blk = 2 * t_loc
    nb = t_all // blk
    cexp = HEAD ** -0.5 * LOG2E
    scale = HEAD ** -0.5
    cw = tile.shape[2]
    nt = d // cw
    wr = wrow.shape[2]
    nw = d // wr
    cols = ds(me, HEAD)
    far = sorted(range(1, n), key=lambda e: -min(e, n - e))
    alls = (h_all, gy_all)
    own_src = (hid, gy_hbm)

    again = c == 0
    sent = c == 1
    msg = t_loc // n

    def h2(i):
        off = jnp.where(i == 0, nz // 2, jnp.where(c == 0, 2, nz - 2))
        return lax.rem(z + off, nz) * 2 + jnp.where(i == 0, c, 0)

    def to_send(to):
        gap = lax.rem(to // 2 + nz - z, nz)
        return (gap != nz // 2) & (sent | ((gap != 2) & (gap != nz - 2)))

    def send_all(make, es):
        for e in es:
            @pl.when(to_send(peer(e)))
            def _():
                make(e).start()

    def w2(act):
        for i in range(2):
            act(pltpu.make_async_copy(wk_ref.at[:, hs(h2(i))], wtile.at[0, :, pl.ds(i * HEAD, HEAD)], s_r2.at[0]))
            act(pltpu.make_async_copy(wv_ref.at[:, hs(h2(i))], wtile.at[1, :, pl.ds(i * HEAD, HEAD)], s_r2.at[0]))
            act(pltpu.make_async_copy(wq_ref.at[:, hs(h2(i))], tile.at[0, pl.ds(0, d), pl.ds(i * HEAD, HEAD)], s_r2.at[1]))
            act(pltpu.make_async_copy(wo_ref.at[hs(h2(i)), :], wrow.at[0, 0, pl.ds(i * HEAD, HEAD), :], s_r2.at[2]))

    def peer(e):
        return lax.rem(me + e, n)

    def rows(i):
        return ds(i, t_loc)

    def hs(i):
        return ds(i, HEAD)

    def chip(s):
        k = nz // 2 - (s + 1) // 2
        return lax.rem(z + nz + jnp.where(lax.rem(s, 2) == 0, -k, k), nz)

    def piece(core, direction, s, u):
        bz = lax.rem(z + nz - 1 - s, nz) if direction == 0 else lax.rem(z + 1 + s, nz)
        return ds((bz * 2 + core) * 4 + 2 * direction + u, sub)

    def ring(a, direction, s, u):
        ref = alls[a]
        bz = lax.rem(z + nz - s, nz) if direction == 0 else lax.rem(z + s, nz)
        rs = ds((bz * 2 + c) * 4 + 2 * direction + u, sub)
        return remote(ref.at[rs, :], ref.at[rs, :], s_ring.at[a], r_ring.at[a, direction, s, u], up if direction == 0 else down)

    def ring0(a, direction, u):
        rs = ds(me * 4 + 2 * direction + u, sub)
        return remote(own_src[a].at[pl.ds((2 * direction + u) * sub, sub), :], alls[a].at[rs, :], s_ring.at[a], r_ring.at[a, direction, 0, u], up if direction == 0 else down)

    def par(a, direction, s, u):
        rs = piece(c, direction, s, u)
        return remote(alls[a].at[rs, :], alls[a].at[rs, :], s_par.at[a], r_par.at[a, 2 * s + u], mate)

    def own_par(a):
        return remote((hid, gy_ref)[a], alls[a].at[rows(me), :], s_par.at[a], r_own.at[a], mate)

    def own_loc(a):
        return pltpu.make_async_copy((hid, gy_ref)[a], alls[a].at[rows(me), :], s_loc.at[0])

    def comm(a, t):
        s = t // 2
        u = lax.rem(t, 2)
        for direction in range(2):
            ring(a, direction, s, u).wait_recv()

            @pl.when(s < last)
            def _():
                ring(a, direction, s + 1, u).start()
            par(a, direction, s, u).start()

    def loads(a, t):
        s = t // 2
        u = lax.rem(t, 2)
        slot = lax.rem(t, 2)
        out = []
        for i, (core, direction) in enumerate(((c, 0), (c, 1), (1 - c, 0), (1 - c, 1))):
            out.append(pltpu.make_async_copy(alls[a].at[piece(core, direction, s, u), :], xbuf.at[slot, pl.ds(i * sub, sub), :], s_ld.at[slot]))
        return out

    def mate_load(a):
        return pltpu.make_async_copy(alls[a].at[rows(mate), :], xbuf.at[1], s_ld.at[1])

    def spots(t):
        s = t // 2
        u = lax.rem(t, 2)
        return [piece(c, 0, s, u), piece(c, 1, s, u), piece(1 - c, 0, s, u), piece(1 - c, 1, s, u)]

    def gather(a, t, work, put):
        @pl.when((t >= a) & (t < ticks))
        def _():
            with scope('comm'):
                comm(a, t)

        @pl.when(t == 0)
        def _():
            own_par(a).wait_recv()
            mate_load(a).start()
            put(work((hid, gy_ref)[a][...]), [rows(me)])

        @pl.when(t == 1)
        def _():
            mate_load(a).wait()
            put(work(xbuf[1]), [rows(mate)])

        @pl.when(t >= 2)
        def _():
            settle(xbuf.at[lax.rem(t, 2)], s_ld.at[lax.rem(t, 2)])
            put(work(xbuf[lax.rem(t, 2)]), spots(t - 2))

        @pl.when((t >= 1) & (t < ticks + 1))
        def _():
            settle(alls[a].at[pl.ds(0, 2 * sub), :], r_par.at[a, t - 1])
            for cp in loads(a, t - 1):
                cp.start()

    def stat_tile(i, act):
        slot = lax.rem(i, 2)
        cs = ds(lax.rem(i, nt), cw)

        @pl.when(i < nt)
        def _():
            act(pltpu.make_async_copy(wq_ref.at[:, cs], wtile.at[slot], s_w.at[slot]))

        @pl.when(i >= nt)
        def _():
            act(pltpu.make_async_copy(wk_ref.at[:, cs], wtile.at[slot], s_w.at[slot]))

    def start(cp):
        cp.start()

    def wait(cp):
        cp.wait()

    def stat_step(i):
        stat_tile(i, wait)

        @pl.when(i + 1 < 2 * nt)
        def _():
            stat_tile(i + 1, start)
        r = dotf(hid[...], wtile[lax.rem(i, 2)], NN)
        w = i // nt
        qkl[w, :, ds(lax.rem(i, nt), cw)] = r
        acc = r[:, :HEAD] * r[:, :HEAD]
        for j in range(1, cw // HEAD):
            acc = acc + r[:, j * HEAD:(j + 1) * HEAD] * r[:, j * HEAD:(j + 1) * HEAD]
        inv[w] = inv[w] + acc

    def st_send(e):
        return remote(mine.at[pl.ds(0, 3)], sall.at[me, pl.ds(0, 3)], s_st.at[0], r_st.at[0], peer(e))

    sgn = jnp.where(lax.broadcasted_iota(jnp.int32, (1, HEAD), 1) < half, -1.0, 1.0).astype(f32)

    def stat_done():
        for w in range(2):
            iv = lax.rsqrt(jnp.sum(inv[w], axis=1, keepdims=True) * (1.0 / d) + NORM_EPS)
            inv[w] = jnp.broadcast_to(iv, (t_loc, HEAD))
            mine[w:w + 1, :] = as_row(iv)
        mine[2:3, :] = pos_ref[...].astype(f32)
        sall[me, 0:3, :] = mine[0:3, :]
        ang = spread_col(pos_ref[...].astype(f32)) * fr_ref[0:1, :]
        cl_s[...] = jnp.cos(ang)
        sl_s[...] = jnp.sin(ang) * (-sgn)

    def spread_col(row):
        return jnp.broadcast_to(row, (HEAD, row.shape[1])).T

    def head_w(i):
        w = (wq_ref, wk_ref, wv_ref)[i]
        return pltpu.make_async_copy(w.at[:, cols], wh.at[:, pl.ds(i * HEAD, HEAD)], s_x.at[0])

    def wo_load():
        return pltpu.make_async_copy(wo_ref.at[cols, :], woh, s_x.at[1])

    with scope('begin'):
        barrier = pltpu.get_barrier_semaphore()
        for to in (up, down, mate):
            pl.semaphore_signal(barrier, inc=1, device_id={'sp': to}, device_id_type=MESH)

        def x_piece(p):
            rs = pl.ds(p * sub, sub)
            return pltpu.make_async_copy(x_hbm.at[rs, :], x_ref.at[rs, :], s_x.at[2 + p])

        smalls = [pltpu.make_async_copy(src, dst, s_in.at[i]) for i, (src, dst) in enumerate(((gn1_hbm, gn1_ref), (gq_hbm, gq_ref), (gk_hbm, gk_ref), (pos_hbm, pos_ref), (fr_hbm, fr_ref)))]
        smalls[0].start()
        for p in (0, 2, 1, 3):
            x_piece(p).start()
        for cp in smalls[1:]:
            cp.start()
        gy_load = pltpu.make_async_copy(gy_hbm, gy_ref, s_x.at[6])
        gy_load.start()
        for i in range(3):
            head_w(i).start()
        wo_load().start()
        stat_tile(0, start)
        pl.semaphore_wait(barrier, 3)
        ring0(1, 0, 0).start()
        ring0(1, 1, 0).start()
        smalls[0].wait()
        g_ref[2:3, :] = gn1_ref[...].astype(f32).reshape(1, d)

        def norm_piece(p):
            rs = pl.ds(p * sub, sub)
            x_piece(p).wait()

            def sq_step(i, acc):
                xf = x_ref[rs, hs(i)].astype(f32)
                return acc + xf * xf

            acc = lax.fori_loop(0, nd, sq_step, jnp.zeros((sub, HEAD), f32))
            xi = lax.rsqrt(jnp.sum(acc, axis=1, keepdims=True) * (1.0 / d) + NORM_EPS)
            xinv[rs, :] = jnp.broadcast_to(xi, (sub, HEAD))

            def hid_step(i):
                hid[rs, hs(i)] = (x_ref[rs, hs(i)].astype(f32) * xi * g_ref[2:3, hs(i)]).astype(bf16)

            loop(0, nd, hid_step)

        for p in (0, 2, 1, 3):
            norm_piece(p)
            ring0(0, p // 2, p % 2).start()
        for cp in smalls[1:]:
            cp.wait()
        for w, src in enumerate((gq_ref, gk_ref)):
            g_ref[w:w + 1, :] = src[...].astype(f32).reshape(1, d)
        zero = jnp.zeros((t_loc, HEAD), f32)
        inv[...] = jnp.zeros_like(inv)
        gy_load.wait()
        own_loc(1).start()
    own_par(0).start()
    own_par(1).start()
    own_loc(0).start()
    settle(wh, s_x.at[0])
    wo_load().wait()

    hb = t_loc // 2

    def finish(s):
        for direction in range(2):
            bz = lax.rem(z + nz - 1 - s, nz) if direction == 0 else lax.rem(z + 1 + s, nz)

            def one(core):
                b = bz * 2 + core
                rs = ds(b * 2 + direction, hb)
                st = sall[b, 0:3, direction * hb:(direction + 1) * hb]
                ang = spread_col(st[2:3, :]) * fr_ref[0:1, :]
                co = jnp.cos(ang)
                si = jnp.sin(ang)
                csT[0, :, rs] = co.T[:half, :]
                csT[1, :, rs] = si.T[:half, :]
                si = si * sgn
                for w, dst in enumerate((q_s, k_s)):
                    hat = raw[w, rs, :] * spread_col(st[w:w + 1, :])
                    hatT[w, :, rs] = hat.T
                    hat = hat * g_ref[w:w + 1, cols]
                    dst[rs, :] = (hat * co + pltpu.roll(hat, half, 1) * si).astype(bf16)
                v_s[rs, :] = raw[2, rs, :].astype(bf16)

            loop(0, 2, one)

    def qkv_work(xv):
        return dotf(xv, wh[...], NN)

    def qkv_put(r, where):
        step = r.shape[0] // len(where)
        for i, rs in enumerate(where):
            for w in range(3):
                raw[w, rs, :] = r[i * step:(i + 1) * step, w * HEAD:(w + 1) * HEAD]

    spt = 2 * nt // 4

    def x_tick(t):
        gather(0, t, qkv_work, qkv_put)

        @pl.when(t == 2 * last - 1)
        def _():
            for direction in range(2):
                ring0(1, direction, 1).start()
            comm(1, 0)

        @pl.when(t < 4)
        def _():
            with scope('stat'):
                loop(t * spt, (t + 1) * spt, stat_step)

        @pl.when(t == 4)
        def _():
            with scope('statdone'):
                stat_done()

        @pl.when(t == 8)
        def _():
            for e in far:
                st_send(e).start()
            w2(start)

        @pl.when(t == 10)
        def _():
            settle(sall.at[pl.ds(0, n - 1), pl.ds(0, 3)], s_st.at[0], r_st.at[0])
        lo = jnp.where(t == 10, -1, jnp.where(t == 11, 1, jnp.where(t >= 12, t - 9, 0)))
        hi = jnp.where(t == 10, 1, jnp.where(t == 11, 3, jnp.where((t >= 12) & (t <= 14), t - 8, -1)))
        with scope('finish'):
            loop(lo, hi, finish)

    with scope('gather_x'):
        loop(0, ticks + 2, x_tick)

    def attend(j):
        qs = ds(j, blk)
        q = q_s[qs, :]

        def unit(kb, carry, masked):
            m, l, acc = carry
            ks = ds(kb, blk)
            s = dotf(q, k_s[ks, :], NT)
            if masked:
                r = lax.broadcasted_iota(jnp.int32, (blk, blk), 0)
                cc = lax.broadcasted_iota(jnp.int32, (blk, blk), 1)
                s = jnp.where(r >= cc, s, -1e30)
            mn = jnp.maximum(m, jnp.max(s, axis=1, keepdims=True))
            al = jnp.exp2((m - mn) * cexp)
            p = jnp.exp2((s - mn) * cexp)
            l = l * al + jnp.sum(p, axis=1, keepdims=True)
            acc = acc * al + dotf(p.astype(bf16), v_s[ks, :], NN)
            return mn, l, acc

        init = (jnp.full((blk, 1), -1e30, f32), jnp.zeros((blk, 1), f32), jnp.zeros((blk, HEAD), f32))
        carry = lax.fori_loop(0, j, functools.partial(unit, masked=False), init)
        m, l, acc = unit(j, carry, True)
        o = acc / l
        raw[2, qs, :] = o
        o_s[qs, :] = o.astype(bf16)
        lse[0:1, qs] = as_row(m * cexp + jnp.log2(l))

    def o_send(e):
        to = peer(e)
        return remote(o_s.at[rows(to), :], att.at[:, cols], s_o.at[0], r_o.at[0], to)

    def h_unit(u):
        return pltpu.make_async_copy(h_all.at[rows(u), :], wrow.at[1, lax.rem(u, 2)], s_hu.at[lax.rem(u, 2)])

    def kv_unit(u):
        h_unit(u).wait()

        @pl.when(u < n - 1)
        def _():
            h_unit(u + 1).start()
        xv = wrow[1, lax.rem(u, 2)]
        rs = rows(u)
        st = sall[u, 0:3, :]
        ang = spread_col(st[2:3, :]) * fr_ref[0:1, :]
        co = jnp.cos(ang)
        si = jnp.sin(ang) * sgn

        def turned(r, w, i):
            hat = r[:, i * HEAD:(i + 1) * HEAD] * spread_col(st[w:w + 1, :]) * g_ref[w:w + 1, hs(h2(i))]
            return (hat * co + pltpu.roll(hat, half, 1) * si).astype(bf16)

        @pl.when(u < 2 * z + 2)
        def _():
            rk = dotf(xv, wtile[0], NN)
            rv = dotf(xv, wtile[1], NN).astype(bf16)
            for i in range(2):
                k2[i, rs, :] = turned(rk, 1, i)
                v2[i, rs, :] = rv[:, i * HEAD:(i + 1) * HEAD]

        @pl.when(u >= 2 * z)
        def _():
            rq = dotf(xv, tile[0, 0:d, :], NN)
            for i in range(2):
                @pl.when(u < 2 * z + 2)
                def _():
                    q2[i, rows(u - 2 * z), :] = turned(rq, 0, i)

                @pl.when(u >= 2 * z + 2)
                def _():
                    k2[i, rs, :] = turned(rq, 0, i)

    def do_again(gv, core):
        r = dotf(gv, wrow[0, 0], NT).astype(bf16)
        for i in range(2):
            do2[i, rows(core), :] = r[:, i * HEAD:(i + 1) * HEAD]

    def do_work(xv):
        return dotf(xv, woh[...], NT).astype(bf16), xv

    def do_put(r, where):
        r, xv = r
        step = r.shape[0] // len(where)
        for i, rs in enumerate(where):
            do_s[rs, :] = r[i * step:(i + 1) * step]
        if len(where) == 4:
            w = dotf(xv, wrow[0, 0], NT).astype(bf16)
            for j, rs in enumerate(where):
                @pl.when(rs.start >= 2 * t_loc * (z + 1))
                def _():
                    for i in range(2):
                        v2[i, rs, :] = w[j * step:(j + 1) * step, i * HEAD:(i + 1) * HEAD]

    def y_tick(t):
        gather(1, t, do_work, do_put)

        @pl.when(t == 1)
        def _():
            with scope('finish'):
                finish(last)
        t = t - 1
        lo = jnp.where(t == 0, 0, jnp.where(t <= 4, t + 1, jnp.where(t <= 6, 6, 7)))
        hi = jnp.where(t == 0, 2, jnp.where(t <= 4, t + 2, jnp.where(t == 5, 6, jnp.where(t == 8, 8, 7))))
        hi = jnp.where(t < 0, 0, hi)
        with scope('attend'):
            loop(lo, hi, attend)

        @pl.when(t == ticks - 3)
        def _():
            send_all(o_send, far[-5:])

        @pl.when(t == ticks - 2)
        def _():
            send_all(o_send, far[:-5])

        @pl.when(t == -1)
        def _():
            settle(wrow.at[0, 0], s_r2.at[2])
            do_again(gy_ref[...], c)
            settle(h_all.at[pl.ds(0, 2 * t_loc), :], s_loc.at[0])
            h_unit(0).start()
            settle(wtile, s_r2.at[0])
            settle(tile.at[0, pl.ds(0, d), :], s_r2.at[1])

        @pl.when(t == 0)
        def _():
            do_again(xbuf[1], 1 - c)
        first = jnp.where(t == 1, 0, jnp.where(t == 2, 1, jnp.where(t == 5, 2, jnp.where(t == 7, 5, jnp.where(t == 9, 8, jnp.where(t == 10, 11, jnp.where(t == 11, 14, 16)))))))
        count = jnp.where((t == 1) | (t == 2), 1, jnp.where((t == 5) | (t == 7) | (t == 9) | (t == 10), 3, jnp.where(t == 11, 2, 0)))
        with scope('again_kv'):
            loop(first, first + count, kv_unit)

    with scope('gather_y'):
        loop(0, ticks + 2, y_tick)

    def gy_copy(t):
        return pltpu.make_async_copy(gy_all.at[:, ds(t, cw)], tile.at[lax.rem(t, 2)], s_t.at[lax.rem(t, 2)])

    def h_copy(t):
        return pltpu.make_async_copy(h_all.at[:, ds(lax.rem(t, nt), cw)], tile.at[lax.rem(t, 2)], s_t.at[lax.rem(t, 2)])

    def h2_copy(t):
        return pltpu.make_async_copy(h_all.at[:, ds(chip(t), cw)], tile.at[lax.rem(t, 2)], s_t.at[lax.rem(t, 2)])

    hw = d // 2

    def wo_half(h):
        k = lax.rem(h, 2)
        return pltpu.make_async_copy(wo_ref.at[ds(k, hw), ds(h // 2, cw)], wtile.at[lax.rem(h // 2, 2), ds(k, hw), :], s_w4.at[lax.rem(h, 4)])

    def q_send(e):
        to = peer(e)
        return remote(dq_s.at[rows(to), :], tq.at[:, cols], s_q.at[0], r_q.at[0], to)

    def kv_send(to):
        return remote(dkv.at[to], tkv.at[:, :, cols], s_kv.at[0], r_kv.at[0], to)

    gy_copy(0).start()
    for h in range(4):
        wo_half(h).start()
    settle(h_all.at[pl.ds(0, (nz - 1) * t_loc), :], s_ring.at[0])
    settle(h_all.at[pl.ds(0, nz * t_loc), :], s_par.at[0])

    att[:, cols] = o_s[rows(me), :]
    raw[0] = jnp.zeros((t_all, HEAD), f32)

    def delta(j):
        qs = ds(j, blk)
        lse[1:2, qs] = as_row(jnp.sum(raw[2, qs, :] * do_s[qs, :].astype(f32), axis=1, keepdims=True))

    with scope('delta'):
        loop(0, nb, delta)

    def ld_send(gap, core, slot):
        to = lax.rem(z + gap, nz) * 2 + core
        return remote(lse.at[pl.ds(0, 2)], ld2.at[slot, pl.ds(0, 2)], s_ld2.at[0], r_ld2.at[0], to)

    ld_send(nz // 2, c, 0).start()

    @pl.when(again)
    def _():
        ld_send(nz - 2, 0, 1).start()
        ld_send(2, 1, 1).start()

    def bwd_step(s):
        kb = chip(lax.rem(s + 1, nz))
        ks = ds(kb, blk)
        k = k_s[ks, :]
        v = v_s[ks, :]

        def unit(qb, carry, masked):
            dk, dv = carry
            qs = ds(qb, blk)
            q = q_s[qs, :]
            do = do_s[qs, :]
            p = jnp.exp2(dotf(k, q, NT) * cexp - lse[0:1, qs])
            if masked:
                r = lax.broadcasted_iota(jnp.int32, (blk, blk), 0)
                cc = lax.broadcasted_iota(jnp.int32, (blk, blk), 1)
                p = jnp.where(cc >= r, p, 0.0)
            g = (p * (dotf(v, do, NT) - lse[1:2, qs])).astype(bf16)
            dv = dv + dotf(p.astype(bf16), do, NN)
            dk = dk + dotf(g, q, NN)
            raw[0, qs, :] = raw[0, qs, :] + dotf(g, k, TN)
            return dk, dv

        zk = jnp.zeros((blk, HEAD), f32)
        carry = unit(kb, (zk, zk), True)
        dk, dv = lax.fori_loop(kb + 1, nb, functools.partial(unit, masked=False), carry)
        dk = (dk * scale).astype(bf16)
        dv = dv.astype(bf16)
        for u in range(2):
            dkv[2 * kb + u, 0] = dk[u * t_loc:(u + 1) * t_loc]
            dkv[2 * kb + u, 1] = dv[u * t_loc:(u + 1) * t_loc]

        @pl.when((kb != z) & to_send(2 * kb))
        def _():
            for u in range(2):
                kv_send(2 * kb + u).start()

        @pl.when(kb == z)
        def _():
            kv_send(mate).start()

    with scope('bwd'):
        loop(0, nb, bwd_step)
        dq_s[...] = (raw[0] * scale).astype(bf16)
    gcol = [spread_col(g_ref[w:w + 1, cols])[:, 0:1] for w in range(2)]

    def unroped(src, js):
        ct = csT[0, :, js]
        sn = csT[1, :, js]
        t = src.astype(f32).T
        p, r = t[:half], t[half:]
        return jnp.concatenate([p * ct + r * sn, r * ct - p * sn], axis=0)

    def share_step(j, carry):
        js = rows(j)
        res = []
        for w, src in enumerate((dq_s[js, :], dkv[j, 0])):
            th = unroped(src, js) * hatT[w, :, js]
            res.append(carry[w] + th)
            pm[j, w:w + 1, :] = jnp.sum(th * gcol[w], axis=0, keepdims=True)
        return tuple(res)

    def p_send(e):
        to = peer(e)
        return remote(pm.at[to, pl.ds(0, 2)], pall.at[me, pl.ds(0, 2)], s_p.at[0], r_p.at[0], to)

    with scope('share'):
        zt = jnp.zeros((HEAD, t_loc), f32)
        sums = lax.fori_loop(0, n, share_step, (zt, zt))
    for e in far:
        p_send(e).start()
    send_all(q_send, far)

    tq[:, cols] = dq_s[rows(me), :]
    tkv[:, :, cols] = dkv[me]

    pall[me, 0:2, :] = pm[me, 0:2, :]
    for w in range(2):
        gg_s[w] = jnp.broadcast_to(jnp.sum(sums[w], axis=1, keepdims=True), (HEAD, HEAD)).T[0:8, :]

    def flip_o(i):
        rawT[0:HEAD, rows(i)] = o_s[rows(i), :].T

    def flip_v(i):
        rawT[0:HEAD, rows(i)] = dkv[i, 1].T

    def dwo_step(t):
        gy_copy(t).wait()

        @pl.when(t + 1 < nt)
        def _():
            gy_copy(t + 1).start()

        @pl.when(t + 1 == nt)
        def _():
            h_copy(t + 1).start()
        r = dotf(rawT[0:HEAD, :], tile[lax.rem(t, 2)], NN)
        for u in range(cw // HEAD):
            raw[2, hs(n + t * (cw // HEAD) + u), :] = r[:, u * HEAD:(u + 1) * HEAD]

    def dwv_step(t):
        h_copy(t).wait()

        @pl.when(t + 1 < 2 * nt)
        def _():
            h_copy(t + 1).start()

        @pl.when(t + 1 == 2 * nt)
        def _():
            h2_copy(0).start()
        r = dotf(rawT[0:HEAD, :], tile[lax.rem(t, 2)], NN)
        for u in range(cw // HEAD):
            raw[2, hs((t - nt) * (cw // HEAD) + u), :] = r[:, u * HEAD:(u + 1) * HEAD].T

    def y_step(t):
        cs = ds(t, cw)
        acc = x_ref[:, cs].astype(f32)
        for k in range(2):
            h = 2 * t + k
            wo_half(h).wait()
            acc = acc + dotf(att[:, k * hw:(k + 1) * hw], wtile[lax.rem(t, 2), k * hw:(k + 1) * hw, :], NN)

            @pl.when(h + 4 < 2 * nt)
            def _():
                wo_half(h + 4).start()
        hid[:, cs] = acc.astype(bf16)

    def v_send(e):
        to = peer(e)
        return remote(raw.at[2, hs(to), :], dwv_out.at[:, cols], s_v.at[0], r_v.at[0], to)

    def out(i):
        src, dst, k = ((hid, y_out, 0), None, (xbuf.at[0], gx_out, 0), (raw.at[2, hs(me), :], dwv_out.at[:, cols], 2),
                       (raw.at[1, rows_f(0, me), :], dwq_out.at[:, cols], 2), (raw.at[1, rows_f(1, me), :], dwk_out.at[:, cols], 2),
                       (gg_s, gg_out, 3), (gpart.at[me], gall.at[me], 4))[i]
        return pltpu.make_async_copy(src, dst, s_out.at[k])

    def rows_f(w, to):
        return ds(w * n + to, HEAD)

    with scope('dwo'):
        loop(0, n, flip_o)
        loop(0, nt, dwo_step)
        for j in range(n):
            pltpu.make_async_copy(raw.at[2, pl.ds((n + j) * HEAD, HEAD), :], dwo_out.at[:, pl.ds(j * HEAD, HEAD)], s_out.at[1]).start()

    def m_send(e):
        return remote(mine2.at[pl.ds(0, 2)], mall.at[me, pl.ds(0, 2)], s_m.at[0], r_m.at[0], peer(e))

    with scope('dwv'):
        loop(0, n, flip_v)
        loop(nt, 2 * nt, dwv_step)
        out(3).start()
    with scope('pwait'):
        settle(pall.at[pl.ds(0, n - 1), pl.ds(0, 2)], s_p.at[0], r_p.at[0])
        tot = pall[0, 0:2, :]
        for j in range(1, n):
            tot = tot + pall[j, 0:2, :]
        mine2[0:2, :] = tot * (1.0 / d)
    for e in far:
        m_send(e).start()
    mall[me, 0:2, :] = mine2[0:2, :]
    for e in far:
        v_send(e).start()
    def got(buf, s_sem, r_sem):
        settle(buf.at[pl.ds(0, (n - 5) * msg), :], r_sem.at[0])

        @pl.when(sent)
        def _():
            settle(buf.at[pl.ds(0, (n - 3) * msg), :], s_sem.at[0])

        @pl.when(again)
        def _():
            settle(buf.at[pl.ds(0, (n - 7) * msg), :], s_sem.at[0])

    def o2_send(i):
        return remote(o2.at[i, rows(1 - c), :], att.at[:, hs(h2(i))], s_o2.at[0], r_o2.at[0], mate)

    def q2_send(i):
        return remote(dq2.at[i, rows(1 - c), :], tq.at[:, hs(h2(i))], s_q2.at[0], r_q2.at[0], mate)

    def again_head(i):
        q = q2[i]
        do = do2[i]
        r0 = lax.broadcasted_iota(jnp.int32, (blk, blk), 0)
        c0 = lax.broadcasted_iota(jnp.int32, (blk, blk), 1)

        def unit(kb, carry, masked):
            m, l, acc = carry
            ks = ds(kb, blk)
            s = dotf(q, k2[i, ks, :], NT)
            if masked:
                s = jnp.where(r0 >= c0, s, -1e30)
            mn = jnp.maximum(m, jnp.max(s, axis=1, keepdims=True))
            al = jnp.exp2((m - mn) * cexp)
            p = jnp.exp2((s - mn) * cexp)
            l = l * al + jnp.sum(p, axis=1, keepdims=True)
            acc = acc * al + dotf(p.astype(bf16), v2[i, ks, :], NN)
            return mn, l, acc

        init = (jnp.full((blk, 1), -1e30, f32), jnp.zeros((blk, 1), f32), jnp.zeros((blk, HEAD), f32))
        m, l, acc = unit(z, lax.fori_loop(0, z, functools.partial(unit, masked=False), init), True)
        o = acc / l
        o2[i] = o.astype(bf16)
        ls = m * cexp + jnp.log2(l)
        de = jnp.sum(o * do.astype(f32), axis=1, keepdims=True)

        def unit2(kb, dq, masked):
            ks = ds(kb, blk)
            k = k2[i, ks, :]
            p = jnp.exp2(dotf(q, k, NT) * cexp - ls)
            if masked:
                p = jnp.where(r0 >= c0, p, 0.0)
            g = (p * (dotf(do, v2[i, ks, :], NT) - de)).astype(bf16)
            return dq + dotf(g, k, NN)

        dq = unit2(z, lax.fori_loop(0, z, functools.partial(unit2, masked=False), jnp.zeros((blk, HEAD), f32)), True)
        dq2[i] = (dq * scale).astype(bf16)

        k = k2[i, ds(z, blk), :]
        v = v2[i, ds(z, blk), :]

        def unit3(carry, qq, dd, qb, masked):
            dk, dv = carry
            qs = ds(qb, blk)
            p = jnp.exp2(dotf(k, qq, NT) * cexp - ld2[i, 0:1, qs])
            if masked:
                p = jnp.where(c0 >= r0, p, 0.0)
            g = (p * (dotf(v, dd, NT) - ld2[i, 1:2, qs])).astype(bf16)
            return dk + dotf(g, qq, NN), dv + dotf(p.astype(bf16), dd, NN)

        def later(qb, carry):
            qs = ds(qb, blk)
            return unit3(carry, k2[i, qs, :], v2[i, qs, :], qb, False)

        zk = jnp.zeros((blk, HEAD), f32)
        dk, dv = lax.fori_loop(z + 1, nb, later, unit3((zk, zk), q, do, z, True))
        dkv2[i, 0] = (dk * scale).astype(bf16)
        dkv2[i, 1] = dv.astype(bf16)
        for w in range(2):
            tkv[w, :, hs(h2(i))] = dkv2[i, w, rows(c), :]
        att[:, hs(h2(i))] = o2[i, rows(c), :]
        tq[:, hs(h2(i))] = dq2[i, rows(c), :]

    def kv2_send(i):
        return remote(dkv2.at[i, :, rows(1 - c), :], tkv.at[:, :, hs(h2(i))], s_kv2.at[0], r_kv2.at[0], mate)

    pair = ld2.at[pl.ds(0, 1), pl.ds(0, 2)]
    with scope('ldwait'):
        settle(ld2.at[:, pl.ds(0, 2)], r_ld2.at[0])

        @pl.when(sent)
        def _():
            settle(pair, s_ld2.at[0])

        @pl.when(again)
        def _():
            settle(ld2.at[:, pl.ds(0, 3)], s_ld2.at[0])

    def again_both(i):
        again_head(i)
        o2_send(i).start()
        q2_send(i).start()
        kv2_send(i).start()


    def w_copies(t):
        slot = lax.rem(t, 2)
        return [pltpu.make_async_copy(w.at[ds(t, wr), :], wrow.at[slot, i], s_wr.at[slot]) for i, w in enumerate((wq_ref, wk_ref, wv_ref))]

    for cp in w_copies(0):
        cp.start()
    cl = cl_s[...]
    sl = sl_s[...]

    def back_rope(a):
        a = a.astype(f32)
        return a * cl + pltpu.roll(a, half, 1) * sl

    def loc_step(i):
        tq[:, hs(i)] = (inv[0] * (back_rope(tq[:, hs(i)]) * g_ref[0:1, hs(i)] - qkl[0, :, hs(i)] * inv[0] * mq)).astype(bf16)
        tkv[0, :, hs(i)] = (inv[1] * (back_rope(tkv[0, :, hs(i)]) * g_ref[1:2, hs(i)] - qkl[1, :, hs(i)] * inv[1] * mk)).astype(bf16)

    def head_step(j):
        js = rows(j)
        for w, src in enumerate((dq_s[js, :], dkv[j, 0])):
            rawT[w * HEAD:(w + 1) * HEAD, js] = (sall[j, w:w + 1, :] * (unroped(src, js) * gcol[w] - hatT[w, :, js] * mall[j, w:w + 1, :])).astype(bf16)

    def a_send(to):
        return remote(raw.at[1, rows_f(0, to), :], dwq_out.at[:, cols], s_a.at[0], r_a.at[0], to)

    def b_send(to):
        return remote(raw.at[1, rows_f(1, to), :], dwk_out.at[:, cols], s_b.at[0], r_b.at[0], to)

    def dw_step(t):
        h2_copy(t).wait()

        @pl.when(t + 1 < nt)
        def _():
            h2_copy(t + 1).start()
        nn = chip(t)
        r = dotf(rawT[...], tile[lax.rem(t, 2)], NN)
        for u in range(cw // HEAD):
            to = nn * (cw // HEAD) + u
            for w in range(2):
                raw[1, rows_f(w, to), :] = r[w * HEAD:(w + 1) * HEAD, u * HEAD:(u + 1) * HEAD].T

            @pl.when(to != me)
            def _():
                a_send(to).start()
                b_send(to).start()

    def phase(i):
        with scope('again'):
            again_both(i)

        @pl.when(i == 0)
        def _():
            with scope('mwait'):
                settle(mall.at[pl.ds(0, n - 1), pl.ds(0, 2)], s_m.at[0], r_m.at[0])
            with scope('head'):
                loop(0, n, head_step)
            with scope('dw'):
                loop(0, nt - 2, dw_step)

    loop(0, 2, phase)
    with scope('waitkv'):
        settle(tkv.at[:, pl.ds(0, (n - 5) * msg), :], r_kv.at[0])

        @pl.when(sent)
        def _():
            settle(tkv.at[:, pl.ds(0, (n - 3) * msg), :], s_kv.at[0])

        @pl.when(again)
        def _():
            settle(tkv.at[:, pl.ds(0, (n - 7) * msg), :], s_kv.at[0])
        settle(tkv.at[:, pl.ds(0, 2 * msg), :], s_kv2.at[0], r_kv2.at[0])
    with scope('waitq'):
        got(tq, s_q, r_q)
        settle(tq.at[pl.ds(0, 2 * msg), :], s_q2.at[0], r_q2.at[0])

    mq = spread_col(mine2[0:1, :])
    mk = spread_col(mine2[1:2, :])
    with scope('loc'):
        loop(0, nd, loc_step)

    def dh_step(t):
        settle(wrow.at[lax.rem(t, 2)], s_wr.at[lax.rem(t, 2)])

        @pl.when(t + 1 < nw)
        def _():
            for cp in w_copies(t + 1):
                cp.start()
        slot = lax.rem(t, 2)
        r = dotf(tq[...], wrow[slot, 0], NT) + dotf(tkv[0], wrow[slot, 1], NT) + dotf(tkv[1], wrow[slot, 2], NT)
        dh[:, ds(t, wr)] = r.astype(bf16).astype(f32)

    with scope('dh'):
        loop(0, nw, dh_step)

    def mx_step(i, acc):
        return acc + dh[:, hs(i)] * g_ref[2:3, hs(i)] * x_ref[:, hs(i)].astype(f32)

    def g_send(e):
        return remote(gpart.at[peer(e), pl.ds(0, 1)], gall.at[me, pl.ds(0, 1)], s_g.at[0], r_g.at[0], peer(e))

    with scope('gx'):
        mx = jnp.sum(lax.fori_loop(0, nd, mx_step, zero), axis=1, keepdims=True) * (1.0 / d) * xinv[...]

        def gx_step(i):
            xh = x_ref[:, hs(i)].astype(f32) * xinv[...]
            dhh = dh[:, hs(i)]
            gpart[i] = jnp.broadcast_to(jnp.sum(dhh * xh, axis=0, keepdims=True), (8, HEAD))
            xbuf[0, :, hs(i)] = (gy_ref[:, hs(i)].astype(f32) + xinv[...] * (dhh * g_ref[2:3, hs(i)] - xh * mx)).astype(bf16)

        loop(0, nd, gx_step)
        out(2).start()
    for e in far:
        g_send(e).start()
    out(7).start()
    out(6).start()
    with scope('dw2'):
        loop(nt - 2, nt, dw_step)
        out(4).start()
        out(5).start()
    with scope('y'):
        got(att, s_o, r_o)
        settle(att.at[pl.ds(0, 2 * msg), :], s_o2.at[0], r_o2.at[0])
        loop(0, nt, y_step)
        out(0).start()
    with scope('end_drain'):
        settle(gy_all.at[pl.ds(0, (nz - 1) * t_loc), :], s_ring.at[1])
        settle(gy_all.at[pl.ds(0, nz * t_loc), :], s_par.at[1])
        settle(tkv, s_out.at[0])
        settle(raw.at[2, pl.ds(0, n * HEAD), :], s_out.at[1])
        settle(raw.at[2, pl.ds(0, 3 * HEAD), :], s_out.at[2])
        settle(gg_s, s_out.at[3])
        settle(gpart.at[0], s_out.at[4])
    most = pl.ds(0, HEAD - HEAD // n)
    with scope('end_v'):
        settle(dwv_out.at[most, :], s_v.at[0], r_v.at[0])
    with scope('end_a'):
        settle(dwq_out.at[most, :], s_a.at[0], r_a.at[0])
    with scope('end_b'):
        settle(dwk_out.at[most, :], s_b.at[0], r_b.at[0])
    with scope('end_g'):
        settle(gall.at[pl.ds(0, n - 1), pl.ds(0, 1)], s_g.at[0], r_g.at[0])


def block(n, x, gy, pos, gq, gk, gn, freq, wq, wk, wv, wo):
    t_loc, d = x.shape
    t_all = t_loc * n
    hb = pl.BlockSpec(memory_space=pl.ANY)
    S = jax.ShapeDtypeStruct
    V = pltpu.VMEM
    sem = pltpu.SemaphoreType.DMA
    hd = (t_all, HEAD)
    tok = (t_loc, d)
    nz = n // 2
    return pl.pallas_call(functools.partial(block_kernel, n),
        in_specs=[hb] * 11,
        out_specs=[hb] * 10,
        out_shape=[S(tok, bf16), S(tok, bf16), S((n, 8, d // n), f32)] + [S((d // n, d), f32)] * 4 + [S((2, 8, HEAD), f32), S((t_all, d), bf16), S((t_all, d), bf16)],
        scratch_shapes=[V((1, t_loc), jnp.int32), V((d,), bf16), V((d,), bf16), V((d,), bf16), V((8, HEAD), f32), V(tok, bf16), V(tok, bf16), V((8, d), f32), V(tok, bf16), V((d, 3 * HEAD), bf16), V((HEAD, d), bf16), V((3,) + hd, f32), V((2,) + tok, bf16), V((2, d, 2 * HEAD), bf16), V((2, t_all, 2 * HEAD), bf16), V((2, 3, 2 * HEAD, d), bf16),
            V((2,) + tok, f32), V((2, HEAD, t_all), f32), V((2, HEAD // 2, t_all), f32)] + [V(hd, bf16)] * 5 + [V((8, t_all), f32), V((2, 8, t_all), f32)]
        + [V(hd, bf16), V((n, 2, t_loc, HEAD), bf16), V(tok, bf16), V((2,) + tok, bf16), V(tok, bf16), V((2 * HEAD, t_all), bf16), V(tok, f32),
            V((t_loc, HEAD), f32), V((t_loc, HEAD), f32), V((2, t_loc, HEAD), f32), V((t_loc, HEAD), f32), V((8, t_loc), f32), V((n, 8, t_loc), f32), V((8, t_loc), f32), V((n, 8, t_loc), f32), V((n, 8, t_loc), f32), V((n, 8, t_loc), f32), V((n, 8, d // n), f32), V((2, 8, HEAD), f32)] + [V((2, t_all, HEAD), bf16)] * 2 + [V((2, 2 * t_loc, HEAD), bf16)] * 4 + [V((2, 2, 2 * t_loc, HEAD), bf16)]
        + [sem((2,)), sem((2, 2, nz - 1, 2)), sem((2,)), sem((2, 2 * (nz - 1))), sem((2,))] + [sem((1,))] * 20
        + [sem((2,)), sem((2,)), sem((2,)), sem((7,)), sem((2,)), sem((1,)), sem((5,)), sem((5,)), sem((3,)), sem((2,))] + [sem((1,))] * 8 + [sem((4,))],
        compiler_params=pltpu.CompilerParams(collective_id=1, has_side_effects=True, vmem_limit_bytes=67043328), name='block')(x, gy, pos, gq, gk, gn, freq, wq, wk, wv, wo)


def copy_kernel(*refs):
    k = (len(refs) - 2) // 3
    src, dst, buf, si, so = list(refs[:k - 1]), refs[k - 1:2 * k - 1], refs[2 * k - 1:3 * k - 1], refs[-2], refs[-1]
    parts = src[k - 3]
    src[k - 3:] = [parts, src[k - 2].at[0, 0:1, :], src[k - 2].at[1, 0:1, :]]
    buf = list(buf)
    total = buf[k - 3]
    buf[k - 3] = refs[-3]
    ins = [pltpu.make_async_copy(src[i], buf[i], si.at[i]) for i in range(k)]
    outs = [pltpu.make_async_copy(buf[i], dst[i], so.at[i]) if i != k - 3 else None for i in range(k)]
    for cp in ins:
        cp.start()
    outs[k - 3] = pltpu.make_async_copy(total, dst[k - 3], so.at[k - 3])
    for i in range(k):
        ins[i].wait()
        if i == k - 3:
            total[...] = jnp.sum(refs[-3][:, 0:1, :], axis=0)
        outs[i].start()
    for cp in outs:
        cp.wait()


def copy_out(arrays):
    hb = pl.BlockSpec(memory_space=pl.ANY)
    shapes = [(a.shape, a.dtype) for a in arrays[:-2]] + [((1, HEAD), f32)] * 3
    k = len(shapes)
    return pl.pallas_call(copy_kernel, in_specs=[hb] * len(arrays), out_specs=[hb] * k, out_shape=[jax.ShapeDtypeStruct(*a) for a in shapes],
        scratch_shapes=[pltpu.VMEM(*a) for a in shapes] + [pltpu.VMEM(arrays[-2].shape, f32)] + [pltpu.SemaphoreType.DMA((k,))] * 2, name='copy_out')(*arrays)


def solution(mesh):
    n = mesh.shape['sp']

    def device_step(x_in, grad_y, positions, g_norm, wq, wk, wv, wo, gq, gk):
        half = HEAD // 2
        inv_freq = ROPE_BASE ** (-np.arange(half) * (2.0 / HEAD))
        freq = jnp.asarray(np.tile(inv_freq, (8, 2)), f32)
        y, gx, gn, dwq, dwk, dwv, dwo, gg, _, _ = block(n, x_in[0], grad_y[0], positions, gq, gk, g_norm, freq, wq, wk, wv, wo)
        y, gx, dwq, dwk, dwv, dwo, gn, ggq, ggk = copy_out([y, gx, dwq, dwk, dwv, dwo, gn, gg])
        return (y[None], gx[None], gn[0], dwq, dwk, dwv, dwo, ggq[0], ggk[0])

    seq_spec = P('dp', 'sp', None)
    rep2, rep1 = P(None, None), P(None)
    row_spec, vec_spec = P(('dp', 'sp'), None), P(('dp', 'sp'))
    return jax.shard_map(device_step, mesh=mesh, in_specs=(seq_spec, seq_spec, P('dp', 'sp'), rep1, rep2, rep2, rep2, rep2, rep1, rep1), out_specs=(seq_spec, seq_spec, vec_spec, row_spec, row_spec, row_spec, row_spec, vec_spec, vec_spec), check_vma=False)
```
